8 devices in a mesh: dp: 1 (over z), tp: 8 (over y, x, core).
Axes of the slice: x: 2, y: 2, z: 1, core: 2. Of those that a mesh axis runs over, the one named last changes fastest.
Arguments:
- x_in: bfloat16 [32, 512, 1024], P('dp', 'tp')
- grad_y: bfloat16 [32, 512, 1024], P('dp', 'tp')
- pad_mask: int32 [32, 512], P('dp')
- ln1_gain: float32 [1024], replicated
- ln1_bias: float32 [1024], replicated
- w_qkv: bfloat16 [3, 1024, 16, 64], P(None, None, 'tp')
- b_qkv: float32 [3, 16, 64], P(None, 'tp')
- w_out: bfloat16 [16, 64, 1024], P('tp')
- b_out: float32 [1024], replicated
- ln2_gain: float32 [1024], replicated
- ln2_bias: float32 [1024], replicated
- w_up: bfloat16 [1024, 4096], P(None, 'tp')
- b_up: float32 [4096], P('tp')
- w_down: bfloat16 [4096, 1024], P('tp')
- b_down: float32 [1024], replicated
Outputs:
- output 1: bfloat16 [32, 512, 1024], P('dp', 'tp')
- output 2: bfloat16 [32, 512, 1024], P('dp', 'tp')
- output 3: float32 [1024], P('dp')
- output 4: float32 [1024], P('dp')
- output 5: float32 [3, 1024, 16, 64], P('dp', None, 'tp')
- output 6: float32 [3, 16, 64], P('dp', 'tp')
- output 7: float32 [16, 64, 1024], P(('dp', 'tp'))
- output 8: float32 [1024], P('dp')
- output 9: float32 [1024], P('dp')
- output 10: float32 [1024], P('dp')
- output 11: float32 [1024, 4096], P('dp', 'tp')
- output 12: float32 [4096], P(('dp', 'tp'))
- output 13: float32 [4096, 1024], P(('dp', 'tp'))
- output 14: float32 [1024], P('dp')
All inputs are finite; a program needn't handle non-finite values.
Results may differ from the reference program's by a relative error of at most 0.0121107.
Values are sent between devices in bfloat16 or wider.
A program may use at most 1 GiB of HBM per device.

```python
import jax
import jax.numpy as jnp
from jax import lax

BATCH_SEQS = 32
SEQ_LEN = 512
MODEL_DIM = 1024
NUM_HEADS = 16
HEAD_DIM = 64
FFN_DIM = 4096
HALF_DIM = HEAD_DIM // 2
TOKENS = BATCH_SEQS * SEQ_LEN
LN_EPS = 1e-5
ROPE_BASE = 10000.0
INV_SQRT2 = 0.7071067811865476
INV_SQRT_2PI = 0.3989422804014327
NEG_LARGE = -1e30


def setup_inputs(seed: int = 0, part: int = 0) -> dict:
    root_key = jax.random.key(seed)
    shared_key, data_key = jax.random.split(root_key)
    weight_keys = jax.random.split(shared_key, 12)
    part_key = jax.random.fold_in(data_key, part)
    data_keys = jax.random.split(part_key, 4)
    tok_shape = (BATCH_SEQS, SEQ_LEN, MODEL_DIM)
    row_scale = 0.5 + jax.random.uniform(data_keys[0], (BATCH_SEQS, SEQ_LEN, 1), jnp.float32)
    x_in = (jax.random.normal(data_keys[1], tok_shape, jnp.float32) * row_scale).astype(jnp.bfloat16)
    grad_y = jax.random.normal(data_keys[2], tok_shape, jnp.float32).astype(jnp.bfloat16)
    lengths = jax.random.randint(data_keys[3], (BATCH_SEQS,), SEQ_LEN // 8, SEQ_LEN + 1)
    pad_mask = (jnp.arange(SEQ_LEN)[None, :] < lengths[:, None]).astype(jnp.int32)
    qkv_gain = jnp.array([1.5, 1.5, 1.0], jnp.float32)[:, None, None, None]
    w_qkv = jax.random.normal(weight_keys[0], (3, MODEL_DIM, NUM_HEADS, HEAD_DIM), jnp.float32) * qkv_gain * MODEL_DIM ** -0.5
    w_out = jax.random.normal(weight_keys[1], (NUM_HEADS, HEAD_DIM, MODEL_DIM), jnp.float32) * MODEL_DIM ** -0.5
    w_up = jax.random.normal(weight_keys[2], (MODEL_DIM, FFN_DIM), jnp.float32) * MODEL_DIM ** -0.5
    w_down = jax.random.normal(weight_keys[3], (FFN_DIM, MODEL_DIM), jnp.float32) * FFN_DIM ** -0.5
    return {
        'x_in': x_in,
        'grad_y': grad_y,
        'pad_mask': pad_mask,
        'ln1_gain': 1.0 + 0.2 * jax.random.normal(weight_keys[4], (MODEL_DIM,), jnp.float32),
        'ln1_bias': 0.2 * jax.random.normal(weight_keys[5], (MODEL_DIM,), jnp.float32),
        'w_qkv': w_qkv.astype(jnp.bfloat16),
        'b_qkv': 0.5 * jax.random.normal(weight_keys[6], (3, NUM_HEADS, HEAD_DIM), jnp.float32),
        'w_out': w_out.astype(jnp.bfloat16),
        'b_out': 0.3 * jax.random.normal(weight_keys[7], (MODEL_DIM,), jnp.float32),
        'ln2_gain': 1.0 + 0.2 * jax.random.normal(weight_keys[8], (MODEL_DIM,), jnp.float32),
        'ln2_bias': 0.2 * jax.random.normal(weight_keys[9], (MODEL_DIM,), jnp.float32),
        'w_up': w_up.astype(jnp.bfloat16),
        'b_up': 0.5 * jax.random.normal(weight_keys[10], (FFN_DIM,), jnp.float32),
        'w_down': w_down.astype(jnp.bfloat16),
        'b_down': 0.3 * jax.random.normal(weight_keys[11], (MODEL_DIM,), jnp.float32),
    }


def layer_norm(values, ln_gain, ln_bias):
    centered = values - jnp.mean(values, axis=-1, keepdims=True)
    inv_std = lax.rsqrt(jnp.mean(centered * centered, axis=-1, keepdims=True) + LN_EPS)
    x_hat = centered * inv_std
    return x_hat * ln_gain + ln_bias, x_hat, inv_std


def layer_norm_grad(d_out, x_hat, inv_std, ln_gain):
    d_hat = d_out * ln_gain
    return inv_std * (d_hat - jnp.mean(d_hat, axis=-1, keepdims=True) - x_hat * jnp.mean(d_hat * x_hat, axis=-1, keepdims=True))


def rope_tables():
    inv_freq = ROPE_BASE ** (-2.0 * jnp.arange(HALF_DIM, dtype=jnp.float32) / HEAD_DIM)
    angles = jnp.arange(SEQ_LEN, dtype=jnp.float32)[:, None] * inv_freq[None, :]
    angles = jnp.concatenate([angles, angles], axis=-1)
    return jnp.cos(angles)[:, None, :], jnp.sin(angles)[:, None, :]


def rotate(tensor, cos_tab, sin_tab):
    swapped = jnp.concatenate([-tensor[..., HALF_DIM:], tensor[..., :HALF_DIM]], axis=-1)
    return tensor * cos_tab + swapped * sin_tab


def rotate_back(grad_in, cos_tab, sin_tab):
    scaled = grad_in * sin_tab
    swapped = jnp.concatenate([scaled[..., HALF_DIM:], -scaled[..., :HALF_DIM]], axis=-1)
    return grad_in * cos_tab + swapped


def attention_probs(q_seq, k_seq, key_ok):
    scores = jnp.einsum('qhk,shk->hqs', q_seq.astype(jnp.float32), k_seq.astype(jnp.float32))
    return jax.nn.softmax(jnp.where(key_ok[None, None, :], scores, NEG_LARGE), axis=-1)


def seq_attention(operands):
    q_seq, k_seq, v_seq, key_ok = operands
    probs_low = attention_probs(q_seq, k_seq, key_ok).astype(jnp.bfloat16)
    return jnp.einsum('hqs,shk->qhk', probs_low.astype(jnp.float32), v_seq.astype(jnp.float32)).astype(jnp.bfloat16)


def seq_attention_grad(operands):
    q_seq, k_seq, v_seq, key_ok, d_out = operands
    attn_probs = attention_probs(q_seq, k_seq, key_ok)
    probs_low = attn_probs.astype(jnp.bfloat16).astype(jnp.float32)
    d_out_f = d_out.astype(jnp.float32)
    d_value = jnp.einsum('hqs,qhk->shk', probs_low, d_out_f)
    d_probs = jnp.einsum('qhk,shk->hqs', d_out_f, v_seq.astype(jnp.float32))
    d_scores = attn_probs * (d_probs - jnp.sum(d_probs * attn_probs, axis=-1, keepdims=True))
    d_scores_low = d_scores.astype(jnp.bfloat16).astype(jnp.float32)
    d_query = jnp.einsum('hqs,shk->qhk', d_scores_low, k_seq.astype(jnp.float32))
    d_key = jnp.einsum('hqs,qhk->shk', d_scores_low, q_seq.astype(jnp.float32))
    return d_query, d_key, d_value


def reference(x_in, grad_y, pad_mask, ln1_gain, ln1_bias, w_qkv, b_qkv, w_out, b_out, ln2_gain, ln2_bias, w_up, b_up, w_down, b_down):
    q_scale = HEAD_DIM ** -0.5
    cos_tab, sin_tab = rope_tables()
    key_ok = pad_mask > 0
    x_f = x_in.astype(jnp.float32)
    h1_f, x_hat1, inv_std1 = layer_norm(x_f, ln1_gain, ln1_bias)
    h1_b = h1_f.astype(jnp.bfloat16)
    qkv_all = jnp.einsum('bsd,idhk->ibshk', h1_b.astype(jnp.float32), w_qkv.astype(jnp.float32)) + b_qkv[:, None, None]
    q_rot = rotate(qkv_all[0] * q_scale, cos_tab, sin_tab).astype(jnp.bfloat16)
    k_rot = rotate(qkv_all[1], cos_tab, sin_tab).astype(jnp.bfloat16)
    v_heads = qkv_all[2].astype(jnp.bfloat16)
    attn_o = lax.map(seq_attention, (q_rot, k_rot, v_heads, key_ok))
    attn_sum = jnp.einsum('bshk,hkd->bsd', attn_o.astype(jnp.float32), w_out.astype(jnp.float32)) + b_out
    x1_f = (x_f + attn_sum).astype(jnp.bfloat16).astype(jnp.float32)
    h2_f, x_hat2, inv_std2 = layer_norm(x1_f, ln2_gain, ln2_bias)
    h2_flat = h2_f.astype(jnp.bfloat16).reshape(TOKENS, MODEL_DIM)
    pre_act = jnp.dot(h2_flat, w_up, preferred_element_type=jnp.float32) + b_up
    erf_term = lax.erf(pre_act * INV_SQRT2)
    act_b = (0.5 * pre_act * (1.0 + erf_term)).astype(jnp.bfloat16)
    gelu_slope = 0.5 * (1.0 + erf_term) + pre_act * jnp.exp(-0.5 * pre_act * pre_act) * INV_SQRT_2PI
    mlp_sum = jnp.dot(act_b, w_down, preferred_element_type=jnp.float32) + b_down
    y_out = (x1_f + mlp_sum.reshape(x_f.shape)).astype(jnp.bfloat16)
    dy_flat = grad_y.reshape(TOKENS, MODEL_DIM)
    dy_f = grad_y.astype(jnp.float32)
    grad_b_down = jnp.sum(dy_f, axis=(0, 1))
    grad_w_down = jnp.dot(act_b.T, dy_flat, preferred_element_type=jnp.float32)
    d_act = jnp.dot(dy_flat, w_down.T, preferred_element_type=jnp.float32)
    d_pre = d_act * gelu_slope
    grad_b_up = jnp.sum(d_pre, axis=0)
    d_pre_b = d_pre.astype(jnp.bfloat16)
    grad_w_up = jnp.dot(h2_flat.T, d_pre_b, preferred_element_type=jnp.float32)
    d_h2 = jnp.dot(d_pre_b, w_up.T, preferred_element_type=jnp.float32).reshape(x_f.shape)
    grad_ln2_gain = jnp.sum(d_h2 * x_hat2, axis=(0, 1))
    grad_ln2_bias = jnp.sum(d_h2, axis=(0, 1))
    d_x1 = dy_f + layer_norm_grad(d_h2, x_hat2, inv_std2, ln2_gain)
    grad_b_out = jnp.sum(d_x1, axis=(0, 1))
    d_x1_b = d_x1.astype(jnp.bfloat16).astype(jnp.float32)
    grad_w_out = jnp.einsum('bshk,bsd->hkd', attn_o.astype(jnp.float32), d_x1_b)
    d_attn_o = jnp.einsum('bsd,hkd->bshk', d_x1_b, w_out.astype(jnp.float32)).astype(jnp.bfloat16)
    d_query, d_key, d_value = lax.map(seq_attention_grad, (q_rot, k_rot, v_heads, key_ok, d_attn_o))
    d_qkv = jnp.stack([rotate_back(d_query, cos_tab, sin_tab) * q_scale, rotate_back(d_key, cos_tab, sin_tab), d_value])
    grad_b_qkv = jnp.sum(d_qkv, axis=(1, 2))
    d_qkv_b = d_qkv.astype(jnp.bfloat16).astype(jnp.float32)
    grad_w_qkv = jnp.einsum('bsd,ibshk->idhk', h1_b.astype(jnp.float32), d_qkv_b)
    d_h1 = jnp.einsum('ibshk,idhk->bsd', d_qkv_b, w_qkv.astype(jnp.float32))
    grad_ln1_gain = jnp.sum(d_h1 * x_hat1, axis=(0, 1))
    grad_ln1_bias = jnp.sum(d_h1, axis=(0, 1))
    grad_x = (d_x1 + layer_norm_grad(d_h1, x_hat1, inv_std1, ln1_gain)).astype(jnp.bfloat16)
    return (y_out, grad_x, grad_ln1_gain, grad_ln1_bias, grad_w_qkv, grad_b_qkv, grad_w_out, grad_b_out, grad_ln2_gain, grad_ln2_bias, grad_w_up, grad_b_up, grad_w_down, grad_b_down)
```

```python
import functools

import jax
import jax.numpy as jnp
from jax import lax
from jax.experimental import pallas as pl
from jax.experimental.pallas import tpu as pltpu
from jax.sharding import PartitionSpec as P

f32 = jnp.float32
bf16 = jnp.bfloat16
LN_EPS = 1e-5
ROPE_BASE = 10000.0
INV_SQRT2 = 0.7071067811865476
INV_SQRT_2PI = 0.3989422804014327
NEG_LARGE = -1e30
MESH = pl.DeviceIdType.MESH
ANY = pl.BlockSpec(memory_space=pl.ANY)
VMEM_LIMIT = 66_000_000

TP = 8
NS = 4
S = 512
D = 1024
PW = 128
HD = 64
HH = HD // 2
FB = 512
SL = 64
QS = HD ** -0.5
R3 = 3 * PW


def dg(a, b, ca, cb):
    return lax.dot_general(a, b, (((ca,), (cb,)), ((), ())), preferred_element_type=f32)


def sds(shape, dtype):
    return jax.ShapeDtypeStruct(shape, dtype)


class Place:
    def __init__(self):
        me = lax.axis_index("tp")
        self.me = me
        self.c = lax.rem(me, 2)
        self.dc = 1 - 2 * self.c
        self.dx = 2 - 4 * lax.rem(lax.div(me, 2), 2)
        self.dy = 4 - 8 * lax.div(me, 4)
        self.partner = me + self.dc
        self.a = me + (1 - self.c) * self.dx + self.c * self.dy
        self.b = me + (1 - self.c) * self.dy + self.c * self.dx

    def peer(self, m):
        return self.me + (m & 1) * self.dc + ((m >> 1) & 1) * self.dx + (m >> 2) * self.dy

    def slot_of(self, m):
        k = self.c if m % 2 == 0 else 1 - self.c
        lo, hi = {0: (6, 7), 1: (0, 5), 2: (4, 1), 3: (2, 3)}[m >> 1]
        return lo + k * (hi - lo)


def remote(src, dst, send_sem, recv_sem, device):
    return pltpu.make_async_remote_copy(src_ref=src, dst_ref=dst, send_sem=send_sem, recv_sem=recv_sem,
                                        device_id={"tp": device}, device_id_type=MESH)


def wait_for(ref, sem):
    pltpu.make_async_copy(ref, ref, sem).wait()


def entry_barrier(pc):
    bar = pltpu.get_barrier_semaphore()
    for m in range(1, TP):
        pl.semaphore_signal(bar, inc=1, device_id={"tp": pc.peer(m)}, device_id_type=MESH)
    pl.semaphore_wait(bar, TP - 1)


class AllToAll:
    def __init__(self, pc, pos_ref, seq_ref, send_sem, recv_sem, inward):
        self.pc, self.pos, self.seq, self.ss, self.rs, self.inward = pc, pos_ref, seq_ref, send_sem, recv_sem, inward

    def _rows(self, dev):
        return pl.ds(pl.multiple_of(dev * SL, SL), SL)

    def _seqs(self, dev):
        return pl.ds(dev * NS, NS)

    def _copy(self, m):
        pc, dev = self.pc, self.pc.peer(m)
        if self.inward:
            src, dst = self.pos.at[self._seqs(dev)], self.seq.at[:, self._rows(pc.me)]
        else:
            src, dst = self.seq.at[:, self._rows(dev)], self.pos.at[self._seqs(pc.me)]
        return remote(src, dst, self.ss.at[m], self.rs.at[m], dev)

    def start(self):
        for m in (6, 7, 2, 3, 4, 5, 1):
            self._copy(m).start()

    def local(self, buf):
        pc = self.pc
        a, b = self.pos.at[self._seqs(pc.me)], self.seq.at[:, self._rows(pc.me)]
        src, dst = (a, b) if self.inward else (b, a)
        return pltpu.make_async_copy(src, buf, self.ss.at[0]), pltpu.make_async_copy(buf, dst, self.rs.at[0])

    def finish(self):
        for m in range(1, TP):
            self._copy(m).wait()


class Gather:
    def __init__(self, pc, src_ref, dst_ref, send_sem, recv_sem):
        self.pc, self.src, self.dst, self.ss, self.rs = pc, src_ref, dst_ref, send_sem, recv_sem

    def _send(self, i, src, slot, dev):
        return remote(src, self.dst.at[slot], self.ss.at[i], self.rs.at[slot], dev)

    def _direct(self):
        pc, c = self.pc, self.pc.c
        return [self._send(0, self.src, c, pc.a), self._send(1, self.src, 4 + c, pc.b),
                self._send(2, self.src, 6 + c, pc.partner)]

    def _hop(self):
        pc, c = self.pc, self.pc.c
        return [self._send(3, self.dst.at[c], 2 + c, pc.b), self._send(4, self.dst.at[c], c, pc.partner),
                self._send(5, self.dst.at[4 + c], 4 + c, pc.partner)]

    def _last(self):
        pc, c = self.pc, self.pc.c
        return self._send(6, self.dst.at[2 + c], 2 + c, pc.partner)

    def start(self):
        for cp in self._direct():
            cp.start()

    def forward(self):
        c = self.pc.c
        hop = self._hop()
        wait_for(self.dst.at[c], self.rs.at[c])
        hop[0].start()
        hop[1].start()
        wait_for(self.dst.at[4 + c], self.rs.at[4 + c])
        hop[2].start()

    def last(self):
        c = self.pc.c
        wait_for(self.dst.at[2 + c], self.rs.at[2 + c])
        self._last().start()

    def local(self, buf):
        c = self.pc.c
        return (pltpu.make_async_copy(self.src, buf, self.ss.at[7]),
                pltpu.make_async_copy(buf, self.dst.at[6 + c], self.rs.at[6 + c]))

    def finish(self):
        o = 1 - self.pc.c
        for j in range(4):
            wait_for(self.dst.at[2 * j + o], self.rs.at[2 * j + o])
        for cp in self._direct() + self._hop() + [self._last()]:
            cp.wait_send()


def row_add(acc, others):
    rows = acc.shape[0]
    step = 64

    def body(i, carry):
        r = pl.ds(pl.multiple_of(i * step, step), step)
        v = acc[r, :]
        for o in others:
            v = v + o[r, :]
        acc[r, :] = v
        return carry

    lax.fori_loop(0, rows // step, body, 0)


class ReduceScatter:
    def __init__(self, pc, part, r0, r1, r2, stage, out, sems, bufs, buf_sem):
        self.pc, self.part, self.r0, self.r1, self.r2, self.stage, self.out = pc, part, r0, r1, r2, stage, out
        self.ss, self.rs = sems
        self.rows = part.shape[1]
        self.bufs, self.bs = bufs, buf_sem

    def _pair(self, j):
        pc = self.pc
        return remote(self.part.at[2 * j + 1 - pc.c], self.r0.at[j], self.ss.at[j], self.rs.at[j], pc.partner)

    def _first(self, j):
        pc = self.pc
        return remote(self.stage.at[j], self.r1.at[j], self.ss.at[4 + j], self.rs.at[4 + j], pc.a)

    def _second(self):
        pc = self.pc
        return remote(self.stage.at[2], self.r2, self.ss.at[6], self.rs.at[6], pc.b)

    def start(self):
        for j in range(4):
            self._pair(j).start()

    def _sum(self, j, srcs, dst):
        bufs = [b.at[pl.ds(0, self.rows)] for b in self.bufs[:len(srcs)]]
        cps = [pltpu.make_async_copy(s, b, self.bs.at[i]) for i, (s, b) in enumerate(zip(srcs, bufs))]
        for cp in cps:
            cp.start()
        for cp in cps:
            cp.wait()
        row_add(bufs[0], bufs[1:])
        out = pltpu.make_async_copy(bufs[0], dst, self.bs.at[0])
        out.start()
        out.wait()

    def first(self, j):
        c = self.pc.c
        wait_for(self.r0.at[j], self.rs.at[j])
        self._sum(j, [self.part.at[2 * j + c], self.r0.at[j]], self.stage.at[j])
        self._first(j).start()

    def second(self):
        c = self.pc.c
        wait_for(self.r0.at[2], self.rs.at[2])
        wait_for(self.r1.at[1], self.rs.at[5])
        self._sum(2, [self.part.at[4 + c], self.r0.at[2], self.r1.at[1]], self.stage.at[2])
        self._second().start()

    def last(self):
        c = self.pc.c
        wait_for(self.r0.at[3], self.rs.at[3])
        wait_for(self.r1.at[0], self.rs.at[4])
        wait_for(self.r2, self.rs.at[6])
        self._sum(3, [self.part.at[6 + c], self.r0.at[3], self.r1.at[0], self.r2], self.out)

    def finish(self):
        for j in range(4):
            self._pair(j).wait_send()
        for j in range(2):
            self._first(j).wait_send()
        self._second().wait_send()


def gather_kernel(x_ref, dy_ref, wq, wo, wu, wd, bs, xs_ref, dys_ref, wq_all, wo_all, wu_all, wd_all, bs_all,
                  act_buf, wbufs_q, wbufs_o, wbufs_u, wbufs_d, wbufs_b, a_ss, a_rs, g_ss, g_rs):
    pc = Place()
    entry_barrier(pc)
    a2a = [AllToAll(pc, p, s, a_ss.at[i], a_rs.at[i], True)
           for i, (p, s) in enumerate(((x_ref, xs_ref), (dy_ref, dys_ref)))]
    gathers = [Gather(pc, s, d, g_ss.at[i], g_rs.at[i])
               for i, (s, d) in enumerate(((bs, bs_all), (wq, wq_all), (wo, wo_all), (wu, wu_all), (wd, wd_all)))]
    for g in gathers[:3]:
        g.start()
    a2a[0].start()
    for g in gathers[3:]:
        g.start()
    a2a[1].start()
    local = [a2a[i].local(act_buf.at[i]) for i in range(2)]
    local += [g.local(b) for g, b in zip(gathers, (wbufs_b, wbufs_q, wbufs_o, wbufs_u, wbufs_d))]
    for load, _ in local:
        load.start()
    for load, store in local:
        load.wait()
        store.start()
    for g in gathers:
        g.forward()
    for g in gathers:
        g.last()
    for _, store in local:
        store.wait()
    for g in gathers:
        g.finish()
    for a in a2a:
        a.finish()


def gather_call(x_in, grad_y, wq, wo, wu, wd, bs):
    return pl.pallas_call(
        gather_kernel,
        in_specs=[ANY] * 7,
        out_specs=[ANY] * 7,
        out_shape=[sds((NS, S, D), bf16), sds((NS, S, D), bf16), sds((TP,) + wq.shape, bf16), sds((TP,) + wo.shape, bf16),
                   sds((TP,) + wu.shape, bf16), sds((TP,) + wd.shape, bf16), sds((TP,) + bs.shape, f32)],
        scratch_shapes=[pltpu.VMEM((2, NS, SL, D), bf16), pltpu.VMEM(wq.shape, bf16), pltpu.VMEM(wo.shape, bf16),
                        pltpu.VMEM(wu.shape, bf16), pltpu.VMEM(wd.shape, bf16), pltpu.VMEM(bs.shape, f32),
                        pltpu.SemaphoreType.DMA((2, 8)), pltpu.SemaphoreType.DMA((2, 8)),
                        pltpu.SemaphoreType.DMA((5, 8)), pltpu.SemaphoreType.DMA((5, 8))],
        compiler_params=pltpu.CompilerParams(collective_id=0, has_side_effects=True),
        name="gather_in",
    )(x_in, grad_y, wq, wo, wu, wd, bs)


def ln_stats(v):
    c = v - jnp.mean(v, axis=-1, keepdims=True)
    inv = lax.rsqrt(jnp.mean(c * c, axis=-1, keepdims=True) + LN_EPS)
    return c * inv, inv


def ln_grad(d_out, x_hat, inv, gain):
    dh = d_out * gain
    return inv * (dh - jnp.mean(dh, axis=-1, keepdims=True) - x_hat * jnp.mean(dh * x_hat, axis=-1, keepdims=True))


def masked_scores(q, k, ok):
    return jnp.where(ok, dg(k, q, 0, 0), NEG_LARGE)


def key_mask(mask_ref):
    return jnp.concatenate([mask_ref[0]] * (S // PW), axis=1) > 0


def attn_fwd_kernel(x_ref, mask_ref, cos_ref, sin_ref, g1_ref, b1_ref, wq_ref, bq_ref, wo_ref, bo_ref, g2_ref, b2_ref,
                    qkv_ref, m_ref, l_ref, o_ref, x1_ref, h2_ref, h1_s, o_s):
    g = pl.program_id(1)

    @pl.when(g == 0)
    def _():
        xh, _ = ln_stats(x_ref[0].astype(f32))
        h1_s[...] = (xh * g1_ref[...] + b1_ref[...]).astype(bf16)

    qkv = dg(wq_ref[g], h1_s[...], 1, 1) + bq_ref[g]
    cos, sin = cos_ref[...], sin_ref[...]
    ok = key_mask(mask_ref)

    def rot(t):
        a, b = t[:HH], t[HH:]
        return jnp.concatenate([a * cos - b * sin, b * cos + a * sin], axis=0).astype(bf16)

    for h in range(2):
        r = h * HD
        q = rot(qkv[r:r + HD] * QS)
        k = rot(qkv[PW + r:PW + r + HD])
        v = qkv[2 * PW + r:2 * PW + r + HD].astype(bf16)
        qkv_ref[0, 0, r:r + HD, :] = q
        qkv_ref[0, 0, PW + r:PW + r + HD, :] = k
        qkv_ref[0, 0, 2 * PW + r:2 * PW + r + HD, :] = v
        s = masked_scores(q, k, ok)
        m = jnp.max(s, axis=0, keepdims=True)
        e = jnp.exp(s - m)
        li = 1.0 / jnp.sum(e, axis=0, keepdims=True)
        p = (e * li).astype(bf16)
        m_ref[0, 0, h:h + 1, :] = m
        l_ref[0, 0, h:h + 1, :] = li
        o = dg(v, p, 1, 0).astype(bf16)
        o_ref[0, 0, r:r + HD, :] = o
        o_s[pl.ds(pl.multiple_of(g * PW + r, HD), HD), :] = o

    @pl.when(g == TP - 1)
    def _():
        attn = dg(o_s[...], wo_ref[...], 0, 0)
        x1 = (x_ref[0].astype(f32) + (attn + bo_ref[...])).astype(bf16)
        x1_ref[0] = x1
        xh, _ = ln_stats(x1.astype(f32))
        h2_ref[0] = (xh * g2_ref[...] + b2_ref[...]).astype(bf16)


def whole(shape):
    return pl.BlockSpec(shape, lambda s, g: (0,) * len(shape), pipeline_mode=pl.Buffered(1))


def per_seq(shape):
    return pl.BlockSpec((1,) + shape, lambda s, g: (s,) + (0,) * len(shape))


def per_pair(shape):
    return pl.BlockSpec((1, 1) + shape, lambda s, g: (s, g) + (0,) * len(shape))


def attn_fwd_call(x, mask, cos, sin, g1, b1, wq, bq, wo, bo, g2, b2):
    return pl.pallas_call(
        attn_fwd_kernel,
        grid=(NS, TP),
        in_specs=[per_seq((S, D)), per_seq((S, PW)), whole((HH, S)), whole((HH, S)), whole((1, D)), whole((1, D)),
                  whole((TP, R3, D)), whole((TP, R3, 1)), whole((D, D)), whole((1, D)), whole((1, D)), whole((1, D))],
        out_specs=[per_pair((R3, S)), per_pair((2, S)), per_pair((2, S)), per_pair((PW, S)), per_seq((S, D)), per_seq((S, D))],
        out_shape=[sds((NS, TP, R3, S), bf16), sds((NS, TP, 2, S), f32), sds((NS, TP, 2, S), f32), sds((NS, TP, PW, S), bf16),
                   sds((NS, S, D), bf16), sds((NS, S, D), bf16)],
        scratch_shapes=[pltpu.VMEM((S, D), bf16), pltpu.VMEM((D, S), bf16)],
        compiler_params=pltpu.CompilerParams(dimension_semantics=("arbitrary", "arbitrary"), vmem_limit_bytes=VMEM_LIMIT),
        name="attn_fwd",
    )(x, mask, cos, sin, g1, b1, wq, bq, wo, bo, g2, b2)


def mlp_kernel(h2_ref, dy_ref, x1_ref, wu_ref, wd_ref, bu_ref, bd_ref, y_ref, dh_ref, gd_ref, gu_ref, gb_ref, yacc, dacc):
    i, t = pl.program_id(0), pl.program_id(1)
    rows = pl.ds(pl.multiple_of(t * S, S), S)
    h2, dy = h2_ref[rows, :], dy_ref[rows, :]
    wu, wd = wu_ref[0], wd_ref[0]
    pre = dg(h2, wu, 1, 0) + bu_ref[0]
    d_act = dg(dy, wd, 1, 1)
    cdf = 0.5 * (1.0 + lax.erf(pre * INV_SQRT2))
    act = (pre * cdf).astype(bf16)
    d_pre = d_act * (cdf + pre * jnp.exp(-0.5 * pre * pre) * INV_SQRT_2PI)
    d_pre_b = d_pre.astype(bf16)
    yp = dg(act, wd, 1, 0)
    dp = dg(d_pre_b, wu, 1, 1)
    gd = dg(act, dy, 0, 0)
    gu = dg(d_pre_b, h2, 0, 0)
    gb = jnp.sum(d_pre, axis=0, keepdims=True)

    @pl.when(i == 0)
    def _():
        yacc[rows, :] = yp
        dacc[rows, :] = dp

    @pl.when(i > 0)
    def _():
        yacc[rows, :] += yp
        dacc[rows, :] += dp

    @pl.when(t == 0)
    def _():
        gd_ref[0] = gd
        gu_ref[0] = gu
        gb_ref[0] = gb

    @pl.when(t > 0)
    def _():
        gd_ref[0] += gd
        gu_ref[0] += gu
        gb_ref[0] += gb

    @pl.when(i == TP - 1)
    def _():
        y_ref[...] = (x1_ref[...].astype(f32) + (yacc[rows, :] + bd_ref[...])).astype(bf16)
        dh_ref[...] = dacc[rows, :]


def mlp_call(h2, dy, x1, wu, wd, bu, bd):
    T = NS * S
    res = pl.BlockSpec((T, D), lambda i, t: (0, 0), pipeline_mode=pl.Buffered(1))
    last = pl.BlockSpec((S, D), lambda i, t: (jnp.where(i == TP - 1, t, 0), 0))
    blk = lambda shape: pl.BlockSpec((1,) + shape, lambda i, t: (i, 0, 0))
    return pl.pallas_call(
        mlp_kernel,
        grid=(TP, NS),
        in_specs=[res, res, last, blk((D, FB)), blk((FB, D)), blk((1, FB)), whole((1, D))],
        out_specs=[last, last, blk((FB, D)), blk((FB, D)), blk((1, FB))],
        out_shape=[sds((T, D), bf16), sds((T, D), f32), sds((TP, FB, D), f32), sds((TP, FB, D), f32), sds((TP, 1, FB), f32)],
        scratch_shapes=[pltpu.VMEM((T, D), f32), pltpu.VMEM((T, D), f32)],
        compiler_params=pltpu.CompilerParams(dimension_semantics=("arbitrary", "arbitrary"), vmem_limit_bytes=VMEM_LIMIT),
        name="mlp",
    )(h2, dy, x1, wu, wd, bu, bd)


def attn_bwd_kernel(x_ref, x1_ref, dy_ref, dh2_ref, mask_ref, cos_ref, sin_ref, g1_ref, b1_ref, g2_ref, wq_ref, wo_ref,
                    qkv_ref, m_ref, l_ref, o_ref, gx_ref, gq_ref, go_ref, gbq_ref, vec_ref,
                    h1_s, dx1_s, dx1_b, do_s, dq_s, gq_a, go_a, gb_a, v_a):
    sq, g = pl.program_id(0), pl.program_id(1)

    @pl.when((g == 0) & (sq == 0))
    def _():
        gq_a[...] = jnp.zeros_like(gq_a)
        go_a[...] = jnp.zeros_like(go_a)
        gb_a[...] = jnp.zeros_like(gb_a)
        v_a[...] = jnp.zeros_like(v_a)

    @pl.when(g == 0)
    def _():
        dy, dh2 = dy_ref[0].astype(f32), dh2_ref[0]
        xh2, inv2 = ln_stats(x1_ref[0].astype(f32))
        d = dy + ln_grad(dh2, xh2, inv2, g2_ref[...])
        dx1_s[...] = d
        db = d.astype(bf16)
        dx1_b[...] = db
        v_a[0:1, :] += jnp.sum(dy, axis=0, keepdims=True)
        v_a[1:2, :] += jnp.sum(dh2 * xh2, axis=0, keepdims=True)
        v_a[2:3, :] += jnp.sum(dh2, axis=0, keepdims=True)
        v_a[3:4, :] += jnp.sum(d, axis=0, keepdims=True)
        xh, _ = ln_stats(x_ref[0].astype(f32))
        h1_s[...] = (xh * g1_ref[...] + b1_ref[...]).astype(bf16)
        do_s[...] = dg(wo_ref[...], db, 1, 1).astype(bf16)

    go_a[pl.ds(pl.multiple_of(g * PW, PW), PW), :] += dg(o_ref[0, 0], dx1_b[...], 1, 0)
    cos, sin = cos_ref[...], sin_ref[...]
    ok = key_mask(mask_ref)

    def rot_back(t):
        a, b = t[:HH], t[HH:]
        return jnp.concatenate([a * cos + b * sin, b * cos - a * sin], axis=0)

    base = pl.multiple_of(g * R3, PW)
    for h in range(2):
        r = h * HD
        q = qkv_ref[0, 0, r:r + HD, :]
        k = qkv_ref[0, 0, PW + r:PW + r + HD, :]
        v = qkv_ref[0, 0, 2 * PW + r:2 * PW + r + HD, :]
        do = do_s[pl.ds(pl.multiple_of(g * PW + r, HD), HD), :]
        s = masked_scores(q, k, ok)
        p = jnp.exp(s - m_ref[0, 0, h:h + 1, :]) * l_ref[0, 0, h:h + 1, :]
        dp = dg(v, do, 0, 0)
        ds = (p * (dp - jnp.sum(dp * p, axis=0, keepdims=True))).astype(bf16)
        dv = dg(do, p.astype(bf16), 1, 1)
        dk = rot_back(dg(q, ds, 1, 1))
        dq = rot_back(dg(k, ds, 1, 0)) * QS
        for j, t in enumerate((dq, dk, dv)):
            dq_s[pl.ds(base + j * PW + r, HD), :] = t.astype(bf16)
            gb_a[pl.ds(base + j * PW + r, HD), :] += jnp.sum(t, axis=1, keepdims=True)
    gq_a[g] += dg(dq_s[pl.ds(base, R3), :], h1_s[...], 1, 0)

    @pl.when(g == TP - 1)
    def _():
        dh1 = dg(dq_s[...], wq_ref[...].reshape(TP * R3, D), 0, 0)
        xh, inv = ln_stats(x_ref[0].astype(f32))
        v_a[4:5, :] += jnp.sum(dh1 * xh, axis=0, keepdims=True)
        v_a[5:6, :] += jnp.sum(dh1, axis=0, keepdims=True)
        gx_ref[0] = (dx1_s[...] + ln_grad(dh1, xh, inv, g1_ref[...])).astype(bf16)

    @pl.when(sq == NS - 1)
    def _():
        gq_ref[0] = gq_a[g]
        go_ref[0] = go_a[pl.ds(pl.multiple_of(g * PW, PW), PW), :]
        gbq_ref[0] = gb_a[pl.ds(base, R3), :]
        vec_ref[...] = v_a[...]


def attn_bwd_call(x, x1, dy, dh2, mask, cos, sin, g1, b1, g2, wq, wo, qkv, m, l, o):
    last = lambda shape: pl.BlockSpec((1,) + shape, lambda s, g: (jnp.where(s == NS - 1, g, 0), 0, 0))
    return pl.pallas_call(
        attn_bwd_kernel,
        grid=(NS, TP),
        in_specs=[per_seq((S, D))] * 4 + [per_seq((S, PW)), whole((HH, S)), whole((HH, S)), whole((1, D)), whole((1, D)),
                  whole((1, D)), whole((TP, R3, D)), whole((D, D)), per_pair((R3, S)), per_pair((2, S)), per_pair((2, S)),
                  per_pair((PW, S))],
        out_specs=[per_seq((S, D)), last((R3, D)), last((PW, D)), last((R3, 1)), pl.BlockSpec((8, D), lambda s, g: (0, 0))],
        out_shape=[sds((NS, S, D), bf16), sds((TP, R3, D), f32), sds((TP, PW, D), f32), sds((TP, R3, 1), f32), sds((8, D), f32)],
        scratch_shapes=[pltpu.VMEM((S, D), bf16), pltpu.VMEM((S, D), f32), pltpu.VMEM((S, D), bf16), pltpu.VMEM((D, S), bf16),
                        pltpu.VMEM((TP * R3, S), bf16), pltpu.VMEM((TP, R3, D), f32), pltpu.VMEM((D, D), f32),
                        pltpu.VMEM((TP * R3, 1), f32), pltpu.VMEM((8, D), f32)],
        compiler_params=pltpu.CompilerParams(dimension_semantics=("arbitrary", "arbitrary"), vmem_limit_bytes=VMEM_LIMIT),
        name="attn_bwd",
    )(x, x1, dy, dh2, mask, cos, sin, g1, b1, g2, wq, wo, qkv, m, l, o)


N_RS = 4


def scatter_kernel(y_ref, gx_ref, msg_ref, *refs):
    parts, refs = refs[:N_RS], refs[N_RS:]
    yo_ref, gxo_ref, small_ref, refs = refs[0], refs[1], refs[2], refs[3:]
    outs, refs = refs[:N_RS], refs[N_RS:]
    hbm, refs = refs[:4 * N_RS], refs[4 * N_RS:]
    act_buf, bufs, msgs, buf_sem, a_ss, a_rs, r_ss, r_rs, m_ss, m_rs = refs
    pc = Place()
    entry_barrier(pc)
    rs = [ReduceScatter(pc, parts[i], *hbm[4 * i:4 * i + 4], outs[i], (r_ss.at[i], r_rs.at[i]),
                        [bufs.at[j] for j in range(4)], buf_sem) for i in range(N_RS)]
    a2a = [AllToAll(pc, p, s, a_ss.at[i], a_rs.at[i], False)
           for i, (p, s) in enumerate(((yo_ref, y_ref), (gxo_ref, gx_ref)))]
    for r in rs:
        r.start()
    small = [remote(msg_ref.at[pc.slot_of(m)], msgs.at[pc.me], m_ss.at[m], m_rs.at[m], pc.peer(m)) for m in range(1, TP)]
    for cp in small:
        cp.start()
    own = pltpu.make_async_copy(msg_ref.at[pc.slot_of(0)], msgs.at[pc.me], m_ss.at[0])
    own.start()
    local = [a2a[i].local(act_buf.at[i]) for i in range(2)]
    for load, _ in local:
        load.start()
    for load, store in local:
        load.wait()
        store.start()
    for r in rs:
        r.first(1)
        r.first(0)
    for a in a2a:
        a.start()
    for r in rs:
        r.second()
    for r in rs:
        r.last()
    own.wait()
    for m, cp in enumerate(small):
        cp.wait_send()
        wait_for(msgs.at[pc.peer(m + 1)], m_rs.at[m + 1])
    total = msgs[0]
    for j in range(1, TP):
        total = total + msgs[j]
    small_ref[...] = total
    for _, store in local:
        store.wait()
    for r in rs:
        r.finish()
    for a in a2a:
        a.finish()


def scatter_call(y, gx, msg, parts):
    rows = [p.shape[1] for p in parts]
    hbm = []
    for r in rows:
        hbm += [sds((4, r, D), f32), sds((2, r, D), f32), sds((r, D), f32), sds((3, r, D), f32)]
    out = pl.pallas_call(
        scatter_kernel,
        in_specs=[ANY] * (3 + N_RS),
        out_specs=[ANY, ANY, pl.BlockSpec(memory_space=pltpu.VMEM)] + [ANY] * (N_RS + len(hbm)),
        out_shape=[sds((TP * NS, SL, D), bf16), sds((TP * NS, SL, D), bf16), sds((8, D), f32)]
        + [sds((r, D), f32) for r in rows] + hbm,
        scratch_shapes=[pltpu.VMEM((2, NS, SL, D), bf16), pltpu.VMEM((4, max(rows), D), f32), pltpu.VMEM((TP, 8, D), f32),
                        pltpu.SemaphoreType.DMA((4,)), pltpu.SemaphoreType.DMA((2, 8)), pltpu.SemaphoreType.DMA((2, 8)),
                        pltpu.SemaphoreType.DMA((N_RS, 7)), pltpu.SemaphoreType.DMA((N_RS, 7)),
                        pltpu.SemaphoreType.DMA((8,)), pltpu.SemaphoreType.DMA((8,))],
        compiler_params=pltpu.CompilerParams(collective_id=1, has_side_effects=True, vmem_limit_bytes=VMEM_LIMIT),
        name="scatter_out",
    )(y, gx, msg, *parts)
    return out[0], out[1], out[2], out[3:3 + N_RS]


def rope_tables():
    inv_freq = ROPE_BASE ** (-2.0 * jnp.arange(HH, dtype=f32) / HD)
    angles = jnp.arange(S, dtype=f32)[:, None] * inv_freq[None, :]
    return jnp.cos(angles).T, jnp.sin(angles).T


def solution(mesh):
    act_spec = P('dp', 'tp', None)
    rep_vec = P(None)
    part_vec = P('dp')
    in_specs = (act_spec, act_spec, P('dp', None), rep_vec, rep_vec, P(None, None, 'tp', None), P(None, 'tp', None),
                P('tp', None, None), rep_vec, rep_vec, rep_vec, P(None, 'tp'), P('tp'), P('tp', None), rep_vec)
    out_specs = (act_spec, act_spec, part_vec, part_vec, P('dp', None, 'tp', None), P('dp', 'tp', None),
                 P(('dp', 'tp'), None, None), part_vec, part_vec, part_vec, P('dp', 'tp'), P(('dp', 'tp')),
                 P(('dp', 'tp'), None), part_vec)

    def device_step(x_in, grad_y, pad_mask, ln1_gain, ln1_bias, w_qkv, b_qkv, w_out, b_out, ln2_gain, ln2_bias, w_up, b_up, w_down, b_down):
        assert x_in.shape == (TP * NS, SL, D) and w_qkv.shape == (3, D, 2, HD) and w_up.shape == (D, FB)
        me = lax.axis_index('tp')
        row = lambda v: v.reshape(1, D)
        wq = w_qkv.transpose(0, 2, 3, 1).reshape(R3, D)
        wo = w_out.reshape(PW, D)
        bs = jnp.concatenate([b_qkv.reshape(R3), b_up, jnp.zeros((8 * 128 - R3 - FB,), f32)]).reshape(8, 128)
        x, dy, wq, wo, wu, wd, bs = gather_call(x_in, grad_y, wq, wo, w_up, w_down, bs)
        bs = bs.reshape(TP, 8 * 128)
        bq = bs[:, :R3, None]
        bu = bs[:, None, R3:R3 + FB]
        mask = lax.dynamic_slice_in_dim(pad_mask, me * NS, NS, 0)
        mask = jnp.broadcast_to(mask[:, :, None], (NS, S, PW))
        cos, sin = rope_tables()
        wo2 = wo.reshape(TP * PW, D)
        qkv, m, l, o, x1, h2 = attn_fwd_call(x, mask, cos, sin, row(ln1_gain), row(ln1_bias), wq, bq, wo2, row(b_out),
                                             row(ln2_gain), row(ln2_bias))
        flat = lambda t: t.reshape(NS * S, D)
        y, dh2, gd, gu, gbu = mlp_call(flat(h2), flat(dy), flat(x1), wu, wd, bu, row(b_down))
        gx, gq, go, gbq, vec = attn_bwd_call(x, x1, dy, dh2.reshape(NS, S, D), mask, cos, sin, row(ln1_gain), row(ln1_bias),
                                             row(ln2_gain), wq, wo2, qkv, m, l, o)
        msg = jnp.concatenate([jnp.broadcast_to(vec[:6], (TP, 6, D)),
                               jnp.concatenate([gbq.reshape(TP, R3), gbu.reshape(TP, FB), jnp.zeros((TP, D - R3 - FB), f32)],
                                               axis=1)[:, None, :], jnp.zeros((TP, 1, D), f32)], axis=1)
        y_out, grad_x, small, (gd, gu, gq, go) = scatter_call(y.reshape(NS, S, D), gx, msg, [gd, gu, gq, go])
        return (y_out, grad_x, small[4], small[5], gq.reshape(3, 2, HD, D).transpose(0, 3, 1, 2), small[6, :R3].reshape(3, 2, HD),
                go.reshape(2, HD, D), small[3], small[1], small[2], gu.T, small[6, R3:R3 + FB], gd, small[0])

    return jax.shard_map(device_step, mesh=mesh, in_specs=in_specs, out_specs=out_specs, check_vma=False)
```

```python
import jax
import jax.numpy as jnp
import numpy as np
from jax import lax
from jax.experimental import pallas as pl
from jax.experimental.pallas import tpu as pltpu
from jax.sharding import PartitionSpec as P

f32 = jnp.float32
bf16 = jnp.bfloat16
LN_EPS = 1e-5
ROPE_BASE = 10000.0
INV_SQRT2 = 0.7071067811865476
INV_SQRT_2PI = 0.3989422804014327
NEG_LARGE = -1e30
MESH = pl.DeviceIdType.MESH
ANY = pl.BlockSpec(memory_space=pl.ANY)
VMEM_LIMIT = 66_000_000

TP = 8
NS = 4
S = 512
D = 1024
PW = 128
HD = 64
HH = HD // 2
FB = 512
SL = 64
QS = HD ** -0.5
R3 = 3 * PW


def dg(a, b, ca, cb):
    return lax.dot_general(a, b, (((ca,), (cb,)), ((), ())), preferred_element_type=f32)


def nn(a, b):
    return dg(a, b, 1, 0)


def nt(a, b):
    return dg(a, b, 1, 1)


def tn(a, b):
    return dg(a, b, 0, 0)


def over_rows(reduce, v):
    return reduce(v, axis=0, keepdims=True)


def over_cols(reduce, v):
    return reduce(v, axis=1, keepdims=True)


def sds(shape, dtype):
    return jax.ShapeDtypeStruct(shape, dtype)


class Place:
    def __init__(self):
        me = lax.axis_index("tp")
        self.me = me
        self.c = lax.rem(me, 2)
        self.dc = 1 - 2 * self.c
        self.dx = 2 - 4 * lax.rem(lax.div(me, 2), 2)
        self.dy = 4 - 8 * lax.div(me, 4)
        self.partner = me + self.dc
        self.a = me + (1 - self.c) * self.dx + self.c * self.dy
        self.b = me + (1 - self.c) * self.dy + self.c * self.dx

    def peer(self, m):
        return self.me + (m & 1) * self.dc + ((m >> 1) & 1) * self.dx + (m >> 2) * self.dy

    def slot_of(self, m):
        k = self.c if m % 2 == 0 else 1 - self.c
        lo, hi = {0: (6, 7), 1: (0, 5), 2: (4, 1), 3: (2, 3)}[m >> 1]
        return lo + k * (hi - lo)


def remote(src, dst, send_sem, recv_sem, device):
    return pltpu.make_async_remote_copy(src_ref=src, dst_ref=dst, send_sem=send_sem, recv_sem=recv_sem,
                                        device_id={"tp": device}, device_id_type=MESH)


def wait_for(ref, sem):
    pltpu.make_async_copy(ref, ref, sem).wait()


def entry_barrier(pc):
    bar = pltpu.get_barrier_semaphore()
    for m in range(1, TP):
        pl.semaphore_signal(bar, inc=1, device_id={"tp": pc.peer(m)}, device_id_type=MESH)
    pl.semaphore_wait(bar, TP - 1)


class AllToAll:
    def __init__(self, pc, pos_ref, seq_ref, send_sem, recv_sem, inward):
        self.pc, self.pos, self.seq, self.ss, self.rs, self.inward = pc, pos_ref, seq_ref, send_sem, recv_sem, inward

    def _rows(self, dev):
        return pl.ds(pl.multiple_of(dev * SL, SL), SL)

    def _copy(self, s, m):
        pc, dev = self.pc, self.pc.peer(m)
        if self.inward:
            src, dst = self.pos.at[dev * NS + s], self.seq.at[s, self._rows(pc.me)]
        else:
            src, dst = self.seq.at[s, self._rows(dev)], self.pos.at[pc.me * NS + s]
        return remote(src, dst, self.ss.at[s, m], self.rs.at[s, m], dev)

    def start(self, s):
        for m in (2, 3, 4, 5, 6, 7, 1):
            self._copy(s, m).start()

    def finish(self, s):
        for m in range(1, TP):
            self._copy(s, m).wait()

    def local_in(self, buf):
        pc = self.pc
        return (pltpu.make_async_copy(self.pos.at[pl.ds(pc.me * NS, NS)], buf, self.ss.at[0, 0]),
                pltpu.make_async_copy(buf, self.seq.at[:, self._rows(pc.me)], self.rs.at[0, 0]))

    def local_out(self, s, src):
        return pltpu.make_async_copy(src.at[s, self._rows(self.pc.me)], self.pos.at[self.pc.me * NS + s], self.ss.at[s, 0])


class Gather:
    def __init__(self, pc, src_ref, dst_ref, send_sem, recv_sem):
        self.pc, self.src, self.dst, self.ss, self.rs = pc, src_ref, dst_ref, send_sem, recv_sem

    def _send(self, i, src, slot, dev):
        return remote(src, self.dst.at[slot], self.ss.at[i], self.rs.at[slot], dev)

    def _direct(self):
        pc, c = self.pc, self.pc.c
        return [self._send(0, self.src, c, pc.a), self._send(2, self.src, 6 + c, pc.partner),
                self._send(1, self.src, 4 + c, pc.b)]

    def _hop(self):
        pc, c = self.pc, self.pc.c
        return [self._send(3, self.dst.at[c], 2 + c, pc.b), self._send(4, self.dst.at[c], c, pc.partner),
                self._send(5, self.dst.at[4 + c], 4 + c, pc.partner)]

    def _last(self):
        pc, c = self.pc, self.pc.c
        return self._send(6, self.dst.at[2 + c], 2 + c, pc.partner)

    def arrived(self, slot):
        wait_for(self.dst.at[slot], self.rs.at[slot])

    def start(self):
        self.start_a()
        self.start_b()

    def start_a(self):
        for cp in self._direct()[:2]:
            cp.start()

    def start_b(self):
        self._direct()[2].start()

    def forward(self):
        self.forward_a()
        self.forward_b()

    def forward_a(self):
        hop = self._hop()
        self.arrived(self.pc.c)
        hop[0].start()
        hop[1].start()

    def forward_b(self):
        self.arrived(4 + self.pc.c)
        self._hop()[2].start()

    def last(self):
        self.arrived(2 + self.pc.c)
        self._last().start()

    def local(self, buf):
        return (pltpu.make_async_copy(self.src, buf, self.ss.at[7]),
                pltpu.make_async_copy(buf, self.dst.at[6 + self.pc.c], self.rs.at[6 + self.pc.c]))

    def arrived_rest(self):
        for j in range(4):
            self.arrived(2 * j + 1 - self.pc.c)
        self.arrived(6 + self.pc.c)

    def sent(self):
        for cp in self._direct() + self._hop() + [self._last()]:
            cp.wait_send()


def row_add(acc, others):
    step = 64

    def body(i, carry):
        r = pl.ds(pl.multiple_of(i * step, step), step)
        v = acc[r, :]
        for o in others:
            v = v + o[r, :]
        acc[r, :] = v
        return carry

    lax.fori_loop(0, acc.shape[0] // step, body, 0)


class GradScatter:
    def __init__(self, pc, acc, landing, stage, r1, r2, sems, free):
        self.pc, self.acc, self.landing, self.stage, self.r1, self.r2 = pc, acc, landing, stage, r1, r2
        self.sem, self.free = sems, free

    def _pair(self, b):
        return remote(self.acc.at[b], self.landing, self.sem.at[0], self.sem.at[1], self.pc.partner)

    def _first(self, j):
        return remote(self.stage.at[j], self.r1.at[j], self.sem.at[2 + j], self.sem.at[4 + j], self.pc.a)

    def _second(self):
        return remote(self.stage.at[2], self.r2, self.sem.at[6], self.sem.at[7], self.pc.b)

    def block_done(self, slot, b, needs_credit):
        @pl.when(lax.rem(slot, 2) != self.pc.c)
        def _():
            @pl.when(needs_credit)
            def _():
                pl.semaphore_wait(self.free, 1)

            self._pair(b).start()

    def settle(self, slot, b, gives_credit):
        c = self.pc.c
        own = lax.rem(slot, 2) == c
        j = lax.div(slot, 2)

        @pl.when(own)
        def _():
            wait_for(self.landing, self.sem.at[1])
            row_add(self.acc.at[b], [self.landing])

            @pl.when(gives_credit)
            def _():
                pl.semaphore_signal(self.free, inc=1, device_id={"tp": self.pc.partner}, device_id_type=MESH)

            store = pltpu.make_async_copy(self.acc.at[b], self.stage.at[j], self.sem.at[8])
            store.start()
            store.wait()

            @pl.when(j < 2)
            def _():
                self._first(j).start()

        @pl.when(jnp.logical_not(own))
        def _():
            self._pair(b).wait_send()

    def second(self, bufs, chunk_sem):
        n = chunk_sem.shape[1]
        size = bufs[0].shape[0]
        rows = size // n
        part = lambda ref, k: ref.at[pl.ds(k * rows, rows)]
        wait_for(self.r1.at[1], self.sem.at[5])
        for p in range(self.r2.shape[0] // size):
            mine, theirs = (ref.at[pl.ds(p * size, size)] for ref in (self.stage.at[2], self.r1.at[1]))
            loads = [[pltpu.make_async_copy(part(src, k), part(buf, k), chunk_sem.at[x, k])
                      for x, (src, buf) in enumerate(zip((mine, theirs), bufs))] for k in range(n)]
            stores = [pltpu.make_async_copy(part(bufs[0], k), part(mine, k), chunk_sem.at[2, k]) for k in range(n)]
            for group in loads:
                for cp in group:
                    cp.start()
            for k in range(n):
                for cp in loads[k]:
                    cp.wait()
                row_add(part(bufs[0], k), [part(bufs[1], k)])
                stores[k].start()
            for cp in stores:
                cp.wait()
        self._second().start()

    def finish(self):
        wait_for(self.r1.at[0], self.sem.at[4])
        for j in range(2):
            self._first(j).wait_send()
        self._second().wait()


def ln_stats(v):
    c = v - over_cols(jnp.mean, v)
    inv = lax.rsqrt(over_cols(jnp.mean, c * c) + LN_EPS)
    return c * inv, inv


def ln_grad(d_out, x_hat, inv, gain):
    dh = d_out * gain
    return inv * (dh - over_cols(jnp.mean, dh) - x_hat * over_cols(jnp.mean, dh * x_hat))


def masked_scores(q, k, ok):
    return jnp.where(ok, tn(k, q), NEG_LARGE)


def key_mask(mask):
    return jnp.concatenate([mask] * (S // PW), axis=1) > 0


def column(row):
    return jnp.broadcast_to(row, (128, row.shape[1])).T[:, :1]


def load_all(pairs, sem):
    cps = [pltpu.make_async_copy(s, d, sem.at[i]) for i, (s, d) in enumerate(pairs)]
    for cp in cps:
        cp.start()
    return cps


def vm(*shape, dtype=f32):
    return pltpu.VMEM(shape, dtype)


TT = 1024
NT = NS * S // TT
IN_NAMES = ("x_in", "dy_in", "wq", "wo", "wu", "wd", "bqkv", "bup", "pad", "cos", "sin", "gain1", "bias1", "gain2", "bias2",
            "b_out", "b_down")
OUT_SHAPES = {
    "y_out": ((TP * NS, SL, D), bf16), "gx_out": ((TP * NS, SL, D), bf16), "small": ((8, D), f32), "gd": ((FB, D), f32), "gu": ((D, FB), f32),
    "a_stage": ((4, R3 + PW, D), f32), "a_r1": ((2, R3 + PW, D), f32), "a_r2": ((R3 + PW, D), f32),
    "m_stage": ((4, 2 * FB, D), f32), "m_r1": ((2, 2 * FB, D), f32), "m_r2": ((2 * FB, D), f32),
    "xs": ((NS, S, D), bf16), "dys": ((NS, S, D), bf16), "wq_all": ((TP, R3, D), bf16), "wo_all": ((TP, PW, D), bf16),
    "wu_all": ((TP, D, FB), bf16), "wd_all": ((TP, FB, D), bf16),
    "qkv": ((NS, TP, R3, S), bf16), "ml": ((NS, TP, 4, S), f32), "o": ((NS, TP, PW, S), bf16),
    "x1": ((NS, S, D), bf16), "h2": ((NS, S, D), bf16), "y_seq": ((NS, S, D), bf16),
}
DMA = pltpu.SemaphoreType.DMA
SCRATCH = {
    "bs_all": vm(TP, 8, 128), "bs": vm(8, 128), "mask": vm(NS, S, PW), "dacc": vm(NS * S, D), "landing": vm(2 * FB, D), "gbu": vm(TP, 1, FB), "va": vm(8, D),
    "msg": vm(TP, 8, D), "msgs": vm(TP, 8, D),
    "free": pltpu.SemaphoreType.REGULAR,
    "x_ss": DMA((NS, 8)), "x_rs": DMA((NS, 8)), "dy_ss": DMA((NS, 8)), "dy_rs": DMA((NS, 8)),
    "y_ss": DMA((NS, 8)), "y_rs": DMA((NS, 8)), "gx_ss": DMA((NS, 8)), "gx_rs": DMA((NS, 8)),
    "g_ss": DMA((5, 8)), "g_rs": DMA((5, 8)), "m_sem": DMA((9,)), "a_sem": DMA((9,)), "s_ss": DMA((8,)), "s_rs": DMA((8,)),
    "tmp": DMA((8,)), "chunk": DMA((3, 4)), "w_sem": DMA((2, 2)),
}


class Refs:
    def __init__(self, names, refs):
        for n, r in zip(names, refs):
            setattr(self, n, r)


def layer_kernel(*refs):
    r = Refs(IN_NAMES + tuple(OUT_SHAPES) + tuple(SCRATCH), refs)
    pc = Place()
    for i in range(3):
        for h in range(2):
            r.bs[i:i + 1, h * HD:(h + 1) * HD] = r.bqkv[i, h:h + 1, :]
    for k in range(4):
        r.bs[4 + k:5 + k, :] = r.bup[:, k * 128:(k + 1) * 128]
    entry_barrier(pc)
    x_a2a = AllToAll(pc, r.x_in, r.xs, r.x_ss, r.x_rs, True)
    dy_a2a = AllToAll(pc, r.dy_in, r.dys, r.dy_ss, r.dy_rs, True)
    y_a2a = AllToAll(pc, r.y_out, r.y_seq, r.y_ss, r.y_rs, False)
    g_bs, g_wq, g_wo, g_wu, g_wd = [
        Gather(pc, s, d, r.g_ss.at[i], r.g_rs.at[i])
        for i, (s, d) in enumerate(((r.bs, r.bs_all), (r.wq, r.wq_all), (r.wo, r.wo_all), (r.wu, r.wu_all), (r.wd, r.wd_all)))]
    gain1, bias1, gain2, bias2, b_out, b_down = r.gain1, r.bias1, r.gain2, r.bias2, r.b_out, r.b_down

    def arrivals(b_x, b_dy, b_q, b_o, b_u, b_d):
        first = (g_bs, g_wq, g_wo)
        for g in first:
            g.start()
        x_a2a.start(0)
        own_bs = pltpu.make_async_copy(r.bs, r.bs_all.at[6 + pc.c], r.g_rs.at[0, 6 + pc.c])
        own_bs.start()
        local = [x_a2a.local_in(b_x), dy_a2a.local_in(b_dy)]
        local += [g.local(b) for g, b in ((g_wq, b_q), (g_wo, b_o), (g_wu, b_u), (g_wd, b_d))]
        for load, _ in local:
            load.start()
        for s in range(NS):
            keys = jnp.broadcast_to(r.pad[pl.ds(pc.me * NS + s, 1), :].astype(f32), (PW, S))
            r.mask[s] = keys.T
        for load, store in local:
            load.wait()
            store.start()
        for g in first:
            g.forward_a()
        for g in first:
            g.forward_b()
        x_a2a.finish(0)
        x_a2a.start(1)
        for g in first:
            g.last()
        for s in range(2, NS):
            x_a2a.start(s)
        for s in range(NS):
            dy_a2a.start(s)
        g_wu.start_a()
        g_wd.start_a()
        for g in first:
            g.arrived_rest()
        for g in (g_wu, g_wd):
            g.arrived(6 + pc.c)
        local[0][1].wait()
        local[1][1].wait()

    act = vm(NS, SL, D, dtype=bf16)
    pl.run_scoped(arrivals, act, act, vm(R3, D, dtype=bf16), vm(PW, D, dtype=bf16), vm(D, FB, dtype=bf16), vm(FB, D, dtype=bf16))

    def attn_fwd(wq_v, wo_v, h1_s, o_s):
        cps = load_all([(r.wq_all, wq_v), (r.wo_all, wo_v)], r.tmp)
        for cp in cps:
            cp.wait()

        def body(x_ref, qkv_ref, ml_ref, o_ref, x1_ref, h2_ref):
            s, g = pl.program_id(0), pl.program_id(1)

            @pl.when(g == 0)
            def _():
                xh, _ = ln_stats(x_ref[0].astype(f32))
                h1_s[...] = (xh * gain1[...] + bias1[...]).astype(bf16)

            bias = r.bs_all[g]
            bias = jnp.concatenate([column(bias[i:i + 1]) for i in range(3)], axis=0)
            qkv = nt(wq_v[g], h1_s[...]) + bias
            cos, sin = r.cos[...], r.sin[...]
            ok = key_mask(r.mask[s])

            def rot(t):
                a, b = t[:HH], t[HH:]
                return jnp.concatenate([a * cos - b * sin, b * cos + a * sin], axis=0).astype(bf16)

            for h in range(2):
                lo = h * HD
                q = rot(qkv[lo:lo + HD] * QS)
                k = rot(qkv[PW + lo:PW + lo + HD])
                v = qkv[2 * PW + lo:2 * PW + lo + HD].astype(bf16)
                qkv_ref[0, 0, lo:lo + HD, :] = q
                qkv_ref[0, 0, PW + lo:PW + lo + HD, :] = k
                qkv_ref[0, 0, 2 * PW + lo:2 * PW + lo + HD, :] = v
                sc = masked_scores(q, k, ok)
                m = over_rows(jnp.max, sc)
                e = jnp.exp(sc - m)
                li = 1.0 / over_rows(jnp.sum, e)
                p = (e * li).astype(bf16)
                ml_ref[0, 0, h:h + 1, :] = m
                ml_ref[0, 0, 2 + h:3 + h, :] = li
                o = nn(v, p).astype(bf16)
                o_ref[0, 0, lo:lo + HD, :] = o
                o_s[pl.ds(pl.multiple_of(g * PW + lo, HD), HD), :] = o

            @pl.when(g == TP - 1)
            def _():
                attn = tn(o_s[...], wo_v[...].reshape(TP * PW, D))
                x1 = (x_ref[0].astype(f32) + (attn + b_out[...])).astype(bf16)
                x1_ref[0] = x1
                xh, _ = ln_stats(x1.astype(f32))
                h2_ref[0] = (xh * gain2[...] + bias2[...]).astype(bf16)

            for k in range(1, NS):
                @pl.when((s == k - 1) & (g == TP - 2))
                def _():
                    x_a2a.finish(k)

        seq = pl.BlockSpec((1, S, D), lambda s, g: (s, 0, 0))
        pair = lambda n: pl.BlockSpec((1, 1, n, S), lambda s, g: (s, g, 0, 0))
        pltpu.emit_pipeline(body, grid=(NS, TP), in_specs=[seq], out_specs=[pair(R3), pair(4), pair(PW), seq, seq])(
            r.xs, r.qkv, r.ml, r.o, r.x1, r.h2)

    pl.run_scoped(attn_fwd, vm(TP, R3, D, dtype=bf16), vm(TP, PW, D, dtype=bf16), vm(S, D, dtype=bf16), vm(D, S, dtype=bf16))

    def mlp(h2_v, dy_v, yacc, wu_v, wd_v, acc):
        rs = GradScatter(pc, acc, r.landing, r.m_stage, r.m_r1, r.m_r2, r.m_sem, r.free)
        slot_at = lambda i: lax.rem(i + 6, TP)
        cps = load_all([(r.h2.at[s], h2_v.at[pl.ds(s * S, S)]) for s in range(NS)], r.tmp)
        for s in range(NS):
            dy_a2a.finish(s)
        cps += [pltpu.make_async_copy(r.dys.at[s], dy_v.at[pl.ds(s * S, S)], r.tmp.at[NS + s]) for s in range(NS)]
        for cp in cps[NS:]:
            cp.start()

        def weights(slot, b):
            return (pltpu.make_async_copy(r.wu_all.at[slot], wu_v.at[b], r.w_sem.at[0, b]),
                    pltpu.make_async_copy(r.wd_all.at[slot], wd_v.at[b], r.w_sem.at[1, b]))

        def fetch(i):
            slot = slot_at(i)

            @pl.when(lax.rem(slot, 2) != pc.c)
            def _():
                g_wu.arrived(slot)
                g_wd.arrived(slot)

            for cp in weights(slot, lax.rem(i, 2)):
                cp.start()

        fetch(jnp.int32(0))
        for cp in cps:
            cp.wait()

        def step(n, carry):
            i, t = lax.div(n, NT), lax.rem(n, NT)
            b = lax.rem(i, 2)
            slot = slot_at(i)

            @pl.when(t == 0)
            def _():
                for cp in weights(slot, b):
                    cp.wait()

            @pl.when((t == NT - 1) & (i < TP - 1))
            def _():
                fetch(i + 1)

            rows = pl.ds(pl.multiple_of(t * TT, TT), TT)
            h2, dy = h2_v[rows, :], dy_v[rows, :]
            wu, wd = wu_v[b], wd_v[b]
            bias = r.bs_all[slot]
            bias = jnp.concatenate([bias[4 + k:5 + k] for k in range(FB // 128)], axis=1)
            pre = nn(h2, wu) + bias
            d_act = nt(dy, wd)
            cdf = 0.5 * (1.0 + lax.erf(pre * INV_SQRT2))
            act = (pre * cdf).astype(bf16)
            d_pre = d_act * (cdf + pre * jnp.exp(-0.5 * pre * pre) * INV_SQRT_2PI)
            d_pre_b = d_pre.astype(bf16)
            yp = nn(act, wd)
            dp = nt(d_pre_b, wu)
            gd = tn(act, dy)
            gu = tn(d_pre_b, h2)
            gb = over_rows(jnp.sum, d_pre)

            @pl.when(i == 0)
            def _():
                yacc[rows, :] = yp
                r.dacc[rows, :] = dp

            @pl.when(i > 0)
            def _():
                yacc[rows, :] += yp
                r.dacc[rows, :] += dp

            @pl.when(t == 0)
            def _():
                acc[b, 0:FB, :] = gd
                acc[b, FB:2 * FB, :] = gu
                r.gbu[slot] = gb

            @pl.when(t > 0)
            def _():
                acc[b, 0:FB, :] += gd
                acc[b, FB:2 * FB, :] += gu
                r.gbu[slot] += gb

            @pl.when(t == NT - 1)
            def _():
                rs.block_done(slot, b, i >= 2)

            @pl.when((t == 0) & (i > 0))
            def _():
                rs.settle(slot_at(i - 1), 1 - b, True)

            for when, hops in ((2, ("forward_a", "start_b")), (5, ("last",)), (9, ("forward_b",))):
                @pl.when(n == when)
                def _():
                    for hop in hops:
                        for gather in (g_wu, g_wd):
                            getattr(gather, hop)()

            return carry

        lax.fori_loop(0, TP * NT, step, 0)
        cps = load_all([(r.x1.at[s], h2_v.at[pl.ds(s * S, S)]) for s in range(NS)], r.tmp)
        stores = []
        for s in range(NS):
            rows = pl.ds(s * S, S)
            cps[s].wait()
            dy_v[rows, :] = (h2_v[rows, :].astype(f32) + (yacc[rows, :] + b_down[...])).astype(bf16)
            cp = pltpu.make_async_copy(dy_v.at[rows], r.y_seq.at[s], r.tmp.at[NS + s])
            cp.start()
            stores.append(cp)
        for s in range(NS):
            stores[s].wait()
            y_a2a.start(s)
        last = jnp.int32(TP - 1)
        rs.settle(slot_at(last), lax.rem(last, 2), True)

    tok = vm(NS * S, D, dtype=bf16)
    pl.run_scoped(mlp, tok, tok, vm(NS * S, D), vm(2, D, FB, dtype=bf16), vm(2, FB, D, dtype=bf16), vm(2, 2 * FB, D))

    rs_m = GradScatter(pc, None, None, r.m_stage, r.m_r1, r.m_r2, r.m_sem, r.free)
    rs_a = GradScatter(pc, None, None, r.a_stage, r.a_r1, r.a_r2, r.a_sem, r.free)

    def attn_bwd(h1_s, do_s, go_a, gb_a):
        gx_a2a = AllToAll(pc, r.gx_out, h1_s, r.gx_ss, r.gx_rs, False)

        def open_bwd(wo_v):
            wo_cp = pltpu.make_async_copy(r.wo_all, wo_v, r.tmp.at[0])
            wo_cp.start()
            wo_cp.wait()
            r.va[...] = jnp.zeros_like(r.va)

            def body(x_ref, x1_ref, dy_ref, o_ref):
                s = pl.program_id(0)
                rows = pl.ds(pl.multiple_of(s * S, S), S)
                dy, dh2 = dy_ref[0].astype(f32), r.dacc[rows, :]
                xh2, inv2 = ln_stats(x1_ref[0].astype(f32))
                d = dy + ln_grad(dh2, xh2, inv2, gain2[...])
                r.dacc[rows, :] = d
                db = d.astype(bf16)
                r.va[0:1, :] += over_rows(jnp.sum, dy)
                r.va[1:2, :] += over_rows(jnp.sum, dh2 * xh2)
                r.va[2:3, :] += over_rows(jnp.sum, dh2)
                r.va[3:4, :] += over_rows(jnp.sum, d)
                xh, _ = ln_stats(x_ref[0].astype(f32))
                h1_s[s] = (xh * gain1[...] + bias1[...]).astype(bf16)
                do_s[s] = nt(wo_v[...].reshape(TP * PW, D), db).astype(bf16)
                go = nn(o_ref[0].reshape(TP * PW, S), db)

                @pl.when(s == 0)
                def _():
                    go_a[...] = go

                @pl.when(s > 0)
                def _():
                    go_a[...] += go

            seq = pl.BlockSpec((1, S, D), lambda s: (s, 0, 0))
            pltpu.emit_pipeline(body, grid=(NS,), in_specs=[seq, seq, seq, pl.BlockSpec((1, TP, PW, S), lambda s: (s, 0, 0, 0))])(
                r.xs, r.x1, r.dys, r.o)

        pl.run_scoped(open_bwd, vm(TP, PW, D, dtype=bf16))
        def heads(dq_s, wq_v):
            wq_cp = pltpu.make_async_copy(r.wq_all, wq_v, r.tmp.at[1])
            wq_cp.start()

            def pairs(acc, buf):
                rs = GradScatter(pc, acc, r.landing.at[pl.ds(0, R3 + PW)], r.a_stage, r.a_r1, r.a_r2, r.a_sem, r.free)

                def body(qkv_ref, ml_ref):
                    g, s = pl.program_id(0), pl.program_id(1)
                    b = lax.rem(g, 2)
                    cos, sin = r.cos[...], r.sin[...]
                    ok = key_mask(r.mask[s])

                    def rot_back(t):
                        a, b = t[:HH], t[HH:]
                        return jnp.concatenate([a * cos + b * sin, b * cos - a * sin], axis=0)

                    base = pl.multiple_of(g * R3, PW)
                    for h in range(2):
                        lo = h * HD
                        q = qkv_ref[0, 0, lo:lo + HD, :]
                        k = qkv_ref[0, 0, PW + lo:PW + lo + HD, :]
                        v = qkv_ref[0, 0, 2 * PW + lo:2 * PW + lo + HD, :]
                        do = do_s[s, pl.ds(pl.multiple_of(g * PW + lo, HD), HD), :]
                        sc = masked_scores(q, k, ok)
                        p = jnp.exp(sc - ml_ref[0, 0, h:h + 1, :]) * ml_ref[0, 0, 2 + h:3 + h, :]
                        dp = tn(v, do)
                        ds = (p * (dp - over_rows(jnp.sum, dp * p))).astype(bf16)
                        dv = nt(do, p.astype(bf16))
                        dk = rot_back(nt(q, ds))
                        dq = rot_back(nn(k, ds)) * QS
                        for j, t in enumerate((dq, dk, dv)):
                            at = pl.ds(base + j * PW + lo, HD)
                            dq_s[s, at, :] = t.astype(bf16)
                            tot = over_cols(jnp.sum, t)

                            @pl.when(s == 0)
                            def _():
                                gb_a[at, :] = tot

                            @pl.when(s > 0)
                            def _():
                                gb_a[at, :] += tot

                    gq = nn(dq_s[s, pl.ds(base, R3), :], h1_s[s])

                    @pl.when(s == 0)
                    def _():
                        acc[b, 0:R3, :] = gq
                        acc[b, R3:R3 + PW, :] = go_a[pl.ds(pl.multiple_of(g * PW, PW), PW), :]

                    @pl.when(s > 0)
                    def _():
                        acc[b, 0:R3, :] += gq

                    @pl.when(s == NS - 1)
                    def _():
                        rs.block_done(g, b, True)

                    @pl.when((s == 2) & (g > 0))
                    def _():
                        rs.settle(g - 1, 1 - b, g < TP - 1)

                    @pl.when((s == 0) & (g == 3))
                    def _():
                        rs_m.second([buf, r.landing.at[pl.ds(FB, FB)]], r.chunk)

                pair = lambda n: pl.BlockSpec((1, 1, n, S), lambda g, s: (s, g, 0, 0))
                pltpu.emit_pipeline(body, grid=(TP, NS), in_specs=[pair(R3), pair(4)])(r.qkv, r.ml)
                last = jnp.int32(TP - 1)
                rs.settle(last, lax.rem(last, 2), False)

            pl.run_scoped(pairs, vm(2, R3 + PW, D), vm(FB, D))
            wq_cp.wait()

            def close_bwd(x_ref):
                s = pl.program_id(0)
                rows = pl.ds(pl.multiple_of(s * S, S), S)
                dh1 = tn(dq_s[s], wq_v[...].reshape(TP * R3, D))
                xh, inv = ln_stats(x_ref[0].astype(f32))
                r.va[4:5, :] += over_rows(jnp.sum, dh1 * xh)
                r.va[5:6, :] += over_rows(jnp.sum, dh1)
                h1_s[s] = (r.dacc[rows, :] + ln_grad(dh1, xh, inv, gain1[...])).astype(bf16)
                gx_a2a.start(s)
                gx_a2a.local_out(s, h1_s).start()

            pltpu.emit_pipeline(close_bwd, grid=(NS,), in_specs=[pl.BlockSpec((1, S, D), lambda s: (s, 0, 0))])(r.xs)

        pl.run_scoped(heads, vm(NS, TP * R3, S, dtype=bf16), vm(TP, R3, D, dtype=bf16))

        for g in range(TP):
            r.msg[g] = r.va[...]
            for j in range(3):
                cols = jnp.broadcast_to(gb_a[g * R3 + j * PW:g * R3 + (j + 1) * PW, :], (PW, 128))
                r.msg[g, 6:7, j * PW:(j + 1) * PW] = cols.T[0:1, :]
            r.msg[g, 6:7, R3:R3 + FB] = r.gbu[g]
        small = [remote(r.msg.at[pc.slot_of(m)], r.msgs.at[pc.me], r.s_ss.at[m], r.s_rs.at[m], pc.peer(m)) for m in range(1, TP)]
        for cp in small:
            cp.start()
        own = pltpu.make_async_copy(r.msg.at[pc.slot_of(0)], r.msgs.at[pc.me], r.s_ss.at[0])
        own.start()

        def tail(bufs, act_v, turned):
            b0, b1, b2 = (bufs.at[i] for i in range(3))
            rs_a.second([b0, b1], r.chunk)
            y_own = [(pltpu.make_async_copy(r.y_seq.at[s, y_a2a._rows(pc.me)], act_v.at[s], r.tmp.at[s]),
                      pltpu.make_async_copy(act_v.at[s], r.y_out.at[pc.me * NS + s], r.tmp.at[NS + s])) for s in range(NS)]
            for load, _ in y_own:
                load.start()
            for load, store in y_own:
                load.wait()
                store.start()
            own.wait()
            for m, cp in enumerate(small):
                cp.wait_send()
                wait_for(r.msgs.at[pc.peer(m + 1)], r.s_rs.at[m + 1])
            total = r.msgs[0]
            for j in range(1, TP):
                total = total + r.msgs[j]
            r.small[...] = total
            for g in (g_bs, g_wq, g_wo, g_wu, g_wd):
                g.sent()
            for _, store in y_own:
                store.wait()
            rs_m.finish()
            for p in range(2):
                half = pl.ds(p * FB, FB)
                cps = load_all([(r.m_stage.at[3, half], b0), (r.m_r1.at[0, half], b1), (r.m_r2.at[half], b2)], r.tmp)
                for cp in cps:
                    cp.wait()
                row_add(b0, [b1, b2])
                if p == 0:
                    cp = pltpu.make_async_copy(b0, r.gd, r.tmp.at[0])
                else:
                    for k in range(D // FB):
                        cols = slice(k * FB, (k + 1) * FB)
                        turned[cols, :] = b0[:, cols].T
                    cp = pltpu.make_async_copy(turned, r.gu, r.tmp.at[0])
                cp.start()
                cp.wait()
            for s in range(NS):
                y_a2a.finish(s)
            for s in range(NS):
                gx_a2a.local_out(s, h1_s).wait()
                gx_a2a.finish(s)
            rs_a.finish()

        pl.run_scoped(tail, vm(3, FB, D), vm(NS, SL, D, dtype=bf16), vm(D, FB))

    seqs = vm(NS, S, D, dtype=bf16)
    pl.run_scoped(attn_bwd, seqs, vm(NS, D, S, dtype=bf16), vm(D, D), vm(TP * R3, 1))


def layer_call(*args):
    in_vmem = IN_NAMES[IN_NAMES.index("bqkv"):]
    vmem = pl.BlockSpec(memory_space=pltpu.VMEM)
    out = pl.pallas_call(
        layer_kernel,
        in_specs=[vmem if n in in_vmem else ANY for n in IN_NAMES],
        out_specs=[vmem if n == "small" else ANY for n in OUT_SHAPES],
        out_shape=[sds(*v) for v in OUT_SHAPES.values()],
        scratch_shapes=list(SCRATCH.values()),
        compiler_params=pltpu.CompilerParams(collective_id=0, has_side_effects=True, vmem_limit_bytes=VMEM_LIMIT),
        name="layer",
    )(*args)
    return out[:8]


FINAL = {"y": ((TP * NS, SL, D), bf16), "gx": ((TP * NS, SL, D), bf16), "gd": ((FB, D), f32), "gu": ((D, FB), f32),
         "gq": ((R3, D), f32), "go": ((PW, D), f32), "gbq": ((3, 2, HD), f32), "gbu": ((1, FB), f32)}
N_VEC = 6


def final_kernel(y_in, gx_in, small, gd_in, gu_in, stage, r1, r2, *refs):
    outs, vecs, refs = Refs(FINAL, refs[:len(FINAL)]), refs[len(FINAL):len(FINAL) + N_VEC], refs[len(FINAL) + N_VEC:]
    act, gv, sums, ld, st = refs
    n = act.shape[1]
    size = TP * NS // n
    moves = []
    terms = (stage.at[3], r1.at[0], r2)
    for p, (lo, rows, dst) in enumerate(((0, R3, outs.gq), (R3, PW, outs.go))):
        part = pl.ds(lo, rows)
        moves.append(([(t.at[part], sums.at[x, part]) for x, t in enumerate(terms)], sums.at[0, part], dst))
    for x, (src, dst) in enumerate(((y_in, outs.y), (gx_in, outs.gx))):
        for k in range(n):
            part = pl.ds(k * size, size)
            moves.append(([(src.at[part], act.at[x, k])], act.at[x, k], dst.at[part]))
    moves.append(([(gd_in, gv.at[0])], gv.at[0], outs.gd))
    moves.append(([(gu_in.at[pl.ds(0, FB)], gv.at[1, :, pl.ds(0, FB)])], gv.at[1, :, pl.ds(0, FB)], outs.gu.at[pl.ds(0, FB)]))
    moves.append(([(gu_in.at[pl.ds(FB, FB)], gv.at[1, :, pl.ds(FB, FB)])], gv.at[1, :, pl.ds(FB, FB)], outs.gu.at[pl.ds(FB, FB)]))
    loads = [[pltpu.make_async_copy(s, d, ld.at[i, x]) for x, (s, d) in enumerate(m[0])] for i, m in enumerate(moves)]
    stores = [pltpu.make_async_copy(m[1], m[2], st.at[i]) for i, m in enumerate(moves)]
    order = list(range(2, len(moves))) + [0, 1]
    for i in order:
        for cp in loads[i]:
            cp.start()
    for v, i in zip(vecs, (4, 5, 3, 1, 2, 0)):
        v[...] = small[i:i + 1, :]
    for i in range(3):
        for h in range(2):
            lo = i * PW + h * HD
            outs.gbq[i, h:h + 1, :] = small[6:7, lo:lo + HD]
    outs.gbu[...] = small[6:7, R3:R3 + FB]
    for i in order:
        for cp in loads[i]:
            cp.wait()
        for x in range(1, len(loads[i])):
            row_add(moves[i][1], [moves[i][0][x][1]])
        stores[i].start()
    for cp in stores:
        cp.wait()


def final_call(y, gx, small, gd, gu, stage, r1, r2):
    vmem = pl.BlockSpec(memory_space=pltpu.VMEM)
    n, moves = 4, 13
    return pl.pallas_call(
        final_kernel,
        in_specs=[ANY, ANY, vmem] + [ANY] * 5,
        out_specs=[vmem if k in ("gbq", "gbu") else ANY for k in FINAL] + [vmem] * N_VEC,
        out_shape=[sds(*v) for v in FINAL.values()] + [sds((1, D), f32)] * N_VEC,
        scratch_shapes=[vm(2, n, TP * NS // n, SL, D, dtype=bf16), vm(2, FB, D), vm(3, R3 + PW, D), DMA((moves, 3)), DMA((moves,))],
        compiler_params=pltpu.CompilerParams(vmem_limit_bytes=VMEM_LIMIT),
        name="results",
    )(y, gx, small, gd, gu, stage, r1, r2)


def rope_tables():
    inv_freq = (ROPE_BASE ** (-2.0 * np.arange(HH, dtype=np.float32) / HD)).astype(np.float32)
    angles = inv_freq[:, None] * np.arange(S, dtype=np.float32)[None, :]
    return np.cos(angles), np.sin(angles)


def solution(mesh):
    no = None
    act_spec = P('dp', 'tp', no)
    rep, part = P(no), P('dp')
    in_specs = (act_spec, act_spec, P('dp', no), rep, rep, P(no, no, 'tp', no), P(no, 'tp', no),
                P('tp', no, no), rep, rep, rep, P(no, 'tp'), P('tp'), P('tp', no), rep)
    out_specs = (act_spec, act_spec, part, part, P('dp', no, 'tp', no), P('dp', 'tp', no), P(('dp', 'tp'), no, no),
                 part, part, part, P('dp', 'tp'), P(('dp', 'tp')), P(('dp', 'tp'), no), part)

    def device_step(x_in, grad_y, pad_mask, ln1_gain, ln1_bias, w_qkv, b_qkv, w_out, b_out, ln2_gain, ln2_bias, w_up, b_up, w_down, b_down):
        assert x_in.shape == (TP * NS, SL, D) and w_qkv.shape == (3, D, 2, HD) and w_up.shape == (D, FB)
        row = lambda v: v.reshape(1, -1)
        wq = w_qkv.transpose(0, 2, 3, 1).reshape(R3, D)
        cos, sin = rope_tables()
        parts = layer_call(
            x_in, grad_y, wq, w_out.reshape(PW, D), w_up, w_down, b_qkv, row(b_up), pad_mask, cos, sin,
            row(ln1_gain), row(ln1_bias), row(ln2_gain), row(ln2_bias), row(b_out), row(b_down))
        y, gx, gd, gu, gq, go, gbq, gbu, *vecs = final_call(*parts)
        g1, b1, bo, g2, b2, bd = (v.reshape(D) for v in vecs)
        return (y, gx, g1, b1, gq.reshape(3, 2, HD, D).transpose(0, 3, 1, 2), gbq, go.reshape(2, HD, D), bo, g2, b2,
                gu, gbu.reshape(FB), gd, bd)

    return jax.shard_map(device_step, mesh=mesh, in_specs=in_specs, out_specs=out_specs, check_vma=False)
```

```python
import functools

import jax
import jax.numpy as jnp
import numpy as np
from jax import lax
from jax.experimental import pallas as pl
from jax.experimental.pallas import tpu as pltpu
from jax.sharding import PartitionSpec as P

f32 = jnp.float32
bf16 = jnp.bfloat16
LN_EPS = 1e-5
ROPE_BASE = 10000.0
INV_SQRT2 = 0.7071067811865476
INV_SQRT_2PI = 0.3989422804014327
NEG_LARGE = -1e30
MESH = pl.DeviceIdType.MESH
ANY = pl.BlockSpec(memory_space=pl.ANY)
VMEM_LIMIT = 66_000_000

TP = 8
NS = 4
S = 512
D = 1024
PW = 128
HD = 64
HH = HD // 2
FB = 512
SL = 64
QS = HD ** -0.5
R3 = 3 * PW


def dg(a, b, ca, cb):
    return lax.dot_general(a, b, (((ca,), (cb,)), ((), ())), preferred_element_type=f32)


def nn(a, b):
    return dg(a, b, 1, 0)


def nt(a, b):
    return dg(a, b, 1, 1)


def tn(a, b):
    return dg(a, b, 0, 0)


def over_rows(reduce, v):
    return reduce(v, axis=0, keepdims=True)


def over_cols(reduce, v):
    return reduce(v, axis=1, keepdims=True)


def sds(shape, dtype):
    return jax.ShapeDtypeStruct(shape, dtype)


class Place:
    def __init__(self):
        me = lax.axis_index("tp")
        self.me = me
        self.c = lax.rem(me, 2)
        self.dc = 1 - 2 * self.c
        self.dx = 2 - 4 * lax.rem(lax.div(me, 2), 2)
        self.dy = 4 - 8 * lax.div(me, 4)
        self.partner = me + self.dc
        self.a = me + (1 - self.c) * self.dx + self.c * self.dy
        self.b = me + (1 - self.c) * self.dy + self.c * self.dx

    def peer(self, m):
        return self.me + (m & 1) * self.dc + ((m >> 1) & 1) * self.dx + (m >> 2) * self.dy

    def slot_of(self, m):
        k = self.c if m % 2 == 0 else 1 - self.c
        lo, hi = {0: (6, 7), 1: (0, 5), 2: (4, 1), 3: (2, 3)}[m >> 1]
        return lo + k * (hi - lo)


def remote(src, dst, send_sem, recv_sem, device):
    return pltpu.make_async_remote_copy(src_ref=src, dst_ref=dst, send_sem=send_sem, recv_sem=recv_sem,
                                        device_id={"tp": device}, device_id_type=MESH)


def wait_for(ref, sem):
    pltpu.make_async_copy(ref, ref, sem).wait()


def entry_barrier(pc):
    bar = pltpu.get_barrier_semaphore()
    for m in range(1, TP):
        pl.semaphore_signal(bar, inc=1, device_id={"tp": pc.peer(m)}, device_id_type=MESH)
    pl.semaphore_wait(bar, TP - 1)


class AllToAll:
    def __init__(self, pc, pos_ref, seq_ref, send_sem, recv_sem, inward):
        self.pc, self.pos, self.seq, self.ss, self.rs, self.inward = pc, pos_ref, seq_ref, send_sem, recv_sem, inward

    def _rows(self, dev):
        return pl.ds(pl.multiple_of(dev * SL, SL), SL)

    def _copy(self, s, m):
        pc, dev = self.pc, self.pc.peer(m)
        if self.inward:
            src, dst = self.pos.at[dev * NS + s], self.seq.at[s, self._rows(pc.me)]
        else:
            src, dst = self.seq.at[s, self._rows(dev)], self.pos.at[pc.me * NS + s]
        return remote(src, dst, self.ss.at[s, m], self.rs.at[s, m], dev)

    def start(self, s):
        for m in (2, 3, 4, 5, 6, 7, 1):
            self._copy(s, m).start()

    def finish(self, s):
        for m in range(1, TP):
            self._copy(s, m).wait()

    def local_in(self, buf):
        pc = self.pc
        return (pltpu.make_async_copy(self.pos.at[pl.ds(pc.me * NS, NS)], buf, self.ss.at[0, 0]),
                pltpu.make_async_copy(buf, self.seq.at[:, self._rows(pc.me)], self.rs.at[0, 0]))

    def local_out(self, s, src):
        return pltpu.make_async_copy(src.at[s, self._rows(self.pc.me)], self.pos.at[self.pc.me * NS + s], self.ss.at[s, 0])


class Gather:
    def __init__(self, pc, src_ref, dst_ref, send_sem, recv_sem):
        self.pc, self.src, self.dst, self.ss, self.rs = pc, src_ref, dst_ref, send_sem, recv_sem

    def _send(self, i, src, slot, dev):
        return remote(src, self.dst.at[slot], self.ss.at[i], self.rs.at[slot], dev)

    def _direct(self):
        pc, c = self.pc, self.pc.c
        return [self._send(0, self.src, c, pc.a), self._send(2, self.src, 6 + c, pc.partner),
                self._send(1, self.src, 4 + c, pc.b)]

    def _hop(self):
        pc, c = self.pc, self.pc.c
        return [self._send(3, self.dst.at[c], 2 + c, pc.b), self._send(4, self.dst.at[c], c, pc.partner),
                self._send(5, self.dst.at[4 + c], 4 + c, pc.partner)]

    def _last(self):
        pc, c = self.pc, self.pc.c
        return self._send(6, self.dst.at[2 + c], 2 + c, pc.partner)

    def arrived(self, slot):
        wait_for(self.dst.at[slot], self.rs.at[slot])

    def start(self):
        self.start_a()
        self.start_b()

    def start_a(self):
        for cp in self._direct()[:2]:
            cp.start()

    def start_b(self):
        self._direct()[2].start()

    def forward(self):
        self.forward_a()
        self.forward_b()

    def forward_a(self):
        hop = self._hop()
        self.arrived(self.pc.c)
        hop[0].start()
        hop[1].start()

    def forward_b(self):
        self.arrived(4 + self.pc.c)
        self._hop()[2].start()

    def last(self):
        self.arrived(2 + self.pc.c)
        self._last().start()

    def local(self, buf):
        return (pltpu.make_async_copy(self.src, buf, self.ss.at[7]),
                pltpu.make_async_copy(buf, self.dst.at[6 + self.pc.c], self.rs.at[6 + self.pc.c]))

    def arrived_near(self):
        for j in (0, 2, 3):
            self.arrived(2 * j + 1 - self.pc.c)
        self.arrived(6 + self.pc.c)

    def arrived_far(self):
        self.arrived(3 - self.pc.c)

    def sent(self):
        for cp in self._direct() + self._hop() + [self._last()]:
            cp.wait_send()


def row_add(acc, others):
    step = 64

    def body(i, carry):
        r = pl.ds(pl.multiple_of(i * step, step), step)
        v = acc[r, :]
        for o in others:
            v = v + o[r, :]
        acc[r, :] = v
        return carry

    lax.fori_loop(0, acc.shape[0] // step, body, 0)


class GradScatter:
    def __init__(self, pc, acc, landing, stage, r1, r2, sems, free):
        self.pc, self.acc, self.landing, self.stage, self.r1, self.r2 = pc, acc, landing, stage, r1, r2
        self.sem, self.free = sems, free

    def _pair(self, b):
        return remote(self.acc.at[b], self.landing, self.sem.at[0], self.sem.at[1], self.pc.partner)

    def _first(self, j):
        return remote(self.stage.at[j], self.r1.at[j], self.sem.at[2 + j], self.sem.at[4 + j], self.pc.a)

    def _second(self):
        return remote(self.stage.at[2], self.r2, self.sem.at[6], self.sem.at[7], self.pc.b)

    def block_done(self, slot, b, needs_credit):
        @pl.when(lax.rem(slot, 2) != self.pc.c)
        def _():
            @pl.when(needs_credit)
            def _():
                pl.semaphore_wait(self.free, 1)

            self._pair(b).start()

    def settle(self, slot, b, gives_credit):
        c = self.pc.c
        own = lax.rem(slot, 2) == c
        j = lax.div(slot, 2)

        @pl.when(own)
        def _():
            wait_for(self.landing, self.sem.at[1])
            row_add(self.acc.at[b], [self.landing])

            @pl.when(gives_credit)
            def _():
                pl.semaphore_signal(self.free, inc=1, device_id={"tp": self.pc.partner}, device_id_type=MESH)

            store = pltpu.make_async_copy(self.acc.at[b], self.stage.at[j], self.sem.at[8])
            store.start()
            store.wait()

            @pl.when(j < 2)
            def _():
                self._first(j).start()

        @pl.when(jnp.logical_not(own))
        def _():
            self._pair(b).wait_send()

    def second(self, bufs, chunk_sem):
        n = chunk_sem.shape[1]
        size = bufs[0].shape[0]
        rows = size // n
        part = lambda ref, k: ref.at[pl.ds(k * rows, rows)]
        wait_for(self.r1.at[1], self.sem.at[5])
        for p in range(self.r2.shape[0] // size):
            mine, theirs = (ref.at[pl.ds(p * size, size)] for ref in (self.stage.at[2], self.r1.at[1]))
            loads = [[pltpu.make_async_copy(part(src, k), part(buf, k), chunk_sem.at[x, k])
                      for x, (src, buf) in enumerate(zip((mine, theirs), bufs))] for k in range(n)]
            stores = [pltpu.make_async_copy(part(bufs[0], k), part(mine, k), chunk_sem.at[2, k]) for k in range(n)]
            for group in loads:
                for cp in group:
                    cp.start()
            for k in range(n):
                for cp in loads[k]:
                    cp.wait()
                row_add(part(bufs[0], k), [part(bufs[1], k)])
                stores[k].start()
            for cp in stores:
                cp.wait()
        self._second().start()

    def finish(self):
        wait_for(self.r1.at[0], self.sem.at[4])
        for j in range(2):
            self._first(j).wait_send()
        self._second().wait()


def ln_stats(v):
    c = v - over_cols(jnp.mean, v)
    inv = lax.rsqrt(over_cols(jnp.mean, c * c) + LN_EPS)
    return c * inv, inv


def ln_grad(d_out, x_hat, inv, gain):
    dh = d_out * gain
    return inv * (dh - over_cols(jnp.mean, dh) - x_hat * over_cols(jnp.mean, dh * x_hat))


def masked_scores(q, k, ok):
    return jnp.where(ok, tn(k, q), NEG_LARGE)


def key_mask(mask):
    return jnp.concatenate([mask] * (S // PW), axis=1) > 0


def column(row):
    return jnp.broadcast_to(row, (128, row.shape[1])).T[:, :1]


def clear(*refs):
    for ref in refs:
        ref[...] = jnp.zeros(ref.shape, ref.dtype)


def load_all(pairs, sem):
    cps = [pltpu.make_async_copy(s, d, sem.at[i]) for i, (s, d) in enumerate(pairs)]
    for cp in cps:
        cp.start()
    return cps


def vm(*shape, dtype=f32):
    return pltpu.VMEM(shape, dtype)


TT = 1024
NT = NS * S // TT
IN_NAMES = ("x_in", "dy_in", "wq", "wo", "wu", "wd", "bqkv", "bup", "pad", "cos", "sin", "gain1", "bias1", "gain2", "bias2",
            "b_out", "b_down")
OUT_SHAPES = {
    "y_out": ((TP * NS, SL, D), bf16), "gx_out": ((TP * NS, SL, D), bf16), "small": ((8, D), f32), "gd": ((FB, D), f32), "gu": ((D, FB), f32),
    "a_stage": ((4, R3 + PW, D), f32), "a_r1": ((2, R3 + PW, D), f32), "a_r2": ((R3 + PW, D), f32),
    "m_stage": ((4, 2 * FB, D), f32), "m_r1": ((2, 2 * FB, D), f32), "m_r2": ((2 * FB, D), f32),
    "xs": ((NS, S, D), bf16), "dys": ((NS, S, D), bf16), "wq_all": ((TP, R3, D), bf16), "wo_all": ((TP, PW, D), bf16),
    "wu_all": ((TP, D, FB), bf16), "wd_all": ((TP, FB, D), bf16),
    "qkv": ((NS, TP, R3, S), bf16), "ml": ((NS, TP, 4, S), f32), "o": ((NS, TP, PW, S), bf16),
    "x1": ((NS, S, D), bf16), "y_seq": ((NS, S, D), bf16),
}
DMA = pltpu.SemaphoreType.DMA
SCRATCH = {
    "bs_all": vm(TP, 8, 128), "bs": vm(8, 128), "mask": vm(NS, S, PW), "dacc": vm(NS * S, D), "landing": vm(2 * FB, D), "gbu": vm(TP, 1, FB), "va": vm(8, D),
    "msg": vm(TP, 8, D), "msgs": vm(TP, 8, D),
    "free": pltpu.SemaphoreType.REGULAR,
    "x_ss": DMA((NS, 8)), "x_rs": DMA((NS, 8)), "dy_ss": DMA((NS, 8)), "dy_rs": DMA((NS, 8)),
    "y_ss": DMA((NS, 8)), "y_rs": DMA((NS, 8)), "gx_ss": DMA((NS, 8)), "gx_rs": DMA((NS, 8)),
    "g_ss": DMA((5, 8)), "g_rs": DMA((5, 8)), "m_sem": DMA((9,)), "a_sem": DMA((9,)), "s_ss": DMA((8,)), "s_rs": DMA((8,)),
    "tmp": DMA((8,)), "chunk": DMA((3, 4)), "w_sem": DMA((2, 2)),
}


class Refs:
    def __init__(self, names, refs):
        for n, r in zip(names, refs):
            setattr(self, n, r)


def layer_kernel(*refs):
    r = Refs(IN_NAMES + tuple(OUT_SHAPES) + tuple(SCRATCH), refs)
    pc = Place()
    for i in range(3):
        for h in range(2):
            r.bs[pl.ds(i, 1), pl.ds(h * HD, HD)] = r.bqkv[i, pl.ds(h, 1), :]
    for k in range(FB // PW):
        r.bs[pl.ds(4 + k, 1), :] = r.bup[:, pl.ds(k * PW, PW)]
    entry_barrier(pc)
    x_a2a = AllToAll(pc, r.x_in, r.xs, r.x_ss, r.x_rs, True)
    dy_a2a = AllToAll(pc, r.dy_in, r.dys, r.dy_ss, r.dy_rs, True)
    y_a2a = AllToAll(pc, r.y_out, r.y_seq, r.y_ss, r.y_rs, False)
    g_bs, g_wq, g_wo, g_wu, g_wd = [
        Gather(pc, s, d, r.g_ss.at[i], r.g_rs.at[i])
        for i, (s, d) in enumerate(((r.bs, r.bs_all), (r.wq, r.wq_all), (r.wo, r.wo_all), (r.wu, r.wu_all), (r.wd, r.wd_all)))]
    gain1, bias1, gain2, bias2, b_out, b_down = r.gain1, r.bias1, r.gain2, r.bias2, r.b_out, r.b_down

    def arrivals(b_x, b_dy, b_q, b_o, b_u, b_d):
        first = (g_bs, g_wq, g_wo)
        for g in first:
            g.start()
        x_a2a.start(0)
        own_bs = pltpu.make_async_copy(r.bs, r.bs_all.at[6 + pc.c], r.g_rs.at[0, 6 + pc.c])
        own_bs.start()
        local = [x_a2a.local_in(b_x), dy_a2a.local_in(b_dy)]
        local += [g.local(b) for g, b in ((g_wq, b_q), (g_wo, b_o), (g_wu, b_u), (g_wd, b_d))]
        for load, _ in local:
            load.start()
        for s in range(NS):
            keys = jnp.broadcast_to(r.pad[pl.ds(pc.me * NS + s, 1), :].astype(f32), (PW, S))
            r.mask[s] = keys.T
        for load, store in local:
            load.wait()
            store.start()
        for g in first:
            g.forward_a()
        for g in first:
            g.forward_b()
        x_a2a.finish(0)
        x_a2a.start(1)
        for g in first:
            g.arrived_near()
        for g in (g_wu, g_wd):
            g.arrived(6 + pc.c)
        local[0][1].wait()
        local[1][1].wait()

    def later_arrivals():
        for g in (g_bs, g_wq, g_wo):
            g.last()
        for s in range(2, NS):
            x_a2a.start(s)
        for s in range(NS):
            dy_a2a.start(s)
        g_wu.start_a()
        g_wd.start_a()
        for g in (g_bs, g_wq, g_wo):
            g.arrived_far()

    act = vm(NS, SL, D, dtype=bf16)
    pl.run_scoped(arrivals, act, act, vm(R3, D, dtype=bf16), vm(PW, D, dtype=bf16), vm(D, FB, dtype=bf16), vm(FB, D, dtype=bf16))

    def attn_fwd(h2_v, wq_v, wo_v, h1_s, o_s):
        def fetch(*pairs):
            for cp in load_all(pairs, r.tmp):
                cp.wait()

        fetch(*[(r.wq_all.at[pl.ds(k, 2)], wq_v.at[pl.ds(k, 2)]) for k in (6, 0, 4)])

        def slot_at(n):
            return jnp.where(n < 2, n + 6, jnp.where(n < 4, n - 2, jnp.where(n < 6, n, n - 4)))

        def body(x_ref, qkv_ref, ml_ref, o_ref, x1_ref):
            s, n = pl.program_id(0), pl.program_id(1)
            g = slot_at(n)

            @pl.when(n == 0)
            def _():
                xh, _ = ln_stats(x_ref[0].astype(f32))
                h1_s[...] = (xh * gain1[...] + bias1[...]).astype(bf16)

            bias = r.bs_all[g]
            bias = jnp.concatenate([column(bias[i:i + 1]) for i in range(3)], axis=0)
            qkv = nt(wq_v[g], h1_s[...]) + bias
            cos, sin = r.cos[...], r.sin[...]
            ok = key_mask(r.mask[s])

            def rot(t):
                a, b = t[:HH], t[HH:]
                return jnp.concatenate([a * cos - b * sin, b * cos + a * sin], axis=0).astype(bf16)

            for h in range(2):
                lo = h * HD
                at_q, at_k, at_v = (slice(j * PW + lo, j * PW + lo + HD) for j in range(3))
                q, k, v = rot(qkv[at_q] * QS), rot(qkv[at_k]), qkv[at_v].astype(bf16)
                for at, t in ((at_q, q), (at_k, k), (at_v, v)):
                    qkv_ref[0, 0, at, :] = t
                sc = masked_scores(q, k, ok)
                m = over_rows(jnp.max, sc)
                e = jnp.exp(sc - m)
                li = 1.0 / over_rows(jnp.sum, e)
                p = (e * li).astype(bf16)
                ml_ref[0, 0, h:h + 1, :] = m
                ml_ref[0, 0, 2 + h:3 + h, :] = li
                o = nn(v, p).astype(bf16)
                o_ref[0, 0, lo:lo + HD, :] = o
                o_s[pl.ds(pl.multiple_of(g * PW + lo, HD), HD), :] = o

            @pl.when((s == 0) & (n == 5))
            def _():
                later_arrivals()
                fetch((r.wq_all.at[pl.ds(2, 2)], wq_v.at[pl.ds(2, 2)]), (r.wo_all, wo_v))

            @pl.when(n == TP - 1)
            def _():
                attn = tn(o_s[...], wo_v[...].reshape(TP * PW, D))
                x1 = (x_ref[0].astype(f32) + (attn + b_out[...])).astype(bf16)
                x1_ref[0] = x1
                xh, _ = ln_stats(x1.astype(f32))
                h2_v[pl.ds(pl.multiple_of(s * S, S), S), :] = (xh * gain2[...] + bias2[...]).astype(bf16)

            for k in range(1, NS):
                @pl.when((s == k - 1) & (n == TP - 2))
                def _():
                    x_a2a.finish(k)

        seq = pl.BlockSpec((1, S, D), lambda s, n: (s, 0, 0))
        pair = lambda rows: pl.BlockSpec((1, 1, rows, S), lambda s, n: (s, slot_at(n), 0, 0))
        pltpu.emit_pipeline(body, grid=(NS, TP), in_specs=[seq], out_specs=[pair(R3), pair(4), pair(PW), seq])(
            r.xs, r.qkv, r.ml, r.o, r.x1)

    def mlp(h2_v, dy_v, wu_v, wd_v, yacc, acc):
        rs = GradScatter(pc, acc, r.landing, r.m_stage, r.m_r1, r.m_r2, r.m_sem, r.free)

        def slot_at(i):
            return jnp.where(i == 0, 6, jnp.where(i == 5, 7, i - 1 - lax.div(i, 6)))
        def weights(slot, b):
            return (pltpu.make_async_copy(r.wu_all.at[slot], wu_v.at[b], r.w_sem.at[0, b]),
                    pltpu.make_async_copy(r.wd_all.at[slot], wd_v.at[b], r.w_sem.at[1, b]))

        def fetch(i):
            slot = slot_at(i)

            @pl.when(lax.rem(slot, 2) != pc.c)
            def _():
                g_wu.arrived(slot)
                g_wd.arrived(slot)

            for cp in weights(slot, lax.rem(i, 2)):
                cp.start()

        fetch(jnp.int32(0))
        cps = []
        for s in range(NS):
            dy_a2a.finish(s)
            cps.append(pltpu.make_async_copy(r.dys.at[s], dy_v.at[pl.ds(s * S, S)], r.tmp.at[s]))
            cps[s].start()
        clear(yacc, r.dacc, r.gbu)
        for cp in cps:
            cp.wait()

        def step(n, carry):
            i, t = lax.div(n, NT), lax.rem(n, NT)
            b = lax.rem(i, 2)
            slot = slot_at(i)

            @pl.when(t == 0)
            def _():
                for cp in weights(slot, b):
                    cp.wait()
                clear(acc.at[b])

            @pl.when((t == NT - 1) & (i != 0) & (i != 2) & (i < TP - 1))
            def _():
                fetch(i + 1)

            rows = pl.ds(pl.multiple_of(t * TT, TT), TT)
            h2, dy = h2_v[rows, :], dy_v[rows, :]
            wu, wd = wu_v[b], wd_v[b]
            bias = r.bs_all[slot]
            bias = jnp.concatenate([bias[k:k + 1] for k in range(4, TP)], axis=1)
            pre = nn(h2, wu) + bias
            d_act = nt(dy, wd)
            cdf = 0.5 * (1.0 + lax.erf(pre * INV_SQRT2))
            act = (pre * cdf).astype(bf16)
            d_pre = d_act * (cdf + pre * jnp.exp(-0.5 * pre * pre) * INV_SQRT_2PI)
            d_pre_b = d_pre.astype(bf16)
            yacc[rows, :] += nn(act, wd)
            r.dacc[rows, :] += nt(d_pre_b, wu)
            acc[b, :FB, :] += tn(act, dy)
            acc[b, FB:, :] += tn(d_pre_b, h2)
            r.gbu[slot] += over_rows(jnp.sum, d_pre)

            @pl.when(t == NT - 1)
            def _():
                rs.block_done(slot, b, i > 2 * (1 - pc.c))

            @pl.when((t == 0) & (i > 0))
            def _():
                rs.settle(slot_at(i - 1), 1 - b, True)

            for when, hops in ((1, ("forward_a", "start_b")), (4, ("last",)), (5, ()), (9, ("forward_b",))):
                @pl.when(n == when)
                def _():
                    for hop in hops:
                        for gather in (g_wu, g_wd):
                            getattr(gather, hop)()
                    if when in (1, 5):
                        fetch(i + 1)

            return carry

        lax.fori_loop(0, TP * NT, step, 0)
        cps = load_all([(r.x1.at[s], h2_v.at[pl.ds(s * S, S)]) for s in range(NS)], r.tmp)
        stores = []
        for s in range(NS):
            rows = pl.ds(s * S, S)
            cps[s].wait()
            dy_v[rows, :] = (h2_v[rows, :].astype(f32) + (yacc[rows, :] + b_down[...])).astype(bf16)
            cp = pltpu.make_async_copy(dy_v.at[rows], r.y_seq.at[s], r.tmp.at[NS + s])
            cp.start()
            stores.append(cp)
        for s in range(NS):
            stores[s].wait()
            y_a2a.start(s)
        last = jnp.int32(TP - 1)
        rs.settle(slot_at(last), lax.rem(last, 2), True)

    tok = vm(NS * S, D, dtype=bf16)

    def forward_and_mlp(h2_v, dy_v, wu_v, wd_v):
        pl.run_scoped(functools.partial(attn_fwd, h2_v), vm(TP, R3, D, dtype=bf16), vm(TP, PW, D, dtype=bf16),
                      vm(S, D, dtype=bf16), vm(D, S, dtype=bf16))
        pl.run_scoped(functools.partial(mlp, h2_v, dy_v, wu_v, wd_v), vm(NS * S, D), vm(2, 2 * FB, D))

    pl.run_scoped(forward_and_mlp, tok, tok, vm(2, D, FB, dtype=bf16), vm(2, FB, D, dtype=bf16))

    rs_m = GradScatter(pc, None, None, r.m_stage, r.m_r1, r.m_r2, r.m_sem, r.free)

    def attn_bwd(h1_s, do_s, acc, gb_a):
        gx_a2a = AllToAll(pc, r.gx_out, h1_s, r.gx_ss, r.gx_rs, False)

        def open_bwd(wo_v):
            wo_cp = pltpu.make_async_copy(r.wo_all, wo_v, r.tmp.at[0])
            wo_cp.start()
            wo_cp.wait()
            clear(r.va, acc, gb_a)

            def body(x_ref, x1_ref, dy_ref, o_ref):
                s = pl.program_id(0)
                rows = pl.ds(pl.multiple_of(s * S, S), S)
                dy, dh2 = dy_ref[0].astype(f32), r.dacc[rows, :]
                xh2, inv2 = ln_stats(x1_ref[0].astype(f32))
                d = dy + ln_grad(dh2, xh2, inv2, gain2[...])
                r.dacc[rows, :] = d
                db = d.astype(bf16)
                r.va[0:1, :] += over_rows(jnp.sum, dy)
                r.va[1:2, :] += over_rows(jnp.sum, dh2 * xh2)
                r.va[2:3, :] += over_rows(jnp.sum, dh2)
                r.va[3:4, :] += over_rows(jnp.sum, d)
                xh, _ = ln_stats(x_ref[0].astype(f32))
                h1_s[s] = (xh * gain1[...] + bias1[...]).astype(bf16)
                do_s[s] = nt(wo_v[...].reshape(TP * PW, D), db).astype(bf16)
                acc[:, R3:, :] += nn(o_ref[0].reshape(TP * PW, S), db).reshape(TP, PW, D)

            seq = pl.BlockSpec((1, S, D), lambda s: (s, 0, 0))
            pltpu.emit_pipeline(body, grid=(NS,), in_specs=[seq, seq, seq, pl.BlockSpec((1, TP, PW, S), lambda s: (s, 0, 0, 0))])(
                r.xs, r.x1, r.dys, r.o)

        pl.run_scoped(open_bwd, vm(TP, PW, D, dtype=bf16))
        n_half = NS // 2
        rs = GradScatter(pc, acc, r.landing.at[pl.ds(0, R3 + PW)], r.a_stage, r.a_r1, r.a_r2, r.a_sem, r.free)

        def slot_at(g):
            return jnp.where(g < 4, lax.rem(g + 2, 4), g)

        def heads(dq_s, wq_v, buf):
            wq_cp = pltpu.make_async_copy(r.wq_all, wq_v, r.tmp.at[1])
            wq_cp.start()
            for half in range(2):
                def body(qkv_ref, ml_ref):
                    n, sh = pl.program_id(0), pl.program_id(1)
                    g = slot_at(n)
                    s = half * n_half + sh
                    cos, sin = r.cos[...], r.sin[...]
                    ok = key_mask(r.mask[s])

                    def rot_back(t):
                        a, b = t[:HH], t[HH:]
                        return jnp.concatenate([a * cos + b * sin, b * cos - a * sin], axis=0)

                    base = pl.multiple_of(g * R3, PW)
                    for h in range(2):
                        lo = h * HD
                        q, k, v = (qkv_ref[0, 0, j * PW + lo:j * PW + lo + HD, :] for j in range(3))
                        do = do_s[s, pl.ds(pl.multiple_of(g * PW + lo, HD), HD), :]
                        sc = masked_scores(q, k, ok)
                        p = jnp.exp(sc - ml_ref[0, 0, h:h + 1, :]) * ml_ref[0, 0, 2 + h:3 + h, :]
                        dp = tn(v, do)
                        ds = (p * (dp - over_rows(jnp.sum, dp * p))).astype(bf16)
                        dv = nt(p.astype(bf16), do).T
                        dk = rot_back(nt(ds, q).T)
                        dq = rot_back(nn(k, ds)) * QS
                        for j, t in enumerate((dq, dk, dv)):
                            at = pl.ds(base + j * PW + lo, HD)
                            dq_s[sh, at, :] = t.astype(bf16)
                            gb_a[at, :] += over_cols(jnp.sum, t)

                    acc[g, :R3, :] += nn(dq_s[sh, pl.ds(base, R3), :], h1_s[s])
                    if half == 0:
                        @pl.when((sh == 0) & (n == 1))
                        def _():
                            rs_m.second([buf, r.landing.at[pl.ds(FB, FB)]], r.chunk)
                    else:
                        @pl.when(sh == n_half - 1)
                        def _():
                            rs.block_done(g, g, True)

                            @pl.when(n > 0)
                            def _():
                                rs.settle(slot_at(n - 1), slot_at(n - 1), n < TP - 1)

                pair = lambda rows: pl.BlockSpec((1, 1, rows, S), lambda n, sh: (half * n_half + sh, slot_at(n), 0, 0))
                pltpu.emit_pipeline(body, grid=(TP, n_half), in_specs=[pair(R3), pair(4)])(r.qkv, r.ml)
                if half == 0:
                    wq_cp.wait()

                def close_bwd(x_ref):
                    sh = pl.program_id(0)
                    s = half * n_half + sh
                    rows = pl.ds(pl.multiple_of(s * S, S), S)
                    dh1 = tn(dq_s[sh], wq_v[...].reshape(TP * R3, D))
                    xh, inv = ln_stats(x_ref[0].astype(f32))
                    r.va[4:5, :] += over_rows(jnp.sum, dh1 * xh)
                    r.va[5:6, :] += over_rows(jnp.sum, dh1)
                    h1_s[s] = (r.dacc[rows, :] + ln_grad(dh1, xh, inv, gain1[...])).astype(bf16)
                    gx_a2a.start(s)
                    gx_a2a.local_out(s, h1_s).start()

                pltpu.emit_pipeline(close_bwd, grid=(n_half,),
                                    in_specs=[pl.BlockSpec((1, S, D), lambda sh: (half * n_half + sh, 0, 0))])(r.xs)
            last = jnp.int32(TP - 1)
            rs.settle(last, last, False)
            rs.second([buf, r.landing.at[pl.ds(FB, FB)]], r.chunk)

        pl.run_scoped(heads, vm(n_half, TP * R3, S, dtype=bf16), vm(TP, R3, D, dtype=bf16), vm(FB, D))

        for g in range(TP):
            r.msg[g] = r.va[...]
            for j in range(3):
                cols = jnp.broadcast_to(gb_a[g * R3 + j * PW:g * R3 + (j + 1) * PW, :], (PW, 128))
                r.msg[g, 6:7, j * PW:(j + 1) * PW] = cols.T[0:1, :]
            r.msg[g, 6:7, R3:R3 + FB] = r.gbu[g]
        small = [remote(r.msg.at[pc.slot_of(m)], r.msgs.at[pc.me], r.s_ss.at[m], r.s_rs.at[m], pc.peer(m)) for m in range(1, TP)]
        for cp in small:
            cp.start()
        own = pltpu.make_async_copy(r.msg.at[pc.slot_of(0)], r.msgs.at[pc.me], r.s_ss.at[0])
        own.start()

        def tail(bufs, act_v, turned):
            b0, b1, b2 = (bufs.at[i] for i in range(3))
            y_own = [(pltpu.make_async_copy(r.y_seq.at[s, y_a2a._rows(pc.me)], act_v.at[s], r.tmp.at[s]),
                      pltpu.make_async_copy(act_v.at[s], r.y_out.at[pc.me * NS + s], r.tmp.at[NS + s])) for s in range(NS)]
            for load, _ in y_own:
                load.start()
            for load, store in y_own:
                load.wait()
                store.start()
            for g in (g_bs, g_wq, g_wo, g_wu, g_wd):
                g.sent()
            for _, store in y_own:
                store.wait()
            rs_m.finish()
            for p in range(2):
                half = pl.ds(p * FB, FB)
                cps = load_all([(r.m_stage.at[3, half], b0), (r.m_r1.at[0, half], b1), (r.m_r2.at[half], b2)], r.tmp)
                for cp in cps:
                    cp.wait()
                row_add(b0, [b1, b2])
                if p == 0:
                    cp = pltpu.make_async_copy(b0, r.gd, r.tmp.at[0])
                else:
                    for k in range(D // FB):
                        cols = slice(k * FB, (k + 1) * FB)
                        turned[cols, :] = b0[:, cols].T
                    cp = pltpu.make_async_copy(turned, r.gu, r.tmp.at[0])
                cp.start()
                cp.wait()
            for s in range(NS):
                y_a2a.finish(s)
            for s in range(NS):
                gx_a2a.local_out(s, h1_s).wait()
                gx_a2a.finish(s)
            rs.finish()
            own.wait()
            for m, cp in enumerate(small):
                cp.wait_send()
                wait_for(r.msgs.at[pc.peer(m + 1)], r.s_rs.at[m + 1])
            total = r.msgs[0]
            for j in range(1, TP):
                total = total + r.msgs[j]
            r.small[...] = total

        pl.run_scoped(tail, vm(3, FB, D), vm(NS, SL, D, dtype=bf16), vm(D, FB))

    seqs = vm(NS, S, D, dtype=bf16)
    pl.run_scoped(attn_bwd, seqs, vm(NS, D, S, dtype=bf16), vm(TP, R3 + PW, D), vm(TP * R3, 1))


def layer_call(*args):
    in_vmem = IN_NAMES[IN_NAMES.index("bqkv"):]
    vmem = pl.BlockSpec(memory_space=pltpu.VMEM)
    out = pl.pallas_call(
        layer_kernel,
        in_specs=[vmem if n in in_vmem else ANY for n in IN_NAMES],
        out_specs=[vmem if n == "small" else ANY for n in OUT_SHAPES],
        out_shape=[sds(*v) for v in OUT_SHAPES.values()],
        scratch_shapes=list(SCRATCH.values()),
        compiler_params=pltpu.CompilerParams(collective_id=0, has_side_effects=True, vmem_limit_bytes=VMEM_LIMIT),
        name="layer",
    )(*args)
    return out[:8]


FINAL = {"y": ((TP * NS, SL, D), bf16), "gx": ((TP * NS, SL, D), bf16), "gd": ((FB, D), f32), "gu": ((D, FB), f32),
         "gq": ((R3, D), f32), "go": ((PW, D), f32), "gbq": ((3, 2, HD), f32), "gbu": ((1, FB), f32)}
N_VEC = 6


def final_kernel(y_in, gx_in, small, gd_in, gu_in, stage, r1, r2, *refs):
    outs, vecs, refs = Refs(FINAL, refs[:len(FINAL)]), refs[len(FINAL):len(FINAL) + N_VEC], refs[len(FINAL) + N_VEC:]
    act, gv, sums, ld, st = refs
    n = act.shape[1]
    size = TP * NS // n
    moves = []
    terms = (stage.at[3], r1.at[0], r2)
    for p, (lo, rows, dst) in enumerate(((0, R3, outs.gq), (R3, PW, outs.go))):
        part = pl.ds(lo, rows)
        moves.append(([(t.at[part], sums.at[x, part]) for x, t in enumerate(terms)], sums.at[0, part], dst))
    for x, (src, dst) in enumerate(((y_in, outs.y), (gx_in, outs.gx))):
        for k in range(n):
            part = pl.ds(k * size, size)
            moves.append(([(src.at[part], act.at[x, k])], act.at[x, k], dst.at[part]))
    moves.append(([(gd_in, gv.at[0])], gv.at[0], outs.gd))
    for k in range(D // FB):
        part = pl.ds(k * FB, FB)
        moves.append(([(gu_in.at[part], gv.at[1, :, part])], gv.at[1, :, part], outs.gu.at[part]))
    loads = [[pltpu.make_async_copy(s, d, ld.at[i, x]) for x, (s, d) in enumerate(m[0])] for i, m in enumerate(moves)]
    stores = [pltpu.make_async_copy(m[1], m[2], st.at[i]) for i, m in enumerate(moves)]
    order = list(range(2, len(moves))) + [0, 1]
    for i in order:
        for cp in loads[i]:
            cp.start()
    for v, i in zip(vecs, (4, 5, 3, 1, 2, 0)):
        v[...] = small[i:i + 1, :]
    for i in range(3):
        for h in range(2):
            lo = i * PW + h * HD
            outs.gbq[i, h:h + 1, :] = small[6:7, lo:lo + HD]
    outs.gbu[...] = small[6:7, R3:R3 + FB]
    for i in order:
        for cp in loads[i]:
            cp.wait()
        for x in range(1, len(loads[i])):
            row_add(moves[i][1], [moves[i][0][x][1]])
        stores[i].start()
    for cp in stores:
        cp.wait()


def final_call(y, gx, small, gd, gu, stage, r1, r2):
    vmem = pl.BlockSpec(memory_space=pltpu.VMEM)
    n, moves = 4, 13
    return pl.pallas_call(
        final_kernel,
        in_specs=[ANY, ANY, vmem] + [ANY] * 5,
        out_specs=[vmem if k in ("gbq", "gbu") else ANY for k in FINAL] + [vmem] * N_VEC,
        out_shape=[sds(*v) for v in FINAL.values()] + [sds((1, D), f32)] * N_VEC,
        scratch_shapes=[vm(2, n, TP * NS // n, SL, D, dtype=bf16), vm(2, FB, D), vm(3, R3 + PW, D), DMA((moves, 3)), DMA((moves,))],
        compiler_params=pltpu.CompilerParams(vmem_limit_bytes=VMEM_LIMIT),
        name="results",
    )(y, gx, small, gd, gu, stage, r1, r2)


def rope_tables():
    inv_freq = (ROPE_BASE ** (-2.0 * np.arange(HH, dtype=np.float32) / HD)).astype(np.float32)
    angles = np.outer(inv_freq, np.arange(S, dtype=np.float32))
    return np.cos(angles), np.sin(angles)


def solution(mesh):
    no = None
    act_spec = P('dp', 'tp', no)
    rep, part = P(no), P('dp')
    in_specs = (act_spec, act_spec, P('dp', no), rep, rep, P(no, no, 'tp', no), P(no, 'tp', no),
                P('tp', no, no), rep, rep, rep, P(no, 'tp'), P('tp'), P('tp', no), rep)
    out_specs = (act_spec, act_spec, part, part, P('dp', no, 'tp', no), P('dp', 'tp', no), P(('dp', 'tp'), no, no),
                 part, part, part, P('dp', 'tp'), P(('dp', 'tp')), P(('dp', 'tp'), no), part)

    def device_step(x_in, grad_y, pad_mask, ln1_gain, ln1_bias, w_qkv, b_qkv, w_out, b_out, ln2_gain, ln2_bias, w_up, b_up, w_down, b_down):
        assert x_in.shape == (TP * NS, SL, D) and w_qkv.shape == (3, D, 2, HD) and w_up.shape == (D, FB)
        row = lambda v: v.reshape(1, -1)
        wq = w_qkv.transpose(0, 2, 3, 1).reshape(R3, D)
        cos, sin = rope_tables()
        parts = layer_call(
            x_in, grad_y, wq, w_out.reshape(PW, D), w_up, w_down, b_qkv, row(b_up), pad_mask, cos, sin,
            row(ln1_gain), row(ln1_bias), row(ln2_gain), row(ln2_bias), row(b_out), row(b_down))
        y, gx, gd, gu, gq, go, gbq, gbu, *vecs = final_call(*parts)
        g1, b1, bo, g2, b2, bd = (v.reshape(D) for v in vecs)
        return (y, gx, g1, b1, gq.reshape(3, 2, HD, D).transpose(0, 3, 1, 2), gbq, go.reshape(2, HD, D), bo, g2, b2,
                gu, gbu.reshape(FB), gd, bd)

    return jax.shard_map(device_step, mesh=mesh, in_specs=in_specs, out_specs=out_specs, check_vma=False)
```

```python
import functools

import jax
import jax.numpy as jnp
import numpy as np
from jax import lax
from jax.experimental import pallas as pl
from jax.experimental.pallas import tpu as pltpu
from jax.sharding import PartitionSpec as P

f32 = jnp.float32
bf16 = jnp.bfloat16
LN_EPS = 1e-5
ROPE_BASE = 10000.0
INV_SQRT2 = 0.7071067811865476
INV_SQRT_2PI = 0.3989422804014327
NEG_LARGE = -1e30
MESH = pl.DeviceIdType.MESH
ANY = pl.BlockSpec(memory_space=pl.ANY)
VMEM_LIMIT = 66_000_000

TP = 8
NS = 4
S = 512
D = 1024
PW = 128
HD = 64
HH = HD // 2
FB = 512
SL = 64
QS = HD ** -0.5
R3 = 3 * PW


def dg(a, b, ca, cb):
    return lax.dot_general(a, b, (((ca,), (cb,)), ((), ())), preferred_element_type=f32)


def nn(a, b):
    return dg(a, b, 1, 0)


def nt(a, b):
    return dg(a, b, 1, 1)


def tn(a, b):
    return dg(a, b, 0, 0)


def over_rows(reduce, v):
    return reduce(v, axis=0, keepdims=True)


def over_cols(reduce, v):
    return reduce(v, axis=1, keepdims=True)


def sds(shape, dtype):
    return jax.ShapeDtypeStruct(shape, dtype)


class Place:
    def __init__(self):
        me = lax.axis_index("tp")
        self.me = me
        self.c = lax.rem(me, 2)
        self.dc = 1 - 2 * self.c
        self.dx = 2 - 4 * lax.rem(lax.div(me, 2), 2)
        self.dy = 4 - 8 * lax.div(me, 4)
        self.partner = me + self.dc
        self.a = me + (1 - self.c) * self.dx + self.c * self.dy
        self.b = me + (1 - self.c) * self.dy + self.c * self.dx

    def peer(self, m):
        return self.me + (m & 1) * self.dc + ((m >> 1) & 1) * self.dx + (m >> 2) * self.dy

    def slot_of(self, m):
        k = self.c if m % 2 == 0 else 1 - self.c
        lo, hi = {0: (6, 7), 1: (0, 5), 2: (4, 1), 3: (2, 3)}[m >> 1]
        return lo + k * (hi - lo)


def remote(src, dst, send_sem, recv_sem, device):
    return pltpu.make_async_remote_copy(src_ref=src, dst_ref=dst, send_sem=send_sem, recv_sem=recv_sem,
                                        device_id={"tp": device}, device_id_type=MESH)


def wait_for(ref, sem):
    pltpu.make_async_copy(ref, ref, sem).wait()


def entry_barrier(pc):
    bar = pltpu.get_barrier_semaphore()
    for m in range(1, TP):
        pl.semaphore_signal(bar, inc=1, device_id={"tp": pc.peer(m)}, device_id_type=MESH)
    pl.semaphore_wait(bar, TP - 1)


class AllToAll:
    def __init__(self, pc, pos_ref, seq_ref, send_sem, recv_sem, inward):
        self.pc, self.pos, self.seq, self.ss, self.rs, self.inward = pc, pos_ref, seq_ref, send_sem, recv_sem, inward

    def _rows(self, dev):
        return pl.ds(pl.multiple_of(dev * SL, SL), SL)

    def _copy(self, s, m):
        pc, dev = self.pc, self.pc.peer(m)
        if self.inward:
            src, dst = self.pos.at[dev * NS + s], self.seq.at[s, self._rows(pc.me)]
        else:
            src, dst = self.seq.at[s, self._rows(dev)], self.pos.at[pc.me * NS + s]
        return remote(src, dst, self.ss.at[s], self.rs.at[s], dev)

    def start(self, s):
        for m in (2, 3, 4, 5, 6, 7, 1):
            self._copy(s, m).start()

    def finish(self, s):
        all_rows = self.seq.at[s, pl.ds(0, S - SL)]
        wait_for(all_rows, self.ss.at[s])
        wait_for(all_rows, self.rs.at[s])

    def local_in(self, buf):
        pc = self.pc
        return (pltpu.make_async_copy(self.pos.at[pl.ds(pc.me * NS, NS)], buf, self.ss.at[NS]),
                pltpu.make_async_copy(buf, self.seq.at[:, self._rows(pc.me)], self.rs.at[NS]))

    def local_out(self, s, src):
        return pltpu.make_async_copy(src.at[s, self._rows(self.pc.me)], self.pos.at[self.pc.me * NS + s], self.ss.at[NS])


class Gather:
    def __init__(self, pc, src_ref, dst_ref, send_sem, recv_sem):
        self.pc, self.src, self.dst, self.ss, self.rs = pc, src_ref, dst_ref, send_sem, recv_sem

    def _send(self, src, slot, dev):
        return remote(src, self.dst.at[slot], self.ss, self.rs.at[slot], dev)

    def _direct(self):
        pc, c = self.pc, self.pc.c
        return [self._send(self.src, c, pc.a), self._send(self.src, 6 + c, pc.partner),
                self._send(self.src, 4 + c, pc.b)]

    def _hop(self):
        pc, c = self.pc, self.pc.c
        return [self._send(self.dst.at[c], 2 + c, pc.b), self._send(self.dst.at[c], c, pc.partner),
                self._send(self.dst.at[4 + c], 4 + c, pc.partner)]

    def _last(self):
        pc, c = self.pc, self.pc.c
        return self._send(self.dst.at[2 + c], 2 + c, pc.partner)

    def arrived(self, slot):
        wait_for(self.dst.at[slot], self.rs.at[slot])

    def start(self):
        self.start_a()
        self.start_b()

    def start_a(self):
        for cp in self._direct()[:2]:
            cp.start()

    def start_b(self):
        self._direct()[2].start()

    def forward(self):
        self.forward_a()
        self.forward_b()

    def forward_a(self):
        hop = self._hop()
        self.arrived(self.pc.c)
        hop[0].start()
        hop[1].start()

    def forward_b(self):
        self.arrived(4 + self.pc.c)
        self._hop()[2].start()

    def last(self):
        self.arrived(2 + self.pc.c)
        self._last().start()

    def local(self, buf):
        return (pltpu.make_async_copy(self.src, buf, self.rs.at[TP]),
                pltpu.make_async_copy(buf, self.dst.at[6 + self.pc.c], self.rs.at[6 + self.pc.c]))

    def arrived_near(self):
        for j in (0, 2, 3):
            self.arrived(2 * j + 1 - self.pc.c)
        self.arrived(6 + self.pc.c)

    def arrived_far(self):
        self.arrived(3 - self.pc.c)

    def sent(self):
        wait_for(self.dst.at[pl.ds(0, TP - 1)], self.ss)


def row_add(acc, others):
    step = 64

    def body(i, carry):
        r = pl.ds(pl.multiple_of(i * step, step), step)
        v = acc[r, :]
        for o in others:
            v = v + o[r, :]
        acc[r, :] = v
        return carry

    lax.fori_loop(0, acc.shape[0] // step, body, 0)


class GradScatter:
    def __init__(self, pc, acc, landing, stage, r1, r2, sems, free):
        self.pc, self.acc, self.landing, self.stage, self.r1, self.r2 = pc, acc, landing, stage, r1, r2
        self.sem, self.free = sems, free

    def _pair(self, b):
        return remote(self.acc.at[b], self.landing, self.sem.at[0], self.sem.at[1], self.pc.partner)

    def _first(self, j):
        return remote(self.stage.at[j], self.r1.at[j], self.sem.at[2 + j], self.sem.at[4 + j], self.pc.a)

    def _second(self):
        return remote(self.stage.at[2], self.r2, self.sem.at[6], self.sem.at[7], self.pc.b)

    def block_done(self, slot, b, needs_credit):
        @pl.when(lax.rem(slot, 2) != self.pc.c)
        def _():
            @pl.when(needs_credit)
            def _():
                pl.semaphore_wait(self.free, 1)

            self._pair(b).start()

    def settle(self, slot, b, gives_credit):
        c = self.pc.c
        own = lax.rem(slot, 2) == c
        j = lax.div(slot, 2)

        @pl.when(own)
        def _():
            wait_for(self.landing, self.sem.at[1])
            row_add(self.acc.at[b], [self.landing])

            @pl.when(gives_credit)
            def _():
                pl.semaphore_signal(self.free, inc=1, device_id={"tp": self.pc.partner}, device_id_type=MESH)

            store = pltpu.make_async_copy(self.acc.at[b], self.stage.at[j], self.sem.at[8])
            store.start()
            store.wait()

            @pl.when(j < 2)
            def _():
                self._first(j).start()

        @pl.when(jnp.logical_not(own))
        def _():
            self._pair(b).wait_send()

    def second(self, bufs, chunk_sem):
        n = chunk_sem.shape[1]
        size = bufs[0].shape[0]
        rows = size // n
        part = lambda ref, k: ref.at[pl.ds(k * rows, rows)]
        wait_for(self.r1.at[1], self.sem.at[5])
        for p in range(self.r2.shape[0] // size):
            mine, theirs = (ref.at[pl.ds(p * size, size)] for ref in (self.stage.at[2], self.r1.at[1]))
            loads = [[pltpu.make_async_copy(part(src, k), part(buf, k), chunk_sem.at[x, k])
                      for x, (src, buf) in enumerate(zip((mine, theirs), bufs))] for k in range(n)]
            stores = [pltpu.make_async_copy(part(bufs[0], k), part(mine, k), chunk_sem.at[2, k]) for k in range(n)]
            for group in loads:
                for cp in group:
                    cp.start()
            for k in range(n):
                for cp in loads[k]:
                    cp.wait()
                row_add(part(bufs[0], k), [part(bufs[1], k)])
                stores[k].start()
            for cp in stores:
                cp.wait()
        self._second().start()

    def own_part(self, b0, b1, sem):
        wait_for(self.r1.at[0], self.sem.at[4])
        for cp in load_all([(self.stage.at[3], b0), (self.r1.at[0], b1)], sem):
            cp.wait()
        row_add(b0, [b1])
        cp = pltpu.make_async_copy(b0, self.stage.at[3], sem.at[0])
        cp.start()
        cp.wait()

    def finish(self):
        for j in range(2):
            self._first(j).wait_send()
        self._second().wait()


def ln_stats(v):
    c = v - over_cols(jnp.mean, v)
    inv = lax.rsqrt(over_cols(jnp.mean, c * c) + LN_EPS)
    return c * inv, inv


def ln_grad(d_out, x_hat, inv, gain):
    dh = d_out * gain
    return inv * (dh - over_cols(jnp.mean, dh) - x_hat * over_cols(jnp.mean, dh * x_hat))


def masked_scores(q, k, ok):
    return jnp.where(ok, tn(k, q), NEG_LARGE)


def key_mask(mask):
    return jnp.concatenate([mask] * (S // PW), axis=1) > 0


def column(row):
    return jnp.broadcast_to(row, (128, row.shape[1])).T[:, :1]


def clear(*refs):
    for ref in refs:
        ref[...] = jnp.zeros(ref.shape, ref.dtype)


def load_all(pairs, sem):
    cps = [pltpu.make_async_copy(s, d, sem.at[i]) for i, (s, d) in enumerate(pairs)]
    for cp in cps:
        cp.start()
    return cps


def vm(*shape, dtype=f32):
    return pltpu.VMEM(shape, dtype)


TT = 1024
NT = NS * S // TT
SMALL = {
    "bqkv": vm(3, 2, HD), "bup": vm(1, FB), "pad": vm(TP * NS, S, dtype=jnp.int32), "cos": vm(HH, S), "sin": vm(HH, S),
    "gain1": vm(1, D), "bias1": vm(1, D), "gain2": vm(1, D), "bias2": vm(1, D), "b_out": vm(1, D), "b_down": vm(1, D),
}
IN_NAMES = ("x_in", "dy_in", "wq", "wo", "wu", "wd") + tuple("in_" + k for k in SMALL)
OUT_SHAPES = {
    "y_out": ((TP * NS, SL, D), bf16), "gx_out": ((TP * NS, SL, D), bf16), "msgs": ((TP // 2, 8, D), f32), "gd": ((FB, D), f32), "gu": ((D, FB), f32),
    "a_stage": ((4, R3 + PW, D), f32), "a_r2": ((R3 + PW, D), f32), "a_r1": ((2, R3 + PW, D), f32),
    "m_stage": ((4, 2 * FB, D), f32), "m_r1": ((2, 2 * FB, D), f32), "m_r2": ((2 * FB, D), f32),
    "xs": ((NS, S, D), bf16), "dys": ((NS, S, D), bf16), "wq_all": ((TP, R3, D), bf16), "wo_all": ((TP, PW, D), bf16),
    "wu_all": ((TP, D, FB), bf16), "wd_all": ((TP, FB, D), bf16),
    "qkv": ((NS, TP, R3, S), bf16), "ml": ((NS, TP, 4, S), f32), "o": ((NS, TP, PW, S), bf16),
    "x1": ((NS, S, D), bf16), "y_seq": ((NS, S, D), bf16),
}
DMA = pltpu.SemaphoreType.DMA
SCRATCH = SMALL | {
    "in_sem": DMA((len(SMALL),)),
    "bs_all": vm(TP, 8, 128), "bs": vm(8, 128), "mask": vm(NS, S, PW), "dacc": vm(NS * S, D), "landing": vm(2 * FB, D), "gbu": vm(TP, 1, FB), "va": vm(8, D),
    "msg": vm(TP, 8, D), "msg_in": vm(TP, 8, D),
    "free": pltpu.SemaphoreType.REGULAR,
    "x_ss": DMA((NS + 1,)), "x_rs": DMA((NS + 1,)), "dy_ss": DMA((NS + 1,)), "dy_rs": DMA((NS + 1,)),
    "y_ss": DMA((NS + 1,)), "y_rs": DMA((NS + 1,)), "gx_ss": DMA((NS + 1,)), "gx_rs": DMA((NS + 1,)),
    "g_ss": DMA((5,)), "g_rs": DMA((5, TP + 1)), "m_sem": DMA((9,)), "a_sem": DMA((9,)), "s_ss": DMA((3,)), "s_rs": DMA((2,)),
    "tmp": DMA((8,)), "chunk": DMA((3, 4)), "w_sem": DMA((2, 2)),
}


class Refs:
    def __init__(self, names, refs):
        for n, r in zip(names, refs):
            setattr(self, n, r)


def layer_kernel(*refs):
    r = Refs(IN_NAMES + tuple(OUT_SHAPES) + tuple(SCRATCH), refs)
    pc = Place()
    small_in = load_all([(getattr(r, "in_" + k), getattr(r, k)) for k in SMALL], r.in_sem)
    entry_barrier(pc)
    x_a2a = AllToAll(pc, r.x_in, r.xs, r.x_ss, r.x_rs, True)
    dy_a2a = AllToAll(pc, r.dy_in, r.dys, r.dy_ss, r.dy_rs, True)
    y_a2a = AllToAll(pc, r.y_out, r.y_seq, r.y_ss, r.y_rs, False)
    g_bs, g_wq, g_wo, g_wu, g_wd = [
        Gather(pc, s, d, r.g_ss.at[i], r.g_rs.at[i])
        for i, (s, d) in enumerate(((r.bs, r.bs_all), (r.wq, r.wq_all), (r.wo, r.wo_all), (r.wu, r.wu_all), (r.wd, r.wd_all)))]
    gain1, bias1, gain2, bias2, b_out, b_down = r.gain1, r.bias1, r.gain2, r.bias2, r.b_out, r.b_down

    def arrivals(b_x, b_dy, b_q, b_o, b_u, b_d):
        first = (g_bs, g_wq, g_wo)
        for g in first[1:]:
            g.start()
        x_a2a.start(0)
        for cp in small_in:
            cp.wait()
        for i in range(3):
            for h in range(2):
                r.bs[pl.ds(i, 1), pl.ds(h * HD, HD)] = r.bqkv[i, pl.ds(h, 1), :]
        for k in range(FB // PW):
            r.bs[pl.ds(4 + k, 1), :] = r.bup[:, pl.ds(k * PW, PW)]
        local = [x_a2a.local_in(b_x), dy_a2a.local_in(b_dy)]
        local += [g.local(b) for g, b in ((g_wq, b_q), (g_wo, b_o), (g_wu, b_u), (g_wd, b_d))]
        for load, _ in local:
            load.start()
        for s in range(NS):
            keys = jnp.broadcast_to(r.pad[pl.ds(pc.me * NS + s, 1), :].astype(f32), (PW, S))
            r.mask[s] = keys.T
        g_bs.start()
        pltpu.make_async_copy(r.bs, r.bs_all.at[6 + pc.c], r.g_rs.at[0, 6 + pc.c]).start()
        for load, store in local:
            load.wait()
            store.start()
        for g in (g_wq, g_wo, g_bs):
            g.forward_a()
        for g in (g_wq, g_wo, g_bs):
            g.forward_b()
        x_a2a.finish(0)
        x_a2a.start(1)
        for g in first:
            g.arrived_near()
        for g in (g_wu, g_wd):
            g.arrived(6 + pc.c)
        local[0][1].wait()
        local[1][1].wait()

    def later_arrivals():
        for g in (g_bs, g_wq, g_wo):
            g.last()
        for s in range(2, NS):
            x_a2a.start(s)
        for s in range(NS):
            dy_a2a.start(s)
        g_wu.start_a()
        g_wd.start_a()
        for g in (g_bs, g_wq, g_wo):
            g.arrived_far()

    act = vm(NS, SL, D, dtype=bf16)
    pl.run_scoped(arrivals, act, act, vm(R3, D, dtype=bf16), vm(PW, D, dtype=bf16), vm(D, FB, dtype=bf16), vm(FB, D, dtype=bf16))

    def attn_fwd(h2_v, wq_v, wo_v, h1_s, o_s):
        def fetch(*pairs):
            for cp in load_all(pairs, r.tmp):
                cp.wait()

        fetch(*[(r.wq_all.at[pl.ds(k, 2)], wq_v.at[pl.ds(k, 2)]) for k in (6, 0, 4)])

        def slot_at(n):
            return jnp.where(n < 2, n + 6, jnp.where(n < 4, n - 2, jnp.where(n < 6, n, n - 4)))

        def body(x_ref, qkv_ref, ml_ref, o_ref, x1_ref):
            s, n = pl.program_id(0), pl.program_id(1)
            g = slot_at(n)

            @pl.when(n == 0)
            def _():
                xh, _ = ln_stats(x_ref[0].astype(f32))
                h1_s[...] = (xh * gain1[...] + bias1[...]).astype(bf16)

            bias = r.bs_all[g]
            bias = jnp.concatenate([column(bias[i:i + 1]) for i in range(3)], axis=0)
            qkv = nt(wq_v[g], h1_s[...]) + bias
            cos, sin = r.cos[...], r.sin[...]
            ok = key_mask(r.mask[s])

            def rot(t):
                a, b = t[:HH], t[HH:]
                return jnp.concatenate([a * cos - b * sin, b * cos + a * sin], axis=0).astype(bf16)

            for h in range(2):
                lo = h * HD
                at_q, at_k, at_v = (slice(j * PW + lo, j * PW + lo + HD) for j in range(3))
                q, k, v = rot(qkv[at_q] * QS), rot(qkv[at_k]), qkv[at_v].astype(bf16)
                for at, t in ((at_q, q), (at_k, k), (at_v, v)):
                    qkv_ref[0, 0, at, :] = t
                sc = masked_scores(q, k, ok)
                m = over_rows(jnp.max, sc)
                e = jnp.exp(sc - m)
                li = 1.0 / over_rows(jnp.sum, e)
                p = (e * li).astype(bf16)
                ml_ref[0, 0, h:h + 1, :] = m
                ml_ref[0, 0, 2 + h:3 + h, :] = li
                o = nn(v, p).astype(bf16)
                o_ref[0, 0, lo:lo + HD, :] = o
                o_s[pl.ds(pl.multiple_of(g * PW + lo, HD), HD), :] = o

            @pl.when((s == 0) & (n == 5))
            def _():
                later_arrivals()
                fetch((r.wq_all.at[pl.ds(2, 2)], wq_v.at[pl.ds(2, 2)]), (r.wo_all, wo_v))

            @pl.when(n == TP - 1)
            def _():
                attn = tn(o_s[...], wo_v[...].reshape(TP * PW, D))
                x1 = (x_ref[0].astype(f32) + (attn + b_out[...])).astype(bf16)
                x1_ref[0] = x1
                xh, _ = ln_stats(x1.astype(f32))
                h2_v[pl.ds(pl.multiple_of(s * S, S), S), :] = (xh * gain2[...] + bias2[...]).astype(bf16)

            for k in range(1, NS):
                @pl.when((s == k - 1) & (n == TP - 2))
                def _():
                    x_a2a.finish(k)

        seq = pl.BlockSpec((1, S, D), lambda s, n: (s, 0, 0))
        pair = lambda rows: pl.BlockSpec((1, 1, rows, S), lambda s, n: (s, slot_at(n), 0, 0))
        pltpu.emit_pipeline(body, grid=(NS, TP), in_specs=[seq], out_specs=[pair(R3), pair(4), pair(PW), seq])(
            r.xs, r.qkv, r.ml, r.o, r.x1)

    def mlp(h2_v, dy_v, wu_v, wd_v, yacc, acc):
        rs = GradScatter(pc, acc, r.landing, r.m_stage, r.m_r1, r.m_r2, r.m_sem, r.free)

        def slot_at(i):
            return jnp.where(i == 0, 6, jnp.where(i == 5, 7, i - 1 - lax.div(i, 6)))
        def weights(slot, b):
            return (pltpu.make_async_copy(r.wu_all.at[slot], wu_v.at[b], r.w_sem.at[0, b]),
                    pltpu.make_async_copy(r.wd_all.at[slot], wd_v.at[b], r.w_sem.at[1, b]))

        def fetch(i):
            slot = slot_at(i)

            @pl.when(lax.rem(slot, 2) != pc.c)
            def _():
                g_wu.arrived(slot)
                g_wd.arrived(slot)

            for cp in weights(slot, lax.rem(i, 2)):
                cp.start()

        fetch(jnp.int32(0))
        cps = []
        for s in range(NS):
            dy_a2a.finish(s)
            cps.append(pltpu.make_async_copy(r.dys.at[s], dy_v.at[pl.ds(s * S, S)], r.tmp.at[s]))
            cps[s].start()
        clear(yacc, r.dacc, r.gbu)
        for cp in cps:
            cp.wait()

        def step(n, carry):
            i, t = lax.div(n, NT), lax.rem(n, NT)
            b = lax.rem(i, 2)
            slot = slot_at(i)

            @pl.when(t == 0)
            def _():
                for cp in weights(slot, b):
                    cp.wait()
                clear(acc.at[b])

            @pl.when((t == NT - 1) & (i != 0) & (i != 2) & (i < TP - 1))
            def _():
                fetch(i + 1)

            rows = pl.ds(pl.multiple_of(t * TT, TT), TT)
            h2, dy = h2_v[rows, :], dy_v[rows, :]
            wu, wd = wu_v[b], wd_v[b]
            bias = r.bs_all[slot]
            bias = jnp.concatenate([bias[k:k + 1] for k in range(4, TP)], axis=1)
            pre = nn(h2, wu) + bias
            d_act = nt(dy, wd)
            cdf = 0.5 * (1.0 + lax.erf(pre * INV_SQRT2))
            act = (pre * cdf).astype(bf16)
            d_pre = d_act * (cdf + pre * jnp.exp(-0.5 * pre * pre) * INV_SQRT_2PI)
            d_pre_b = d_pre.astype(bf16)
            yacc[rows, :] += nn(act, wd)
            r.dacc[rows, :] += nt(d_pre_b, wu)
            acc[b, :FB, :] += tn(act, dy)
            acc[b, FB:, :] += tn(d_pre_b, h2)
            r.gbu[slot] += over_rows(jnp.sum, d_pre)

            @pl.when(t == NT - 1)
            def _():
                rs.block_done(slot, b, i > 2 * (1 - pc.c))

            @pl.when((t == 0) & (i > 0))
            def _():
                rs.settle(slot_at(i - 1), 1 - b, True)

            for when, hops in ((1, ("forward_a", "start_b")), (4, ("last",)), (5, ()), (9, ("forward_b",))):
                @pl.when(n == when)
                def _():
                    for hop in hops:
                        for gather in (g_wu, g_wd):
                            getattr(gather, hop)()
                    if when in (1, 5):
                        fetch(i + 1)

            return carry

        lax.fori_loop(0, TP * NT, step, 0)
        cps = load_all([(r.x1.at[s], h2_v.at[pl.ds(s * S, S)]) for s in range(NS)], r.tmp)
        stores = []
        for s in range(NS):
            rows = pl.ds(s * S, S)
            cps[s].wait()
            dy_v[rows, :] = (h2_v[rows, :].astype(f32) + (yacc[rows, :] + b_down[...])).astype(bf16)
            cp = pltpu.make_async_copy(dy_v.at[rows], r.y_seq.at[s], r.tmp.at[NS + s])
            cp.start()
            stores.append(cp)
        for s in range(NS):
            stores[s].wait()
            y_a2a.start(s)
        last = jnp.int32(TP - 1)
        rs.settle(slot_at(last), lax.rem(last, 2), True)

    tok = vm(NS * S, D, dtype=bf16)

    def forward_and_mlp(h2_v, dy_v, wu_v, wd_v):
        pl.run_scoped(functools.partial(attn_fwd, h2_v), vm(TP, R3, D, dtype=bf16), vm(TP, PW, D, dtype=bf16),
                      vm(S, D, dtype=bf16), vm(D, S, dtype=bf16))
        pl.run_scoped(functools.partial(mlp, h2_v, dy_v, wu_v, wd_v), vm(NS * S, D), vm(2, 2 * FB, D))

    pl.run_scoped(forward_and_mlp, tok, tok, vm(2, D, FB, dtype=bf16), vm(2, FB, D, dtype=bf16))

    rs_m = GradScatter(pc, None, None, r.m_stage, r.m_r1, r.m_r2, r.m_sem, r.free)

    def attn_bwd(h1_s, do_s, acc, gb_a):
        gx_a2a = AllToAll(pc, r.gx_out, h1_s, r.gx_ss, r.gx_rs, False)

        def open_bwd(wo_v):
            wo_cp = pltpu.make_async_copy(r.wo_all, wo_v, r.tmp.at[0])
            wo_cp.start()
            wo_cp.wait()
            clear(r.va, acc, gb_a)

            def body(x_ref, x1_ref, dy_ref, o_ref):
                s = pl.program_id(0)
                rows = pl.ds(pl.multiple_of(s * S, S), S)
                dy, dh2 = dy_ref[0].astype(f32), r.dacc[rows, :]
                xh2, inv2 = ln_stats(x1_ref[0].astype(f32))
                d = dy + ln_grad(dh2, xh2, inv2, gain2[...])
                r.dacc[rows, :] = d
                db = d.astype(bf16)
                r.va[0:1, :] += over_rows(jnp.sum, dy)
                r.va[1:2, :] += over_rows(jnp.sum, dh2 * xh2)
                r.va[2:3, :] += over_rows(jnp.sum, dh2)
                r.va[3:4, :] += over_rows(jnp.sum, d)
                xh, _ = ln_stats(x_ref[0].astype(f32))
                h1_s[s] = (xh * gain1[...] + bias1[...]).astype(bf16)
                do_s[s] = nt(wo_v[...].reshape(TP * PW, D), db).astype(bf16)
                acc[:, R3:, :] += nn(o_ref[0].reshape(TP * PW, S), db).reshape(TP, PW, D)

            seq = pl.BlockSpec((1, S, D), lambda s: (s, 0, 0))
            pltpu.emit_pipeline(body, grid=(NS,), in_specs=[seq, seq, seq, pl.BlockSpec((1, TP, PW, S), lambda s: (s, 0, 0, 0))])(
                r.xs, r.x1, r.dys, r.o)

        pl.run_scoped(open_bwd, vm(TP, PW, D, dtype=bf16))
        n_half = NS // 2
        rs = GradScatter(pc, acc, r.landing.at[pl.ds(0, R3 + PW)], r.a_stage, r.a_r1, r.a_r2, r.a_sem, r.free)

        def slot_at(g):
            return jnp.where(g < 4, lax.rem(g + 2, 4), g)

        def heads(dq_s, wq_v, buf):
            wq_cp = pltpu.make_async_copy(r.wq_all, wq_v, r.tmp.at[1])
            wq_cp.start()
            for half in range(2):
                def body(qkv_ref, ml_ref):
                    n, sh = pl.program_id(0), pl.program_id(1)
                    g = slot_at(n)
                    s = half * n_half + sh
                    cos, sin = r.cos[...], r.sin[...]
                    ok = key_mask(r.mask[s])

                    def rot_back(t):
                        a, b = t[:HH], t[HH:]
                        return jnp.concatenate([a * cos + b * sin, b * cos - a * sin], axis=0)

                    base = pl.multiple_of(g * R3, PW)
                    for h in range(2):
                        lo = h * HD
                        q, k, v = (qkv_ref[0, 0, j * PW + lo:j * PW + lo + HD, :] for j in range(3))
                        do = do_s[s, pl.ds(pl.multiple_of(g * PW + lo, HD), HD), :]
                        sc = masked_scores(q, k, ok)
                        p = jnp.exp(sc - ml_ref[0, 0, h:h + 1, :]) * ml_ref[0, 0, 2 + h:3 + h, :]
                        dp = tn(v, do)
                        ds = (p * (dp - over_rows(jnp.sum, dp * p))).astype(bf16)
                        dv = nt(p.astype(bf16), do).T
                        dk = rot_back(nt(ds, q).T)
                        dq = rot_back(nn(k, ds)) * QS
                        for j, t in enumerate((dq, dk, dv)):
                            at = pl.ds(base + j * PW + lo, HD)
                            dq_s[sh, at, :] = t.astype(bf16)
                            gb_a[at, :] += over_cols(jnp.sum, t)

                    acc[g, :R3, :] += nn(dq_s[sh, pl.ds(base, R3), :], h1_s[s])
                    if half == 0:
                        @pl.when((sh == 0) & (n == 1))
                        def _():
                            rs_m.second([buf, r.landing.at[pl.ds(FB, FB)]], r.chunk)
                    else:
                        @pl.when(sh == n_half - 1)
                        def _():
                            rs.block_done(g, g, True)

                            @pl.when(n > 0)
                            def _():
                                rs.settle(slot_at(n - 1), slot_at(n - 1), n < TP - 1)

                pair = lambda rows: pl.BlockSpec((1, 1, rows, S), lambda n, sh: (half * n_half + sh, slot_at(n), 0, 0))
                pltpu.emit_pipeline(body, grid=(TP, n_half), in_specs=[pair(R3), pair(4)])(r.qkv, r.ml)
                if half == 0:
                    wq_cp.wait()

                def close_bwd(x_ref):
                    sh = pl.program_id(0)
                    s = half * n_half + sh
                    rows = pl.ds(pl.multiple_of(s * S, S), S)
                    dh1 = tn(dq_s[sh], wq_v[...].reshape(TP * R3, D))
                    xh, inv = ln_stats(x_ref[0].astype(f32))
                    r.va[4:5, :] += over_rows(jnp.sum, dh1 * xh)
                    r.va[5:6, :] += over_rows(jnp.sum, dh1)
                    h1_s[s] = (r.dacc[rows, :] + ln_grad(dh1, xh, inv, gain1[...])).astype(bf16)
                    gx_a2a.start(s)
                    cp = gx_a2a.local_out(s, h1_s)
                    cp.start()
                    cp.wait()

                pltpu.emit_pipeline(close_bwd, grid=(n_half,),
                                    in_specs=[pl.BlockSpec((1, S, D), lambda sh: (half * n_half + sh, 0, 0))])(r.xs)
            last = jnp.int32(TP - 1)
            rs.settle(last, last, False)
            rs.second([buf, r.landing.at[pl.ds(FB, FB)]], r.chunk)

        pl.run_scoped(heads, vm(n_half, TP * R3, S, dtype=bf16), vm(TP, R3, D, dtype=bf16), vm(FB, D))

        for g in range(TP):
            r.msg[g] = r.va[...]
            for j in range(3):
                cols = jnp.broadcast_to(gb_a[g * R3 + j * PW:g * R3 + (j + 1) * PW, :], (PW, 128))
                r.msg[g, 6:7, j * PW:(j + 1) * PW] = cols.T[0:1, :]
            r.msg[g, 6:7, R3:R3 + FB] = r.gbu[g]
        pair = remote(r.msg, r.msg_in, r.s_ss.at[0], r.s_rs.at[0], pc.partner)
        pair.start()
        pair.wait()
        r.msg_in[...] = r.msg_in[...] + r.msg[...]
        chip = lax.div(pc.me, 2)
        small = [remote(r.msg_in.at[pc.slot_of(m)], r.msgs.at[chip], r.s_ss.at[1], r.s_rs.at[1], pc.peer(m)) for m in (2, 4, 6)]
        for cp in small:
            cp.start()
        own = pltpu.make_async_copy(r.msg_in.at[pc.slot_of(0)], r.msgs.at[chip], r.s_ss.at[2])
        own.start()

        def tail(bufs, act_v, turned):
            b0, b1, b2 = (bufs.at[i] for i in range(3))
            y_own = [(pltpu.make_async_copy(r.y_seq.at[s, y_a2a._rows(pc.me)], act_v.at[s], r.tmp.at[s]),
                      pltpu.make_async_copy(act_v.at[s], r.y_out.at[pc.me * NS + s], r.tmp.at[NS + s])) for s in range(NS)]
            for load, _ in y_own:
                load.start()
            for load, store in y_own:
                load.wait()
                store.start()
            for g in (g_bs, g_wq, g_wo, g_wu, g_wd):
                g.sent()
            for _, store in y_own:
                store.wait()
            rs_m.finish()
            wait_for(r.m_r1.at[0], r.m_sem.at[4])
            for p in range(2):
                half = pl.ds(p * FB, FB)
                for cp in load_all([(r.m_stage.at[3, half], b0), (r.m_r1.at[0, half], b1), (r.m_r2.at[half], b2)], r.tmp):
                    cp.wait()
                row_add(b0, [b1, b2])
                if p == 0:
                    cp = pltpu.make_async_copy(b0, r.gd, r.tmp.at[0])
                else:
                    for k in range(D // FB):
                        cols = slice(k * FB, (k + 1) * FB)
                        turned[cols, :] = b0[:, cols].T
                    cp = pltpu.make_async_copy(turned, r.gu, r.tmp.at[0])
                cp.start()
                cp.wait()
            rs.own_part(b0, b1, r.tmp)
            for s in range(NS):
                y_a2a.finish(s)
            for s in range(NS):
                gx_a2a.finish(s)
            rs.finish()
            own.wait()
            for sem in (r.s_ss.at[1], r.s_rs.at[1]):
                wait_for(r.msgs.at[pl.ds(0, len(small))], sem)

        pl.run_scoped(tail, vm(3, FB, D), vm(NS, SL, D, dtype=bf16), vm(D, FB))

    seqs = vm(NS, S, D, dtype=bf16)
    pl.run_scoped(attn_bwd, seqs, vm(NS, D, S, dtype=bf16), vm(TP, R3 + PW, D), vm(TP * R3, 1))


def layer_call(*args):
    out = pl.pallas_call(
        layer_kernel,
        in_specs=[ANY] * len(IN_NAMES),
        out_specs=[ANY] * len(OUT_SHAPES),
        out_shape=[sds(*v) for v in OUT_SHAPES.values()],
        scratch_shapes=list(SCRATCH.values()),
        compiler_params=pltpu.CompilerParams(collective_id=0, has_side_effects=True, vmem_limit_bytes=VMEM_LIMIT),
        name="layer",
    )(*args)
    return out[:7]


FINAL = {"y": ((TP * NS, SL, D), bf16), "gx": ((TP * NS, SL, D), bf16), "gd": ((FB, D), f32), "gu": ((D, FB), f32),
         "gq": ((R3, D), f32), "go": ((PW, D), f32), "gbq": ((3, 2, HD), f32), "gbu": ((1, FB), f32)}
VECS = ("bd", "g2", "b2", "bo", "g1", "b1")
FINAL |= {k: ((1, D), f32) for k in VECS}
LATE = ("gbq", "gbu") + VECS


def final_kernel(y_in, gx_in, msgs, gd_in, gu_in, stage, r2, *refs):
    outs, refs = Refs(FINAL, refs), refs[len(FINAL):]
    msg_v, y_v, gx_v, gd_v, gu_v, sums, ld, st = refs[:8]
    late = Refs(LATE, refs[8:])
    moves = [([(msgs, msg_v)], [])]
    moves.append(([(t, sums.at[x]) for x, t in enumerate((stage.at[3], r2))],
                  [(sums.at[0, pl.ds(0, R3)], outs.gq), (sums.at[0, pl.ds(R3, PW)], outs.go)]))
    for src, buf, dst in ((gd_in, gd_v, outs.gd), (gu_in, gu_v, outs.gu), (y_in, y_v, outs.y), (gx_in, gx_v, outs.gx)):
        moves.append(([(src, buf)], [(buf, dst)]))
    copy = pltpu.make_async_copy
    loads = [[copy(s, d, ld.at[i, x]) for x, (s, d) in enumerate(m[0])] for i, m in enumerate(moves)]
    stores = [[copy(s, d, st.at[i, x]) for x, (s, d) in enumerate(m[1])] for i, m in enumerate(moves)]
    for cps in loads:
        for cp in cps:
            cp.start()
    for i, (cps, outward) in enumerate(zip(loads, stores)):
        for cp in cps:
            cp.wait()
        if i == 0:
            small = msg_v[0]
            for j in range(1, msg_v.shape[0]):
                small = small + msg_v[j]
            for j, k in enumerate(VECS):
                getattr(late, k)[...] = small[j:j + 1, :]
            for j in range(3):
                for h in range(2):
                    lo = j * PW + h * HD
                    late.gbq[j, h:h + 1, :] = small[6:7, lo:lo + HD]
            late.gbu[...] = small[6:7, R3:R3 + FB]
        if i == 1:
            row_add(sums.at[0], [sums.at[1]])
        for cp in outward:
            cp.start()
    small_out = load_all([(getattr(late, k), getattr(outs, k)) for k in LATE], st.at[len(moves)])
    for cps in stores + [small_out]:
        for cp in cps:
            cp.wait()


def final_call(y, gx, msgs, gd, gu, stage, r2):
    act = vm(*y.shape, dtype=bf16)
    return pl.pallas_call(
        final_kernel,
        in_specs=[ANY] * 7,
        out_specs=[ANY] * len(FINAL),
        out_shape=[sds(*v) for v in FINAL.values()],
        scratch_shapes=[vm(*msgs.shape), act, act, vm(FB, D), vm(D, FB), vm(2, R3 + PW, D), DMA((6, 2)), DMA((7, len(LATE)))]
        + [vm(*FINAL[k][0]) for k in LATE],
        compiler_params=pltpu.CompilerParams(vmem_limit_bytes=VMEM_LIMIT),
        name="results",
    )(y, gx, msgs, gd, gu, stage, r2)


def rope_tables():
    inv_freq = (ROPE_BASE ** (-2.0 * np.arange(HH, dtype=np.float32) / HD)).astype(np.float32)
    angles = np.outer(inv_freq, np.arange(S, dtype=np.float32))
    return np.cos(angles), np.sin(angles)


def solution(mesh):
    no = None
    act_spec = P('dp', 'tp', no)
    rep, part = P(no), P('dp')
    in_specs = (act_spec, act_spec, P('dp', no), rep, rep, P(no, no, 'tp', no), P(no, 'tp', no),
                P('tp', no, no), rep, rep, rep, P(no, 'tp'), P('tp'), P('tp', no), rep)
    out_specs = (act_spec, act_spec, part, part, P('dp', no, 'tp', no), P('dp', 'tp', no), P(('dp', 'tp'), no, no),
                 part, part, part, P('dp', 'tp'), P(('dp', 'tp')), P(('dp', 'tp'), no), part)

    def device_step(x_in, grad_y, pad_mask, ln1_gain, ln1_bias, w_qkv, b_qkv, w_out, b_out, ln2_gain, ln2_bias, w_up, b_up, w_down, b_down):
        assert x_in.shape == (TP * NS, SL, D) and w_qkv.shape == (3, D, 2, HD) and w_up.shape == (D, FB)
        row = lambda v: v.reshape(1, -1)
        wq = w_qkv.transpose(0, 2, 3, 1).reshape(R3, D)
        cos, sin = rope_tables()
        parts = layer_call(
            x_in, grad_y, wq, w_out.reshape(PW, D), w_up, w_down, b_qkv, row(b_up), pad_mask, cos, sin,
            row(ln1_gain), row(ln1_bias), row(ln2_gain), row(ln2_bias), row(b_out), row(b_down))
        y, gx, gd, gu, gq, go, gbq, gbu, *vecs = final_call(*parts)
        bd, g2, b2, bo, g1, b1 = (v.reshape(D) for v in vecs)
        return (y, gx, g1, b1, gq.reshape(3, 2, HD, D).transpose(0, 3, 1, 2), gbq, go.reshape(2, HD, D), bo, g2, b2,
                gu, gbu.reshape(FB), gd, bd)

    return jax.shard_map(device_step, mesh=mesh, in_specs=in_specs, out_specs=out_specs, check_vma=False)
```

```python
import functools

import jax
import jax.numpy as jnp
import numpy as np
from jax import lax
from jax.experimental import pallas as pl
from jax.experimental.pallas import tpu as pltpu
from jax.sharding import PartitionSpec as P

f32 = jnp.float32
bf16 = jnp.bfloat16
LN_EPS = 1e-5
ROPE_BASE = 10000.0
INV_SQRT2 = 0.7071067811865476
INV_SQRT_2PI = 0.3989422804014327
NEG_LARGE = -1e30
MESH = pl.DeviceIdType.MESH
ANY = pl.BlockSpec(memory_space=pl.ANY)
VMEM_LIMIT = 66_000_000

TP = 8
NS = 4
S = 512
D = 1024
PW = 128
HD = 64
HH = HD // 2
FB = 512
SL = 64
QS = HD ** -0.5
R3 = 3 * PW


def dg(a, b, ca, cb):
    return lax.dot_general(a, b, (((ca,), (cb,)), ((), ())), preferred_element_type=f32)


def nn(a, b):
    return dg(a, b, 1, 0)


def nt(a, b):
    return dg(a, b, 1, 1)


def tn(a, b):
    return dg(a, b, 0, 0)


def over_rows(reduce, v):
    return reduce(v, axis=0, keepdims=True)


def over_cols(reduce, v):
    return reduce(v, axis=1, keepdims=True)


def sds(shape, dtype):
    return jax.ShapeDtypeStruct(shape, dtype)


class Place:
    def __init__(self):
        me = lax.axis_index("tp")
        self.me = me
        self.c = lax.rem(me, 2)
        self.dc = 1 - 2 * self.c
        self.dx = 2 - 4 * lax.rem(lax.div(me, 2), 2)
        self.dy = 4 - 8 * lax.div(me, 4)
        self.partner = me + self.dc
        self.a = me + (1 - self.c) * self.dx + self.c * self.dy
        self.b = me + (1 - self.c) * self.dy + self.c * self.dx

    def peer(self, m):
        return self.me + (m & 1) * self.dc + ((m >> 1) & 1) * self.dx + (m >> 2) * self.dy

    def slot_of(self, m):
        k = self.c if m % 2 == 0 else 1 - self.c
        lo, hi = {0: (6, 7), 1: (0, 5), 2: (4, 1), 3: (2, 3)}[m >> 1]
        return lo + k * (hi - lo)


def remote(src, dst, send_sem, recv_sem, device):
    return pltpu.make_async_remote_copy(src_ref=src, dst_ref=dst, send_sem=send_sem, recv_sem=recv_sem,
                                        device_id={"tp": device}, device_id_type=MESH)


def wait_for(ref, sem):
    pltpu.make_async_copy(ref, ref, sem).wait()


def entry_barrier(pc):
    bar = pltpu.get_barrier_semaphore()
    for m in range(1, TP):
        pl.semaphore_signal(bar, inc=1, device_id={"tp": pc.peer(m)}, device_id_type=MESH)
    pl.semaphore_wait(bar, TP - 1)


class AllToAll:
    def __init__(self, pc, pos_ref, seq_ref, send_sem, recv_sem, inward):
        self.pc, self.pos, self.seq, self.ss, self.rs, self.inward = pc, pos_ref, seq_ref, send_sem, recv_sem, inward

    def _rows(self, dev):
        return pl.ds(pl.multiple_of(dev * SL, SL), SL)

    def _copy(self, s, m):
        pc, dev = self.pc, self.pc.peer(m)
        if self.inward:
            src, dst = self.pos.at[dev * NS + s], self.seq.at[s, self._rows(pc.me)]
        else:
            src, dst = self.seq.at[s, self._rows(dev)], self.pos.at[pc.me * NS + s]
        return remote(src, dst, self.ss.at[s], self.rs.at[s], dev)

    def start(self, s):
        for m in (*range(2, TP), 1):
            self._copy(s, m).start()

    def finish(self, s):
        all_rows = self.seq.at[s, pl.ds(0, S - SL)]
        wait_for(all_rows, self.ss.at[s])
        wait_for(all_rows, self.rs.at[s])

    def local_in(self, buf):
        pc = self.pc
        return (pltpu.make_async_copy(self.pos.at[pl.ds(pc.me * NS, NS)], buf, self.ss.at[NS]),
                pltpu.make_async_copy(buf, self.seq.at[:, self._rows(pc.me)], self.rs.at[NS]))

    def local_out(self, s, src):
        return pltpu.make_async_copy(src.at[s, self._rows(self.pc.me)], self.pos.at[self.pc.me * NS + s], self.ss.at[NS])


class Gather:
    def __init__(self, pc, src_ref, dst_ref, send_sem, recv_sem):
        self.pc, self.src, self.dst, self.ss, self.rs = pc, src_ref, dst_ref, send_sem, recv_sem

    def _send(self, src, slot, dev):
        return remote(src, self.dst.at[slot], self.ss, self.rs.at[slot], dev)

    def _direct(self):
        pc, c = self.pc, self.pc.c
        return [self._send(self.src, c, pc.a), self._send(self.src, 6 + c, pc.partner),
                self._send(self.src, 4 + c, pc.b)]

    def _hop(self):
        pc, c = self.pc, self.pc.c
        return [self._send(self.dst.at[c], 2 + c, pc.b), self._send(self.dst.at[c], c, pc.partner),
                self._send(self.dst.at[4 + c], 4 + c, pc.partner)]

    def _last(self):
        pc, c = self.pc, self.pc.c
        return self._send(self.dst.at[2 + c], 2 + c, pc.partner)

    def arrived(self, slot):
        wait_for(self.dst.at[slot], self.rs.at[slot])

    def start(self):
        self.start_a()
        self.start_b()

    def start_a(self):
        for cp in self._direct()[:2]:
            cp.start()

    def start_b(self):
        self._direct()[2].start()

    def forward(self):
        self.forward_a()
        self.forward_b()

    def forward_a(self):
        hop = self._hop()
        self.arrived(self.pc.c)
        hop[0].start()
        hop[1].start()

    def forward_b(self):
        self.arrived(4 + self.pc.c)
        self._hop()[2].start()

    def last(self):
        self.arrived(2 + self.pc.c)
        self._last().start()

    def local(self, buf):
        return (pltpu.make_async_copy(self.src, buf, self.rs.at[TP]),
                pltpu.make_async_copy(buf, self.dst.at[6 + self.pc.c], self.rs.at[6 + self.pc.c]))

    def arrived_near(self):
        for j in (0, 2, 3):
            self.arrived(2 * j + 1 - self.pc.c)
        self.arrived(6 + self.pc.c)

    def arrived_far(self):
        self.arrived(3 - self.pc.c)

    def sent(self):
        wait_for(self.dst.at[pl.ds(0, TP - 1)], self.ss)


def row_add(acc, others):
    step = 64

    def body(i, carry):
        r = pl.ds(pl.multiple_of(i * step, step), step)
        v = acc[r, :]
        for o in others:
            v = v + o[r, :]
        acc[r, :] = v
        return carry

    lax.fori_loop(0, acc.shape[0] // step, body, 0)


class GradScatter:
    def __init__(self, pc, acc, landing, stage, r1, r2, sems, free):
        self.pc, self.acc, self.landing, self.stage, self.r1, self.r2 = pc, acc, landing, stage, r1, r2
        self.sem, self.free = sems, free

    def _pair(self, b):
        return remote(self.acc.at[b], self.landing, self.sem.at[0], self.sem.at[1], self.pc.partner)

    def _first(self, j):
        return remote(self.stage.at[j], self.r1.at[j], self.sem.at[2 + j], self.sem.at[4 + j], self.pc.a)

    def _second(self):
        return remote(self.stage.at[2], self.r2, self.sem.at[6], self.sem.at[7], self.pc.b)

    def send_pair(self, b, needs_credit):
        @pl.when(needs_credit)
        def _():
            pl.semaphore_wait(self.free, 1)

        self._pair(b).start()

    def sent_pair(self, b):
        self._pair(b).wait_send()

    def settle(self, j, b, landed, gives_credit):
        landed()
        row_add(self.acc.at[b], [self.landing])

        @pl.when(gives_credit)
        def _():
            pl.semaphore_signal(self.free, inc=1, device_id={"tp": self.pc.partner}, device_id_type=MESH)

        store = pltpu.make_async_copy(self.acc.at[b], self.stage.at[j], self.sem.at[8])
        store.start()
        store.wait()

        @pl.when(j < 2)
        def _():
            self._first(j).start()

    def landed(self):
        wait_for(self.landing, self.sem.at[1])

    def block_done(self, slot, b):
        pl.when(lax.rem(slot, 2) != self.pc.c)(lambda: self.send_pair(b, True))

    def later(self, slot, b, gives_credit):
        own = lax.rem(slot, 2) == self.pc.c
        pl.when(own)(lambda: self.settle(lax.div(slot, 2), b, self.landed, gives_credit))
        pl.when(jnp.logical_not(own))(lambda: self.sent_pair(b))

    def second(self, bufs, chunk_sem):
        n = chunk_sem.shape[1]
        size = bufs[0].shape[0]
        rows = size // n
        part = lambda ref, k: ref.at[pl.ds(k * rows, rows)]
        wait_for(self.r1.at[1], self.sem.at[5])
        for p in range(self.r2.shape[0] // size):
            mine, theirs = (ref.at[pl.ds(p * size, size)] for ref in (self.stage.at[2], self.r1.at[1]))
            loads = [[pltpu.make_async_copy(part(src, k), part(buf, k), chunk_sem.at[x, k])
                      for x, (src, buf) in enumerate(zip((mine, theirs), bufs))] for k in range(n)]
            stores = [pltpu.make_async_copy(part(bufs[0], k), part(mine, k), chunk_sem.at[2, k]) for k in range(n)]
            for group in loads:
                for cp in group:
                    cp.start()
            for k in range(n):
                for cp in loads[k]:
                    cp.wait()
                row_add(part(bufs[0], k), [part(bufs[1], k)])
                stores[k].start()
            for cp in stores:
                cp.wait()
        self._second().start()

    def own_part(self, b0, b1, sem):
        wait_for(self.r1.at[0], self.sem.at[4])
        for cp in load_all([(self.stage.at[3], b0), (self.r1.at[0], b1)], sem):
            cp.wait()
        row_add(b0, [b1])
        cp = pltpu.make_async_copy(b0, self.stage.at[3], sem.at[0])
        cp.start()
        cp.wait()

    def finish(self):
        for j in range(2):
            self._first(j).wait_send()
        self._second().wait()


def ln_stats(v):
    c = v - over_cols(jnp.mean, v)
    inv = lax.rsqrt(over_cols(jnp.mean, c * c) + LN_EPS)
    return c * inv, inv


def ln_grad(d_out, x_hat, inv, gain):
    dh = d_out * gain
    return inv * (dh - over_cols(jnp.mean, dh) - x_hat * over_cols(jnp.mean, dh * x_hat))


def masked_scores(q, k, ok):
    return jnp.where(ok, tn(k, q), NEG_LARGE)


def key_mask(mask):
    return jnp.concatenate([mask] * (S // PW), axis=1) > 0


def column(row):
    return jnp.broadcast_to(row, (128, row.shape[1])).T[:, :1]


def clear(*refs):
    for ref in refs:
        ref[...] = jnp.zeros(ref.shape, ref.dtype)


def load_all(pairs, sem):
    cps = [pltpu.make_async_copy(s, d, sem.at[i]) for i, (s, d) in enumerate(pairs)]
    for cp in cps:
        cp.start()
    return cps


def vm(*shape, dtype=f32):
    return pltpu.VMEM(shape, dtype)


TT = 1024
NT = NS * S // TT
SMALL = {
    "bqkv": vm(3, 2, HD), "bup": vm(1, FB), "pad": vm(TP * NS, S, dtype=jnp.int32), "cos": vm(HH, S), "sin": vm(HH, S),
    "gain1": vm(1, D), "bias1": vm(1, D), "gain2": vm(1, D), "bias2": vm(1, D), "b_out": vm(1, D), "b_down": vm(1, D),
}
IN_NAMES = ("x_in", "dy_in", "wq", "wo", "wu", "wd") + tuple("in_" + k for k in SMALL)
OUT_SHAPES = {
    "y_out": ((TP * NS, SL, D), bf16), "gx_out": ((TP * NS, SL, D), bf16), "msgs": ((TP // 2, 8, D), f32), "gd": ((FB, D), f32), "gu": ((D, FB), f32),
    "a_stage": ((4, R3 + PW, D), f32), "a_r2": ((R3 + PW, D), f32), "a_r1": ((2, R3 + PW, D), f32),
    "m_r0": ((2 * FB, D), f32), "m_stage": ((4, 2 * FB, D), f32), "m_r1": ((2, 2 * FB, D), f32), "m_r2": ((2 * FB, D), f32),
    "xs": ((NS, S, D), bf16), "dys": ((NS, S, D), bf16), "wq_all": ((TP, R3, D), bf16), "wo_all": ((TP, PW, D), bf16),
    "wu_all": ((TP, D, FB), bf16), "wd_all": ((TP, FB, D), bf16),
    "qkv": ((NS, TP, R3, S), bf16), "ml": ((NS, TP, 4, S), f32), "o": ((NS, TP, PW, S), bf16),
    "x1": ((NS, S, D), bf16), "y_seq": ((NS, S, D), bf16),
}
DMA = pltpu.SemaphoreType.DMA
SCRATCH = SMALL | {
    "in_sem": DMA((len(SMALL),)),
    "bs_all": vm(TP, 8, 128), "bs": vm(8, 128), "mask": vm(NS, S, PW), "dacc": vm(NS * S, D), "landing": vm(2 * FB, D), "gbu": vm(TP, 1, FB), "va": vm(8, D),
    "msg": vm(TP, 8, D), "msg_in": vm(TP, 8, D),
    "free": pltpu.SemaphoreType.REGULAR,
    "x_ss": DMA((NS + 1,)), "x_rs": DMA((NS + 1,)), "dy_ss": DMA((NS + 1,)), "dy_rs": DMA((NS + 1,)),
    "y_ss": DMA((NS + 1,)), "y_rs": DMA((NS + 1,)), "gx_ss": DMA((NS + 1,)), "gx_rs": DMA((NS + 1,)),
    "g_ss": DMA((5,)), "g_rs": DMA((5, TP + 1)), "m_sem": DMA((11,)), "a_sem": DMA((9,)), "s_ss": DMA((3,)), "s_rs": DMA((2,)),
    "tmp": DMA((8,)), "chunk": DMA((3, 4)), "w_sem": DMA((2, 2)),
}


class Refs:
    def __init__(self, names, refs):
        for n, r in zip(names, refs):
            setattr(self, n, r)


def layer_kernel(*refs):
    r = Refs(IN_NAMES + tuple(OUT_SHAPES) + tuple(SCRATCH), refs)
    pc = Place()
    small_in = load_all([(getattr(r, "in_" + k), getattr(r, k)) for k in SMALL], r.in_sem)
    entry_barrier(pc)
    x_a2a = AllToAll(pc, r.x_in, r.xs, r.x_ss, r.x_rs, True)
    dy_a2a = AllToAll(pc, r.dy_in, r.dys, r.dy_ss, r.dy_rs, True)
    y_a2a = AllToAll(pc, r.y_out, r.y_seq, r.y_ss, r.y_rs, False)
    g_bs, g_wq, g_wo, g_wu, g_wd = [
        Gather(pc, s, d, r.g_ss.at[i], r.g_rs.at[i])
        for i, (s, d) in enumerate(((r.bs, r.bs_all), (r.wq, r.wq_all), (r.wo, r.wo_all), (r.wu, r.wu_all), (r.wd, r.wd_all)))]
    gain1, bias1, gain2, bias2, b_out, b_down = r.gain1, r.bias1, r.gain2, r.bias2, r.b_out, r.b_down

    def arrivals(b_x, b_dy, b_q, b_o, b_u, b_d):
        first = (g_bs, g_wq, g_wo)
        for g in first[1:]:
            g.start()
        x_a2a.start(0)
        for cp in small_in:
            cp.wait()
        for i in range(3):
            for h in range(2):
                r.bs[pl.ds(i, 1), pl.ds(h * HD, HD)] = r.bqkv[i, pl.ds(h, 1), :]
        for k in range(FB // PW):
            r.bs[pl.ds(4 + k, 1), :] = r.bup[:, pl.ds(k * PW, PW)]
        local = [x_a2a.local_in(b_x), dy_a2a.local_in(b_dy)]
        local += [g.local(b) for g, b in ((g_wq, b_q), (g_wo, b_o), (g_wu, b_u), (g_wd, b_d))]
        for load, _ in local:
            load.start()
        for s in range(NS):
            keys = jnp.broadcast_to(r.pad[pl.ds(pc.me * NS + s, 1), :].astype(f32), (PW, S))
            r.mask[s] = keys.T
        g_bs.start()
        pltpu.make_async_copy(r.bs, r.bs_all.at[6 + pc.c], r.g_rs.at[0, 6 + pc.c]).start()
        for load, store in local:
            load.wait()
            store.start()
        for g in (g_wq, g_wo, g_bs):
            g.forward_a()
        for g in (g_wq, g_wo, g_bs):
            g.forward_b()
        x_a2a.finish(0)
        x_a2a.start(1)
        for g in first:
            g.arrived_near()
        for g in (g_wu, g_wd):
            g.arrived(6 + pc.c)
        local[0][1].wait()
        local[1][1].wait()

    def later_arrivals():
        for g in (g_bs, g_wq, g_wo):
            g.last()
        for s in range(2, NS):
            x_a2a.start(s)
        for s in range(NS):
            dy_a2a.start(s)
        g_wu.start_a()
        g_wd.start_a()
        for g in (g_bs, g_wq, g_wo):
            g.arrived_far()

    act = vm(NS, SL, D, dtype=bf16)
    pl.run_scoped(arrivals, act, act, vm(R3, D, dtype=bf16), vm(PW, D, dtype=bf16), vm(D, FB, dtype=bf16), vm(FB, D, dtype=bf16))

    def attn_fwd(h2_v, wq_v, wo_v, h1_s, o_s):
        def fetch(*pairs):
            for cp in load_all(pairs, r.tmp):
                cp.wait()

        fetch(*[(r.wq_all.at[pl.ds(k, 2)], wq_v.at[pl.ds(k, 2)]) for k in (6, 0, 4)])

        def slot_at(n):
            return jnp.where(n < 2, n + 6, jnp.where(n < 4, n - 2, jnp.where(n < 6, n, n - 4)))

        def body(x_ref, qkv_ref, ml_ref, o_ref, x1_ref):
            s, n = pl.program_id(0), pl.program_id(1)
            g = slot_at(n)

            @pl.when(n == 0)
            def _():
                xh, _ = ln_stats(x_ref[0].astype(f32))
                h1_s[...] = (xh * gain1[...] + bias1[...]).astype(bf16)

            bias = r.bs_all[g]
            bias = jnp.concatenate([column(bias[i:i + 1]) for i in range(3)], axis=0)
            qkv = nt(wq_v[g], h1_s[...]) + bias
            cos, sin = r.cos[...], r.sin[...]
            ok = key_mask(r.mask[s])

            def rot(t):
                a, b = t[:HH], t[HH:]
                return jnp.concatenate([a * cos - b * sin, b * cos + a * sin], axis=0).astype(bf16)

            for h in range(2):
                lo = h * HD
                at_q, at_k, at_v = (slice(j * PW + lo, j * PW + lo + HD) for j in range(3))
                q, k, v = rot(qkv[at_q] * QS), rot(qkv[at_k]), qkv[at_v].astype(bf16)
                for at, t in ((at_q, q), (at_k, k), (at_v, v)):
                    qkv_ref[0, 0, at, :] = t
                sc = masked_scores(q, k, ok)
                m = over_rows(jnp.max, sc)
                e = jnp.exp(sc - m)
                li = 1.0 / over_rows(jnp.sum, e)
                p = (e * li).astype(bf16)
                ml_ref[0, 0, h:h + 1, :] = m
                ml_ref[0, 0, 2 + h:3 + h, :] = li
                o = nn(v, p).astype(bf16)
                o_ref[0, 0, lo:lo + HD, :] = o
                o_s[pl.ds(pl.multiple_of(g * PW + lo, HD), HD), :] = o

            @pl.when((s == 0) & (n == 5))
            def _():
                later_arrivals()
                fetch((r.wq_all.at[pl.ds(2, 2)], wq_v.at[pl.ds(2, 2)]), (r.wo_all, wo_v))

            @pl.when(n == TP - 1)
            def _():
                attn = tn(o_s[...], wo_v[...].reshape(TP * PW, D))
                x1 = (x_ref[0].astype(f32) + (attn + b_out[...])).astype(bf16)
                x1_ref[0] = x1
                xh, _ = ln_stats(x1.astype(f32))
                h2_v[pl.ds(pl.multiple_of(s * S, S), S), :] = (xh * gain2[...] + bias2[...]).astype(bf16)

            for k in range(1, NS):
                @pl.when((s == k - 1) & (n == TP - 2))
                def _():
                    x_a2a.finish(k)

        seq = pl.BlockSpec((1, S, D), lambda s, n: (s, 0, 0))
        pair = lambda rows: pl.BlockSpec((1, 1, rows, S), lambda s, n: (s, slot_at(n), 0, 0))
        pltpu.emit_pipeline(body, grid=(NS, TP), in_specs=[seq], out_specs=[pair(R3), pair(4), pair(PW), seq])(
            r.xs, r.qkv, r.ml, r.o, r.x1)

    def mlp(h2_v, dy_v, wu_v, wd_v, yacc, acc):
        rs = GradScatter(pc, acc, r.landing, r.m_stage, r.m_r1, r.m_r2, r.m_sem, r.free)

        def is_own(i):
            return (i == 2) | (i == 4) | (i == 5) | (i == 7)

        def role_at(i):
            return jnp.where((i == 0) | (i == 5), 3, jnp.where(i < 3, 0, jnp.where(i < 5, 1, 2)))

        def slot_at(i):
            return 2 * role_at(i) + jnp.where(is_own(i), pc.c, 1 - pc.c)

        early = lambda b: remote(acc.at[b], r.m_r0, r.m_sem.at[9], r.m_sem.at[10], pc.partner)

        def landed(i):
            @pl.when(i == 5)
            def _():
                wait_for(r.m_r0, r.m_sem.at[10])
                cp = pltpu.make_async_copy(r.m_r0, r.landing, r.tmp.at[0])
                cp.start()
                cp.wait()

            pl.when(i != 5)(rs.landed)

        def weights(slot, b):
            return (pltpu.make_async_copy(r.wu_all.at[slot], wu_v.at[b], r.w_sem.at[0, b]),
                    pltpu.make_async_copy(r.wd_all.at[slot], wd_v.at[b], r.w_sem.at[1, b]))

        def fetch(i):
            slot = slot_at(i)

            @pl.when(jnp.logical_not(is_own(i)))
            def _():
                g_wu.arrived(slot)
                g_wd.arrived(slot)

            for cp in weights(slot, lax.rem(i, 2)):
                cp.start()

        fetch(jnp.int32(0))
        cps = []
        for s in range(NS):
            dy_a2a.finish(s)
            cps.append(pltpu.make_async_copy(r.dys.at[s], dy_v.at[pl.ds(s * S, S)], r.tmp.at[s]))
            cps[s].start()
        clear(yacc, r.dacc, r.gbu)
        for cp in cps:
            cp.wait()

        def step(n, carry):
            i, t = lax.div(n, NT), lax.rem(n, NT)
            b = lax.rem(i, 2)
            slot = slot_at(i)

            @pl.when(t == 0)
            def _():
                for cp in weights(slot, b):
                    cp.wait()
                clear(acc.at[b])

            @pl.when((t == NT - 1) & (i != 0) & (i != 2) & (i < TP - 1))
            def _():
                fetch(i + 1)

            rows = pl.ds(pl.multiple_of(t * TT, TT), TT)
            h2, dy = h2_v[rows, :], dy_v[rows, :]
            wu, wd = wu_v[b], wd_v[b]
            bias = r.bs_all[slot]
            bias = jnp.concatenate([bias[k:k + 1] for k in range(4, TP)], axis=1)
            pre = nn(h2, wu) + bias
            d_act = nt(dy, wd)
            cdf = 0.5 * (1.0 + lax.erf(pre * INV_SQRT2))
            act = (pre * cdf).astype(bf16)
            d_pre = d_act * (cdf + pre * jnp.exp(-0.5 * pre * pre) * INV_SQRT_2PI)
            d_pre_b = d_pre.astype(bf16)
            yacc[rows, :] += nn(act, wd)
            r.dacc[rows, :] += nt(d_pre_b, wu)
            acc[b, :FB, :] += tn(act, dy)
            acc[b, FB:, :] += tn(d_pre_b, h2)
            r.gbu[slot] += over_rows(jnp.sum, d_pre)

            done = (t == NT - 1)
            pl.when(done & (i == 0))(lambda: early(b).start())
            pl.when(done & (i > 0) & jnp.logical_not(is_own(i)))(lambda: rs.send_pair(b, i > 1))
            pl.when(done & is_own(i))(lambda: rs.settle(role_at(i), b, lambda: landed(i), i != 4))
            pl.when((t == 0) & (i == 1))(lambda: early(1 - b).wait_send())
            pl.when((t == 0) & (i > 1) & jnp.logical_not(is_own(i - 1)))(lambda: rs.sent_pair(1 - b))

            for when, hops in ((1, ("forward_a", "start_b")), (4, ("last",)), (5, ()), (9, ("forward_b",))):
                @pl.when(n == when)
                def _():
                    for hop in hops:
                        for gather in (g_wu, g_wd):
                            getattr(gather, hop)()
                    if when in (1, 5):
                        fetch(i + 1)

            return carry

        lax.fori_loop(0, TP * NT, step, 0)
        cps = load_all([(r.x1.at[s], h2_v.at[pl.ds(s * S, S)]) for s in range(NS)], r.tmp)
        stores = []
        for s in range(NS):
            rows = pl.ds(s * S, S)
            cps[s].wait()
            dy_v[rows, :] = (h2_v[rows, :].astype(f32) + (yacc[rows, :] + b_down[...])).astype(bf16)
            cp = pltpu.make_async_copy(dy_v.at[rows], r.y_seq.at[s], r.tmp.at[NS + s])
            cp.start()
            stores.append(cp)
        for s in range(NS):
            stores[s].wait()
            y_a2a.start(s)

    tok = vm(NS * S, D, dtype=bf16)

    def forward_and_mlp(h2_v, dy_v, wu_v, wd_v):
        pl.run_scoped(functools.partial(attn_fwd, h2_v), vm(TP, R3, D, dtype=bf16), vm(TP, PW, D, dtype=bf16),
                      vm(S, D, dtype=bf16), vm(D, S, dtype=bf16))
        pl.run_scoped(functools.partial(mlp, h2_v, dy_v, wu_v, wd_v), vm(NS * S, D), vm(2, 2 * FB, D))

    pl.run_scoped(forward_and_mlp, tok, tok, vm(2, D, FB, dtype=bf16), vm(2, FB, D, dtype=bf16))

    rs_m = GradScatter(pc, None, None, r.m_stage, r.m_r1, r.m_r2, r.m_sem, r.free)

    def attn_bwd(h1_s, do_s, acc, gb_a):
        gx_a2a = AllToAll(pc, r.gx_out, h1_s, r.gx_ss, r.gx_rs, False)

        def open_bwd(wo_v):
            wo_cp = pltpu.make_async_copy(r.wo_all, wo_v, r.tmp.at[0])
            wo_cp.start()
            wo_cp.wait()
            clear(r.va, acc, gb_a)

            def body(x_ref, x1_ref, dy_ref, o_ref):
                s = pl.program_id(0)
                rows = pl.ds(pl.multiple_of(s * S, S), S)
                dy, dh2 = dy_ref[0].astype(f32), r.dacc[rows, :]
                xh2, inv2 = ln_stats(x1_ref[0].astype(f32))
                d = dy + ln_grad(dh2, xh2, inv2, gain2[...])
                r.dacc[rows, :] = d
                db = d.astype(bf16)
                r.va[0:1, :] += over_rows(jnp.sum, dy)
                r.va[1:2, :] += over_rows(jnp.sum, dh2 * xh2)
                r.va[2:3, :] += over_rows(jnp.sum, dh2)
                r.va[3:4, :] += over_rows(jnp.sum, d)
                xh, _ = ln_stats(x_ref[0].astype(f32))
                h1_s[s] = (xh * gain1[...] + bias1[...]).astype(bf16)
                do_s[s] = nt(wo_v[...].reshape(TP * PW, D), db).astype(bf16)
                acc[:, R3:, :] += nn(o_ref[0].reshape(TP * PW, S), db).reshape(TP, PW, D)

            seq = pl.BlockSpec((1, S, D), lambda s: (s, 0, 0))
            pltpu.emit_pipeline(body, grid=(NS,), in_specs=[seq, seq, seq, pl.BlockSpec((1, TP, PW, S), lambda s: (s, 0, 0, 0))])(
                r.xs, r.x1, r.dys, r.o)

        pl.run_scoped(open_bwd, vm(TP, PW, D, dtype=bf16))
        n_half = NS // 2
        rs = GradScatter(pc, acc, r.landing.at[pl.ds(0, R3 + PW)], r.a_stage, r.a_r1, r.a_r2, r.a_sem, r.free)

        def slot_at(g):
            return jnp.where(g < 4, lax.rem(g + 2, 4), g)

        def heads(dq_s, wq_v, buf):
            wq_cp = pltpu.make_async_copy(r.wq_all, wq_v, r.tmp.at[1])
            wq_cp.start()
            for half in range(2):
                def body(qkv_ref, ml_ref):
                    n, sh = pl.program_id(0), pl.program_id(1)
                    g = slot_at(n)
                    s = half * n_half + sh
                    cos, sin = r.cos[...], r.sin[...]
                    ok = key_mask(r.mask[s])

                    def rot_back(t):
                        a, b = t[:HH], t[HH:]
                        return jnp.concatenate([a * cos + b * sin, b * cos - a * sin], axis=0)

                    base = pl.multiple_of(g * R3, PW)
                    for h in range(2):
                        lo = h * HD
                        q, k, v = (qkv_ref[0, 0, j * PW + lo:j * PW + lo + HD, :] for j in range(3))
                        do = do_s[s, pl.ds(pl.multiple_of(g * PW + lo, HD), HD), :]
                        sc = masked_scores(q, k, ok)
                        p = jnp.exp(sc - ml_ref[0, 0, h:h + 1, :]) * ml_ref[0, 0, 2 + h:3 + h, :]
                        dp = tn(v, do)
                        ds = (p * (dp - over_rows(jnp.sum, dp * p))).astype(bf16)
                        dv = nt(p.astype(bf16), do).T
                        dk = rot_back(nt(ds, q).T)
                        dq = rot_back(nn(k, ds)) * QS
                        for j, t in enumerate((dq, dk, dv)):
                            at = pl.ds(base + j * PW + lo, HD)
                            dq_s[sh, at, :] = t.astype(bf16)
                            gb_a[at, :] += over_cols(jnp.sum, t)

                    acc[g, :R3, :] += nn(dq_s[sh, pl.ds(base, R3), :], h1_s[s])
                    if half == 0:
                        @pl.when((sh == 0) & (n == 1))
                        def _():
                            rs_m.second([buf, r.landing.at[pl.ds(FB, FB)]], r.chunk)
                    else:
                        @pl.when(sh == n_half - 1)
                        def _():
                            rs.block_done(g, g)

                            @pl.when(n > 0)
                            def _():
                                rs.later(slot_at(n - 1), slot_at(n - 1), n < TP - 1)

                pair = lambda rows: pl.BlockSpec((1, 1, rows, S), lambda n, sh: (half * n_half + sh, slot_at(n), 0, 0))
                pltpu.emit_pipeline(body, grid=(TP, n_half), in_specs=[pair(R3), pair(4)])(r.qkv, r.ml)
                if half == 0:
                    wq_cp.wait()

                def close_bwd(x_ref):
                    sh = pl.program_id(0)
                    s = half * n_half + sh
                    rows = pl.ds(pl.multiple_of(s * S, S), S)
                    dh1 = tn(dq_s[sh], wq_v[...].reshape(TP * R3, D))
                    xh, inv = ln_stats(x_ref[0].astype(f32))
                    r.va[4:5, :] += over_rows(jnp.sum, dh1 * xh)
                    r.va[5:6, :] += over_rows(jnp.sum, dh1)
                    h1_s[s] = (r.dacc[rows, :] + ln_grad(dh1, xh, inv, gain1[...])).astype(bf16)
                    gx_a2a.start(s)
                    cp = gx_a2a.local_out(s, h1_s)
                    cp.start()
                    cp.wait()

                pltpu.emit_pipeline(close_bwd, grid=(n_half,),
                                    in_specs=[pl.BlockSpec((1, S, D), lambda sh: (half * n_half + sh, 0, 0))])(r.xs)
            last = jnp.int32(TP - 1)
            rs.later(last, last, False)
            rs.second([buf, r.landing.at[pl.ds(FB, FB)]], r.chunk)

        pl.run_scoped(heads, vm(n_half, TP * R3, S, dtype=bf16), vm(TP, R3, D, dtype=bf16), vm(FB, D))

        for g in range(TP):
            r.msg[g] = r.va[...]
            for j in range(3):
                cols = jnp.broadcast_to(gb_a[g * R3 + j * PW:g * R3 + (j + 1) * PW, :], (PW, 128))
                r.msg[g, 6:7, j * PW:(j + 1) * PW] = cols.T[0:1, :]
            r.msg[g, 6:7, R3:R3 + FB] = r.gbu[g]
        pair = remote(r.msg, r.msg_in, r.s_ss.at[0], r.s_rs.at[0], pc.partner)
        pair.start()
        pair.wait()
        r.msg_in[...] = r.msg_in[...] + r.msg[...]
        chip = lax.div(pc.me, 2)
        small = [remote(r.msg_in.at[pc.slot_of(m)], r.msgs.at[chip], r.s_ss.at[1], r.s_rs.at[1], pc.peer(m)) for m in (2, 4, 6)]
        for cp in small:
            cp.start()
        own = pltpu.make_async_copy(r.msg_in.at[pc.slot_of(0)], r.msgs.at[chip], r.s_ss.at[2])
        own.start()

        def tail(bufs, act_v, turned):
            b0, b1, b2 = (bufs.at[i] for i in range(3))
            y_own = [(pltpu.make_async_copy(r.y_seq.at[s, y_a2a._rows(pc.me)], act_v.at[s], r.tmp.at[s]),
                      pltpu.make_async_copy(act_v.at[s], r.y_out.at[pc.me * NS + s], r.tmp.at[NS + s])) for s in range(NS)]
            for load, _ in y_own:
                load.start()
            for load, store in y_own:
                load.wait()
                store.start()
            for g in (g_bs, g_wq, g_wo, g_wu, g_wd):
                g.sent()
            for _, store in y_own:
                store.wait()
            rs_m.finish()
            wait_for(r.m_r1.at[0], r.m_sem.at[4])
            for p in range(2):
                half = pl.ds(p * FB, FB)
                for cp in load_all([(r.m_stage.at[3, half], b0), (r.m_r1.at[0, half], b1), (r.m_r2.at[half], b2)], r.tmp):
                    cp.wait()
                row_add(b0, [b1, b2])
                if p == 0:
                    cp = pltpu.make_async_copy(b0, r.gd, r.tmp.at[0])
                else:
                    for k in range(D // FB):
                        cols = slice(k * FB, (k + 1) * FB)
                        turned[cols, :] = b0[:, cols].T
                    cp = pltpu.make_async_copy(turned, r.gu, r.tmp.at[0])
                cp.start()
                cp.wait()
            rs.own_part(b0, b1, r.tmp)
            for s in range(NS):
                y_a2a.finish(s)
            for s in range(NS):
                gx_a2a.finish(s)
            rs.finish()
            own.wait()
            for sem in (r.s_ss.at[1], r.s_rs.at[1]):
                wait_for(r.msgs.at[pl.ds(0, len(small))], sem)

        pl.run_scoped(tail, vm(3, FB, D), vm(NS, SL, D, dtype=bf16), vm(D, FB))

    seqs = vm(NS, S, D, dtype=bf16)
    pl.run_scoped(attn_bwd, seqs, vm(NS, D, S, dtype=bf16), vm(TP, R3 + PW, D), vm(TP * R3, 1))


def layer_call(*args):
    out = pl.pallas_call(
        layer_kernel,
        in_specs=[ANY] * len(IN_NAMES),
        out_specs=[ANY] * len(OUT_SHAPES),
        out_shape=[sds(*v) for v in OUT_SHAPES.values()],
        scratch_shapes=list(SCRATCH.values()),
        compiler_params=pltpu.CompilerParams(collective_id=0, has_side_effects=True, vmem_limit_bytes=VMEM_LIMIT),
        name="layer",
    )(*args)
    return out[:7]


FINAL = {"y": ((TP * NS, SL, D), bf16), "gx": ((TP * NS, SL, D), bf16), "gd": ((FB, D), f32), "gu": ((D, FB), f32),
         "gq": ((R3, D), f32), "go": ((PW, D), f32), "gbq": ((3, 2, HD), f32), "gbu": ((1, FB), f32)}
VECS = ("bd", "g2", "b2", "bo", "g1", "b1")
FINAL |= {k: ((1, D), f32) for k in VECS}
LATE = ("gbq", "gbu") + VECS


def final_kernel(y_in, gx_in, msgs, gd_in, gu_in, stage, r2, *refs):
    outs, refs = Refs(FINAL, refs), refs[len(FINAL):]
    msg_v, y_v, gx_v, gd_v, gu_v, sums, ld, st = refs[:8]
    late = Refs(LATE, refs[8:])
    moves = [([(msgs, msg_v)], [])]
    moves.append(([(t, sums.at[x]) for x, t in enumerate((stage.at[3], r2))],
                  [(sums.at[0, pl.ds(0, R3)], outs.gq), (sums.at[0, pl.ds(R3, PW)], outs.go)]))
    for src, buf, dst in ((gd_in, gd_v, outs.gd), (gu_in, gu_v, outs.gu), (y_in, y_v, outs.y), (gx_in, gx_v, outs.gx)):
        moves.append(([(src, buf)], [(buf, dst)]))
    copy = pltpu.make_async_copy
    loads = [[copy(s, d, ld.at[i, x]) for x, (s, d) in enumerate(m[0])] for i, m in enumerate(moves)]
    stores = [[copy(s, d, st.at[i, x]) for x, (s, d) in enumerate(m[1])] for i, m in enumerate(moves)]
    for cps in loads:
        for cp in cps:
            cp.start()
    for i, (cps, outward) in enumerate(zip(loads, stores)):
        for cp in cps:
            cp.wait()
        if i == 0:
            small = msg_v[0]
            for j in range(1, msg_v.shape[0]):
                small = small + msg_v[j]
            for j, k in enumerate(VECS):
                getattr(late, k)[...] = small[j:j + 1, :]
            for j in range(3):
                for h in range(2):
                    lo = j * PW + h * HD
                    late.gbq[j, h:h + 1, :] = small[6:7, lo:lo + HD]
            late.gbu[...] = small[6:7, R3:R3 + FB]
        if i == 1:
            row_add(sums.at[0], [sums.at[1]])
        for cp in outward:
            cp.start()
    small_out = load_all([(getattr(late, k), getattr(outs, k)) for k in LATE], st.at[len(moves)])
    for cps in stores + [small_out]:
        for cp in cps:
            cp.wait()


def final_call(y, gx, msgs, gd, gu, stage, r2):
    act = vm(*y.shape, dtype=bf16)
    return pl.pallas_call(
        final_kernel,
        in_specs=[ANY] * 7,
        out_specs=[ANY] * len(FINAL),
        out_shape=[sds(*v) for v in FINAL.values()],
        scratch_shapes=[vm(*msgs.shape), act, act, vm(FB, D), vm(D, FB), vm(2, R3 + PW, D), DMA((6, 2)), DMA((7, len(LATE)))]
        + [vm(*FINAL[k][0]) for k in LATE],
        compiler_params=pltpu.CompilerParams(vmem_limit_bytes=VMEM_LIMIT),
        name="results",
    )(y, gx, msgs, gd, gu, stage, r2)


def rope_tables():
    inv_freq = (ROPE_BASE ** (-2.0 * np.arange(HH, dtype=np.float32) / HD)).astype(np.float32)
    angles = np.outer(inv_freq, np.arange(S, dtype=np.float32))
    return np.cos(angles), np.sin(angles)


def solution(mesh):
    no = None
    act_spec = P('dp', 'tp', no)
    rep, part = P(no), P('dp')
    in_specs = (act_spec, act_spec, P('dp', no), rep, rep, P(no, no, 'tp', no), P(no, 'tp', no),
                P('tp', no, no), rep, rep, rep, P(no, 'tp'), P('tp'), P('tp', no), rep)
    out_specs = (act_spec, act_spec, part, part, P('dp', no, 'tp', no), P('dp', 'tp', no), P(('dp', 'tp'), no, no),
                 part, part, part, P('dp', 'tp'), P(('dp', 'tp')), P(('dp', 'tp'), no), part)

    def device_step(x_in, grad_y, pad_mask, ln1_gain, ln1_bias, w_qkv, b_qkv, w_out, b_out, ln2_gain, ln2_bias, w_up, b_up, w_down, b_down):
        assert x_in.shape == (TP * NS, SL, D) and w_qkv.shape == (3, D, 2, HD) and w_up.shape == (D, FB)
        row = lambda v: v.reshape(1, -1)
        wq = w_qkv.transpose(0, 2, 3, 1).reshape(R3, D)
        cos, sin = rope_tables()
        parts = layer_call(
            x_in, grad_y, wq, w_out.reshape(PW, D), w_up, w_down, b_qkv, row(b_up), pad_mask, cos, sin,
            row(ln1_gain), row(ln1_bias), row(ln2_gain), row(ln2_bias), row(b_out), row(b_down))
        y, gx, gd, gu, gq, go, gbq, gbu, *vecs = final_call(*parts)
        bd, g2, b2, bo, g1, b1 = (v.reshape(D) for v in vecs)
        return (y, gx, g1, b1, gq.reshape(3, 2, HD, D).transpose(0, 3, 1, 2), gbq, go.reshape(2, HD, D), bo, g2, b2,
                gu, gbu.reshape(FB), gd, bd)

    return jax.shard_map(device_step, mesh=mesh, in_specs=in_specs, out_specs=out_specs, check_vma=False)
```

```python
import functools

import jax
import jax.numpy as jnp
import numpy as np
from jax import lax
from jax.experimental import pallas as pl
from jax.experimental.pallas import tpu as pltpu
from jax.sharding import PartitionSpec as P

f32 = jnp.float32
bf16 = jnp.bfloat16
LN_EPS = 1e-5
ROPE_BASE = 10000.0
INV_SQRT2 = 0.7071067811865476
INV_SQRT_2PI = 0.3989422804014327
NEG_LARGE = -1e30
MESH = pl.DeviceIdType.MESH
ANY = pl.BlockSpec(memory_space=pl.ANY)
VMEM_LIMIT = 66_000_000

TP = 8
NS = 4
S = 512
D = 1024
PW = 128
HD = 64
HH = HD // 2
FB = 512
SL = 64
QS = HD ** -0.5
R3 = 3 * PW
ROWS = 8


def dg(a, b, ca, cb):
    return lax.dot_general(a, b, (((ca,), (cb,)), ((), ())), preferred_element_type=f32)


def nn(a, b):
    return dg(a, b, 1, 0)


def nt(a, b):
    return dg(a, b, 1, 1)


def tn(a, b):
    return dg(a, b, 0, 0)


def over_rows(reduce, v):
    return reduce(v, axis=0, keepdims=True)


def over_cols(reduce, v):
    return reduce(v, axis=1, keepdims=True)


def sds(shape, dtype):
    return jax.ShapeDtypeStruct(shape, dtype)


class Place:
    def __init__(self):
        me = lax.axis_index("tp")
        self.me = me
        self.c = lax.rem(me, 2)
        self.dc = 1 - 2 * self.c
        self.dx = 2 - 4 * lax.rem(lax.div(me, 2), 2)
        self.dy = 4 - 8 * lax.div(me, 4)
        self.partner = me + self.dc
        self.a = me + (1 - self.c) * self.dx + self.c * self.dy
        self.b = me + (1 - self.c) * self.dy + self.c * self.dx

    def peer(self, m):
        return self.me + (m & 1) * self.dc + ((m >> 1) & 1) * self.dx + (m >> 2) * self.dy

    def slot_of(self, m):
        k = self.c if m % 2 == 0 else 1 - self.c
        lo, hi = {0: (6, 7), 1: (0, 5), 2: (4, 1), 3: (2, 3)}[m >> 1]
        return lo + k * (hi - lo)


def remote(src, dst, send_sem, recv_sem, device):
    return pltpu.make_async_remote_copy(src_ref=src, dst_ref=dst, send_sem=send_sem, recv_sem=recv_sem,
                                        device_id={"tp": device}, device_id_type=MESH)


def wait_for(ref, sem):
    pltpu.make_async_copy(ref, ref, sem).wait()


def entry_barrier(pc):
    bar = pltpu.get_barrier_semaphore()
    for m in range(1, TP):
        pl.semaphore_signal(bar, inc=1, device_id={"tp": pc.peer(m)}, device_id_type=MESH)
    pl.semaphore_wait(bar, TP - 1)


class AllToAll:
    def __init__(self, pc, pos_ref, seq_ref, send_sem, recv_sem, inward):
        self.pc, self.pos, self.seq, self.ss, self.rs, self.inward = pc, pos_ref, seq_ref, send_sem, recv_sem, inward

    def _rows(self, dev):
        return pl.ds(pl.multiple_of(dev * SL, SL), SL)

    def _copy(self, s, m):
        pc, dev = self.pc, self.pc.peer(m)
        if self.inward:
            src, dst = self.pos.at[dev * NS + s], self.seq.at[s, self._rows(pc.me)]
        else:
            src, dst = self.seq.at[s, self._rows(dev)], self.pos.at[pc.me * NS + s]
        return remote(src, dst, self.ss.at[s], self.rs.at[s], dev)

    def start(self, s):
        for m in (*range(2, TP), 1):
            self._copy(s, m).start()

    def finish(self, s):
        all_rows = self.seq.at[s, pl.ds(0, S - SL)]
        wait_for(all_rows, self.ss.at[s])
        wait_for(all_rows, self.rs.at[s])

    def local_in(self, buf):
        pc = self.pc
        return (pltpu.make_async_copy(self.pos.at[pl.ds(pc.me * NS, NS)], buf, self.ss.at[NS]),
                pltpu.make_async_copy(buf, self.seq.at[:, self._rows(pc.me)], self.rs.at[NS]))

    def local_out(self, s, src):
        return pltpu.make_async_copy(src.at[s, self._rows(self.pc.me)], self.pos.at[self.pc.me * NS + s], self.ss.at[NS])


class Gather:
    def __init__(self, pc, src_ref, dst_ref, send_sem, recv_sem):
        self.pc, self.src, self.dst, self.ss, self.rs = pc, src_ref, dst_ref, send_sem, recv_sem

    def _send(self, src, slot, dev):
        return remote(src, self.dst.at[slot], self.ss, self.rs.at[slot], dev)

    def _direct(self):
        pc, c = self.pc, self.pc.c
        return [self._send(self.src, c, pc.a), self._send(self.src, 6 + c, pc.partner),
                self._send(self.src, 4 + c, pc.b)]

    def _hop(self):
        pc, c = self.pc, self.pc.c
        return [self._send(self.dst.at[c], 2 + c, pc.b), self._send(self.dst.at[c], c, pc.partner),
                self._send(self.dst.at[4 + c], 4 + c, pc.partner)]

    def _last(self):
        pc, c = self.pc, self.pc.c
        return self._send(self.dst.at[2 + c], 2 + c, pc.partner)

    def arrived(self, slot):
        wait_for(self.dst.at[slot], self.rs.at[slot])

    def start(self):
        self.start_a()
        self.start_b()

    def start_a(self):
        for cp in self._direct()[:2]:
            cp.start()

    def start_b(self):
        self._direct()[2].start()

    def forward(self):
        self.forward_a()
        self.forward_b()

    def forward_a(self):
        hop = self._hop()
        self.arrived(self.pc.c)
        hop[0].start()
        hop[1].start()

    def forward_b(self):
        self.arrived(4 + self.pc.c)
        self._hop()[2].start()

    def last(self):
        self.arrived(2 + self.pc.c)
        self._last().start()

    def local(self, buf):
        return (pltpu.make_async_copy(self.src, buf, self.rs.at[TP]),
                pltpu.make_async_copy(buf, self.dst.at[6 + self.pc.c], self.rs.at[6 + self.pc.c]))

    def arrived_near(self):
        for j in (0, 2, 3):
            self.arrived(2 * j + 1 - self.pc.c)
        self.arrived(6 + self.pc.c)

    def arrived_far(self):
        self.arrived(3 - self.pc.c)

    def sent(self):
        wait_for(self.dst.at[pl.ds(0, TP - 1)], self.ss)


def row_add(acc, others):
    step = 64

    def body(i, carry):
        r = pl.ds(pl.multiple_of(i * step, step), step)
        v = acc[r, :]
        for o in others:
            v = v + o[r, :]
        acc[r, :] = v
        return carry

    lax.fori_loop(0, acc.shape[0] // step, body, 0)


class GradScatter:
    def __init__(self, pc, acc, landing, stage, r1, r2, sems, free):
        self.pc, self.acc, self.landing, self.stage, self.r1, self.r2 = pc, acc, landing, stage, r1, r2
        self.sem, self.free = sems, free

    def _pair(self, b):
        return remote(self.acc.at[b], self.landing, self.sem.at[0], self.sem.at[1], self.pc.partner)

    def _first(self, j):
        return remote(self.stage.at[j], self.r1.at[j], self.sem.at[2 + j], self.sem.at[4 + j], self.pc.a)

    def _second(self):
        rows = self.r2.shape[0]
        src = self.stage.at[2, pl.ds(self.stage.shape[1] - rows, rows)]
        return remote(src, self.r2, self.sem.at[6], self.sem.at[7], self.pc.b)

    def send_pair(self, b, needs_credit):
        @pl.when(needs_credit)
        def _():
            pl.semaphore_wait(self.free, 1)

        self._pair(b).start()

    def sent_pair(self, b):
        self._pair(b).wait_send()

    def settle(self, j, b, landed, gives_credit):
        landed()
        row_add(self.acc.at[b], [self.landing])

        @pl.when(gives_credit)
        def _():
            pl.semaphore_signal(self.free, inc=1, device_id={"tp": self.pc.partner}, device_id_type=MESH)

        store = pltpu.make_async_copy(self.acc.at[b], self.stage.at[j], self.sem.at[8])
        store.start()
        store.wait()

        @pl.when(j < 2)
        def _():
            self._first(j).start()

    def landed(self):
        wait_for(self.landing, self.sem.at[1])

    def block_done(self, slot, b):
        pl.when(lax.rem(slot, 2) != self.pc.c)(lambda: self.send_pair(b, True))

    def later(self, slot, b, gives_credit):
        own = lax.rem(slot, 2) == self.pc.c
        pl.when(own)(lambda: self.settle(lax.div(slot, 2), b, self.landed, gives_credit))
        pl.when(jnp.logical_not(own))(lambda: self.sent_pair(b))

    def second(self, bufs, chunk_sem, lead=None):
        n = chunk_sem.shape[1]
        size = bufs[0].shape[0]
        rows = size // n
        part = lambda ref, k: ref.at[pl.ds(k * rows, rows)]
        wait_for(self.r1.at[1], self.sem.at[5])
        for p in range(self.stage.shape[1] // size):
            mine, theirs = (ref.at[pl.ds(p * size, size)] for ref in (self.stage.at[2], self.r1.at[1]))
            loads = [[pltpu.make_async_copy(part(src, k), part(buf, k), chunk_sem.at[x, k])
                      for x, (src, buf) in enumerate(zip((mine, theirs), bufs))] for k in range(n)]
            to_lead = 0 if lead is None else lead.shape[0] // rows
            stores = [pltpu.make_async_copy(part(bufs[0], k), part(lead if k < to_lead else mine, k), chunk_sem.at[2, k])
                      for k in range(n)]
            for group in loads:
                for cp in group:
                    cp.start()
            for k in range(n):
                for cp in loads[k]:
                    cp.wait()
                row_add(part(bufs[0], k), [part(bufs[1], k)])
                stores[k].start()
            for cp in stores:
                cp.wait()
        self._second().start()

    def own_part(self, b0, b1, sem):
        wait_for(self.r1.at[0], self.sem.at[4])
        for cp in load_all([(self.stage.at[3], b0), (self.r1.at[0], b1)], sem):
            cp.wait()
        row_add(b0, [b1])
        cp = pltpu.make_async_copy(b0, self.stage.at[3], sem.at[0])
        cp.start()
        cp.wait()

    def finish(self):
        for j in range(2):
            self._first(j).wait_send()
        self._second().wait()


def ln_stats(v):
    c = v - over_cols(jnp.mean, v)
    inv = lax.rsqrt(over_cols(jnp.mean, c * c) + LN_EPS)
    return c * inv, inv


def ln_grad(d_out, x_hat, inv, gain):
    dh = d_out * gain
    return inv * (dh - over_cols(jnp.mean, dh) - x_hat * over_cols(jnp.mean, dh * x_hat))


def masked_scores(q, k, ok):
    return jnp.where(ok, tn(k, q), NEG_LARGE)


def key_mask(mask):
    return jnp.concatenate([mask] * (S // PW), axis=1) > 0


def column(row):
    return jnp.broadcast_to(row, (PW, row.shape[1])).T[:, :1]


def clear(*refs):
    for ref in refs:
        ref[...] = jnp.zeros(ref.shape, ref.dtype)


def load_all(pairs, sem):
    cps = [pltpu.make_async_copy(s, d, sem.at[i]) for i, (s, d) in enumerate(pairs)]
    for cp in cps:
        cp.start()
    return cps


def vm(*shape, dtype=f32):
    return pltpu.VMEM(shape, dtype)


TT = 1024
NT = NS * S // TT
SMALL = {
    "bqkv": vm(3, 2, HD), "bup": vm(1, FB), "pad": vm(TP * NS, S, dtype=jnp.int32), "cos": vm(HH, S), "sin": vm(HH, S),
    "gain1": vm(1, D), "bias1": vm(1, D), "gain2": vm(1, D), "bias2": vm(1, D), "b_out": vm(1, D), "b_down": vm(1, D),
}
IN_NAMES = ("x_in", "dy_in", "wq", "wo", "wu", "wd") + tuple("in_" + k for k in SMALL)
OUT_SHAPES = {
    "y_out": ((TP * NS, SL, D), bf16), "gx_out": ((TP * NS, SL, D), bf16), "msgs": ((TP // 2, ROWS, D), f32), "gd": ((FB, D), f32), "gu": ((D, FB), f32),
    "a_stage": ((4, R3 + PW, D), f32), "a_r2": ((PW, D), f32), "gq_b": ((R3, D), f32), "a_r1": ((2, R3 + PW, D), f32),
    "m_r0": ((2 * FB, D), f32), "m_stage": ((4, 2 * FB, D), f32), "m_r1": ((2, 2 * FB, D), f32), "m_r2": ((2 * FB, D), f32),
    "xs": ((NS, S, D), bf16), "dys": ((NS, S, D), bf16), "wq_all": ((TP, R3, D), bf16), "wo_all": ((TP, PW, D), bf16),
    "wu_all": ((TP, D, FB), bf16), "wd_all": ((TP, FB, D), bf16),
    "qkv": ((NS, TP, R3, S), bf16), "ml": ((NS, TP, 4, S), f32), "o": ((NS, TP, PW, S), bf16),
    "x1": ((NS, S, D), bf16), "y_seq": ((NS, S, D), bf16),
}
DMA = pltpu.SemaphoreType.DMA
SCRATCH = SMALL | {
    "in_sem": DMA((len(SMALL),)),
    "bs_all": vm(TP, ROWS, PW), "bs": vm(ROWS, PW), "mask": vm(NS, S, PW), "dacc": vm(NS * S, D), "landing": vm(2 * FB, D), "gbu": vm(TP, 1, FB), "va": vm(ROWS, D),
    "msg": vm(TP, ROWS, D), "msg_in": vm(TP, ROWS, D),
    "free": pltpu.SemaphoreType.REGULAR,
    "x_ss": DMA((NS + 1,)), "x_rs": DMA((NS + 1,)), "dy_ss": DMA((NS + 1,)), "dy_rs": DMA((NS + 1,)),
    "y_ss": DMA((NS + 1,)), "y_rs": DMA((NS + 1,)), "gx_ss": DMA((NS + 1,)), "gx_rs": DMA((NS + 1,)),
    "g_ss": DMA((5,)), "g_rs": DMA((5, TP + 1)), "m_sem": DMA((11,)), "a_sem": DMA((9,)), "s_ss": DMA((3,)), "s_rs": DMA((2,)),
    "tmp": DMA((TP,)), "chunk": DMA((3, 4)), "w_sem": DMA((2, 2)),
}


class Refs:
    def __init__(self, names, refs):
        for n, r in zip(names, refs):
            setattr(self, n, r)


def layer_kernel(*refs):
    r = Refs(IN_NAMES + tuple(OUT_SHAPES) + tuple(SCRATCH), refs)
    pc = Place()
    small_in = load_all([(getattr(r, "in_" + k), getattr(r, k)) for k in SMALL], r.in_sem)
    entry_barrier(pc)
    x_a2a = AllToAll(pc, r.x_in, r.xs, r.x_ss, r.x_rs, True)
    dy_a2a = AllToAll(pc, r.dy_in, r.dys, r.dy_ss, r.dy_rs, True)
    y_a2a = AllToAll(pc, r.y_out, r.y_seq, r.y_ss, r.y_rs, False)
    g_bs, g_wq, g_wo, g_wu, g_wd = [
        Gather(pc, s, d, r.g_ss.at[i], r.g_rs.at[i])
        for i, (s, d) in enumerate(((r.bs, r.bs_all), (r.wq, r.wq_all), (r.wo, r.wo_all), (r.wu, r.wu_all), (r.wd, r.wd_all)))]
    gain1, bias1, gain2, bias2, b_out, b_down = r.gain1, r.bias1, r.gain2, r.bias2, r.b_out, r.b_down

    def arrivals(b_x, b_dy, b_q, b_o, b_u, b_d):
        first = (g_bs, g_wq, g_wo)
        for g in first[1:]:
            g.start()
        x_a2a.start(0)
        for cp in small_in:
            cp.wait()
        for i in range(3):
            for h in range(2):
                r.bs[pl.ds(i, 1), pl.ds(h * HD, HD)] = r.bqkv[i, pl.ds(h, 1), :]
        for k in range(FB // PW):
            r.bs[pl.ds(4 + k, 1), :] = r.bup[:, pl.ds(k * PW, PW)]
        local = [x_a2a.local_in(b_x), dy_a2a.local_in(b_dy)]
        local += [g.local(b) for g, b in ((g_wq, b_q), (g_wo, b_o), (g_wu, b_u), (g_wd, b_d))]
        for load, _ in local:
            load.start()
        for s in range(NS):
            keys = jnp.broadcast_to(r.pad[pl.ds(pc.me * NS + s, 1), :].astype(f32), (PW, S))
            r.mask[s] = keys.T
        g_bs.start()
        pltpu.make_async_copy(r.bs, r.bs_all.at[6 + pc.c], r.g_rs.at[0, 6 + pc.c]).start()
        for load, store in local:
            load.wait()
            store.start()
        for g in (g_wq, g_wo, g_bs):
            g.forward_a()
        for g in (g_wq, g_wo, g_bs):
            g.forward_b()
        x_a2a.finish(0)
        x_a2a.start(1)
        for g in first:
            g.arrived_near()
        for g in (g_wu, g_wd):
            g.arrived(6 + pc.c)
        local[0][1].wait()
        local[1][1].wait()

    def later_arrivals():
        for g in (g_bs, g_wq, g_wo):
            g.last()
        for s in range(2, NS):
            x_a2a.start(s)
        for s in range(NS):
            dy_a2a.start(s)
        g_wu.start_a()
        g_wd.start_a()
        for g in (g_bs, g_wq, g_wo):
            g.arrived_far()

    act = vm(NS, SL, D, dtype=bf16)
    pl.run_scoped(arrivals, act, act, vm(R3, D, dtype=bf16), vm(PW, D, dtype=bf16), vm(D, FB, dtype=bf16), vm(FB, D, dtype=bf16))

    def attn_fwd(h2_v, wq_v, wo_v, h1_s, o_s):
        def fetch(*pairs):
            for cp in load_all(pairs, r.tmp):
                cp.wait()

        fetch(*[(r.wq_all.at[pl.ds(k, 2)], wq_v.at[pl.ds(k, 2)]) for k in (6, 0, 4)])

        def slot_at(n):
            return jnp.where(n < 2, n + 6, jnp.where(n < 4, n - 2, jnp.where(n < 6, n, n - 4)))

        def body(x_ref, qkv_ref, ml_ref, o_ref, x1_ref):
            s, n = pl.program_id(0), pl.program_id(1)
            g = slot_at(n)

            @pl.when(n == 0)
            def _():
                xh, _ = ln_stats(x_ref[0].astype(f32))
                h1_s[...] = (xh * gain1[...] + bias1[...]).astype(bf16)

            bias = r.bs_all[g]
            bias = jnp.concatenate([column(bias[i:i + 1]) for i in range(3)], axis=0)
            qkv = nt(wq_v[g], h1_s[...]) + bias
            cos, sin = r.cos[...], r.sin[...]
            ok = key_mask(r.mask[s])

            def rot(t):
                a, b = t[:HH], t[HH:]
                return jnp.concatenate([a * cos - b * sin, b * cos + a * sin], axis=0).astype(bf16)

            for h in range(2):
                lo = h * HD
                at_q, at_k, at_v = (slice(j * PW + lo, j * PW + lo + HD) for j in range(3))
                q, k, v = rot(qkv[at_q] * QS), rot(qkv[at_k]), qkv[at_v].astype(bf16)
                for at, t in ((at_q, q), (at_k, k), (at_v, v)):
                    qkv_ref[0, 0, at, :] = t
                sc = masked_scores(q, k, ok)
                m = over_rows(jnp.max, sc)
                e = jnp.exp(sc - m)
                li = 1.0 / over_rows(jnp.sum, e)
                p = (e * li).astype(bf16)
                ml = ml_ref.at[0, 0]
                ml[h:h + 1, :] = m
                ml[2 + h:3 + h, :] = li
                o = nn(v, p).astype(bf16)
                o_ref[0, 0, lo:lo + HD, :] = o
                o_s[pl.ds(pl.multiple_of(g * PW + lo, HD), HD), :] = o

            @pl.when((s == 0) & (n == 5))
            def _():
                later_arrivals()
                fetch((r.wq_all.at[pl.ds(2, 2)], wq_v.at[pl.ds(2, 2)]), (r.wo_all, wo_v))

            @pl.when(n == TP - 1)
            def _():
                attn = tn(o_s[...], wo_v[...].reshape(TP * PW, D))
                x1 = (x_ref[0].astype(f32) + (attn + b_out[...])).astype(bf16)
                x1_ref[0] = x1
                xh, _ = ln_stats(x1.astype(f32))
                h2_v[pl.ds(pl.multiple_of(s * S, S), S), :] = (xh * gain2[...] + bias2[...]).astype(bf16)

            for k in range(1, NS):
                @pl.when((s == k - 1) & (n == TP - 2))
                def _():
                    x_a2a.finish(k)

        seq = pl.BlockSpec((1, S, D), lambda s, n: (s, 0, 0))
        pair = lambda rows: pl.BlockSpec((1, 1, rows, S), lambda s, n: (s, slot_at(n), 0, 0))
        pltpu.emit_pipeline(body, grid=(NS, TP), in_specs=[seq], out_specs=[pair(R3), pair(4), pair(PW), seq])(
            r.xs, r.qkv, r.ml, r.o, r.x1)

    def mlp(h2_v, dy_v, wu_v, wd_v, yacc, acc):
        rs = GradScatter(pc, acc, r.landing, r.m_stage, r.m_r1, r.m_r2, r.m_sem, r.free)

        def is_own(i):
            return (i == 2) | (i == 4) | (i == 5) | (i == 7)

        def role_at(i):
            return jnp.where((i == 0) | (i == 5), 3, jnp.where(i < 3, 0, jnp.where(i < 5, 1, 2)))

        def slot_at(i):
            return 2 * role_at(i) + jnp.where(is_own(i), pc.c, 1 - pc.c)

        early = lambda b: remote(acc.at[b], r.m_r0, r.m_sem.at[9], r.m_sem.at[10], pc.partner)

        def landed(i):
            @pl.when(i == 5)
            def _():
                wait_for(r.m_r0, r.m_sem.at[10])
                cp = pltpu.make_async_copy(r.m_r0, r.landing, r.tmp.at[0])
                cp.start()
                cp.wait()

            pl.when(i != 5)(rs.landed)

        def weights(slot, b):
            return (pltpu.make_async_copy(r.wu_all.at[slot], wu_v.at[b], r.w_sem.at[0, b]),
                    pltpu.make_async_copy(r.wd_all.at[slot], wd_v.at[b], r.w_sem.at[1, b]))

        def fetch(i):
            slot = slot_at(i)

            @pl.when(jnp.logical_not(is_own(i)))
            def _():
                g_wu.arrived(slot)
                g_wd.arrived(slot)

            for cp in weights(slot, lax.rem(i, 2)):
                cp.start()

        fetch(jnp.int32(0))
        cps = []
        for s in range(NS):
            dy_a2a.finish(s)
            cps.append(pltpu.make_async_copy(r.dys.at[s], dy_v.at[pl.ds(s * S, S)], r.tmp.at[s]))
            cps[s].start()
        clear(yacc, r.dacc, r.gbu)
        for cp in cps:
            cp.wait()

        def step(n, carry):
            i, t = lax.div(n, NT), lax.rem(n, NT)
            b = lax.rem(i, 2)
            slot = slot_at(i)

            @pl.when(t == 0)
            def _():
                for cp in weights(slot, b):
                    cp.wait()
                clear(acc.at[b])

            @pl.when((t == NT - 1) & (i != 0) & (i != 2) & (i < TP - 1))
            def _():
                fetch(i + 1)

            rows = pl.ds(pl.multiple_of(t * TT, TT), TT)
            h2, dy = h2_v[rows, :], dy_v[rows, :]
            wu, wd = wu_v[b], wd_v[b]
            bias = r.bs_all[slot]
            bias = jnp.concatenate([bias[k:k + 1] for k in range(4, TP)], axis=1)
            pre = nn(h2, wu) + bias
            d_act = nt(dy, wd)
            cdf = 0.5 * (1.0 + lax.erf(pre * INV_SQRT2))
            act = (pre * cdf).astype(bf16)
            d_pre = d_act * (cdf + pre * jnp.exp(-0.5 * pre * pre) * INV_SQRT_2PI)
            d_pre_b = d_pre.astype(bf16)
            yacc[rows, :] += nn(act, wd)
            r.dacc[rows, :] += nt(d_pre_b, wu)
            acc[b, :FB, :] += tn(act, dy)
            acc[b, FB:, :] += tn(d_pre_b, h2)
            r.gbu[slot] += over_rows(jnp.sum, d_pre)

            done = (t == NT - 1)
            pl.when(done & (i == 0))(lambda: early(b).start())
            pl.when(done & (i > 0) & jnp.logical_not(is_own(i)))(lambda: rs.send_pair(b, i > 1))
            pl.when(done & is_own(i))(lambda: rs.settle(role_at(i), b, lambda: landed(i), i != 4))
            pl.when((t == 0) & (i == 1))(lambda: early(1 - b).wait_send())
            pl.when((t == 0) & (i > 1) & jnp.logical_not(is_own(i - 1)))(lambda: rs.sent_pair(1 - b))

            for when, hops in ((1, ("forward_a", "start_b")), (4, ("last",)), (5, ()), (9, ("forward_b",))):
                @pl.when(n == when)
                def _():
                    for hop in hops:
                        for gather in (g_wu, g_wd):
                            getattr(gather, hop)()
                    if when in (1, 5):
                        fetch(i + 1)

            return carry

        lax.fori_loop(0, TP * NT, step, 0)
        cps = load_all([(r.x1.at[s], h2_v.at[pl.ds(s * S, S)]) for s in range(NS)], r.tmp)
        stores = []
        for s in range(NS):
            rows = pl.ds(s * S, S)
            cps[s].wait()
            dy_v[rows, :] = (h2_v[rows, :].astype(f32) + (yacc[rows, :] + b_down[...])).astype(bf16)
            cp = pltpu.make_async_copy(dy_v.at[rows], r.y_seq.at[s], r.tmp.at[NS + s])
            cp.start()
            stores.append(cp)
        for s in range(NS):
            stores[s].wait()
            y_a2a.start(s)

    tok = vm(NS * S, D, dtype=bf16)

    def forward_and_mlp(h2_v, dy_v, wu_v, wd_v):
        pl.run_scoped(functools.partial(attn_fwd, h2_v), vm(TP, R3, D, dtype=bf16), vm(TP, PW, D, dtype=bf16),
                      vm(S, D, dtype=bf16), vm(D, S, dtype=bf16))
        pl.run_scoped(functools.partial(mlp, h2_v, dy_v, wu_v, wd_v), vm(NS * S, D), vm(2, 2 * FB, D))

    pl.run_scoped(forward_and_mlp, tok, tok, vm(2, D, FB, dtype=bf16), vm(2, FB, D, dtype=bf16))

    rs_m = GradScatter(pc, r.landing, r.landing, r.m_stage, r.m_r1, r.m_r2, r.m_sem, r.free)

    def attn_bwd(h1_s, do_s, acc, gb_a):
        gx_a2a = AllToAll(pc, r.gx_out, h1_s, r.gx_ss, r.gx_rs, False)

        def open_bwd(wo_v):
            wo_cp = pltpu.make_async_copy(r.wo_all, wo_v, r.tmp.at[0])
            wo_cp.start()
            wo_cp.wait()
            clear(r.va, acc, gb_a)

            def body(x_ref, x1_ref, dy_ref, o_ref):
                s = pl.program_id(0)
                rows = pl.ds(pl.multiple_of(s * S, S), S)
                dy, dh2 = dy_ref[0].astype(f32), r.dacc[rows, :]
                xh2, inv2 = ln_stats(x1_ref[0].astype(f32))
                d = dy + ln_grad(dh2, xh2, inv2, gain2[...])
                r.dacc[rows, :] = d
                db = d.astype(bf16)
                r.va[0:1, :] += over_rows(jnp.sum, dy)
                r.va[1:2, :] += over_rows(jnp.sum, dh2 * xh2)
                r.va[2:3, :] += over_rows(jnp.sum, dh2)
                r.va[3:4, :] += over_rows(jnp.sum, d)
                xh, _ = ln_stats(x_ref[0].astype(f32))
                h1_s[s] = (xh * gain1[...] + bias1[...]).astype(bf16)
                do_s[s] = nt(wo_v[...].reshape(TP * PW, D), db).astype(bf16)
                acc[:, R3:, :] += nn(o_ref[0].reshape(TP * PW, S), db).reshape(TP, PW, D)

            seq = pl.BlockSpec((1, S, D), lambda s: (s, 0, 0))
            pltpu.emit_pipeline(body, grid=(NS,), in_specs=[seq, seq, seq, pl.BlockSpec((1, TP, PW, S), lambda s: (s, 0, 0, 0))])(
                r.xs, r.x1, r.dys, r.o)

        pl.run_scoped(open_bwd, vm(TP, PW, D, dtype=bf16))
        n_half = NS // 2
        rs = GradScatter(pc, acc, r.landing.at[pl.ds(0, R3 + PW)], r.a_stage, r.a_r1, r.a_r2, r.a_sem, r.free)

        def slot_at(g):
            return jnp.where(g < 4, lax.rem(g + 2, 4), g)

        def heads(dq_s, wq_v, buf):
            wq_cp = pltpu.make_async_copy(r.wq_all, wq_v, r.tmp.at[1])
            wq_cp.start()
            for half in range(2):
                def body(qkv_ref, ml_ref):
                    n, sh = pl.program_id(0), pl.program_id(1)
                    g = slot_at(n)
                    s = half * n_half + sh
                    cos, sin = r.cos[...], r.sin[...]
                    ok = key_mask(r.mask[s])

                    def rot_back(t):
                        a, b = t[:HH], t[HH:]
                        return jnp.concatenate([a * cos + b * sin, b * cos - a * sin], axis=0)

                    base = pl.multiple_of(g * R3, PW)
                    for h in range(2):
                        lo = h * HD
                        qkv, ml = qkv_ref.at[0, 0], ml_ref.at[0, 0]
                        q, k, v = (qkv[j * PW + lo:j * PW + lo + HD, :] for j in range(3))
                        do = do_s[s, pl.ds(pl.multiple_of(g * PW + lo, HD), HD), :]
                        sc = masked_scores(q, k, ok)
                        p = jnp.exp(sc - ml[h:h + 1, :]) * ml[2 + h:3 + h, :]
                        dp = tn(v, do)
                        ds = (p * (dp - over_rows(jnp.sum, dp * p))).astype(bf16)
                        dv = nt(p.astype(bf16), do).T
                        dk = rot_back(nt(ds, q).T)
                        dq = rot_back(nn(k, ds)) * QS
                        for j, t in enumerate((dq, dk, dv)):
                            at = pl.ds(base + j * PW + lo, HD)
                            dq_s[sh, at, :] = t.astype(bf16)
                            gb_a[at, :] += over_cols(jnp.sum, t)

                    acc[g, :R3, :] += nn(dq_s[sh, pl.ds(base, R3), :], h1_s[s])
                    if half == 0:
                        @pl.when((sh == 0) & (n == 1))
                        def _():
                            rs_m.second([buf, r.landing.at[pl.ds(FB, FB)]], r.chunk)
                    else:
                        @pl.when(sh == n_half - 1)
                        def _():
                            rs.block_done(g, g)

                            @pl.when(n > 0)
                            def _():
                                rs.later(slot_at(n - 1), slot_at(n - 1), n < TP - 1)

                pair = lambda rows: pl.BlockSpec((1, 1, rows, S), lambda n, sh: (half * n_half + sh, slot_at(n), 0, 0))
                pltpu.emit_pipeline(body, grid=(TP, n_half), in_specs=[pair(R3), pair(4)])(r.qkv, r.ml)
                if half == 0:
                    wq_cp.wait()

                def close_bwd(x_ref):
                    sh = pl.program_id(0)
                    s = half * n_half + sh
                    rows = pl.ds(pl.multiple_of(s * S, S), S)
                    dh1 = tn(dq_s[sh], wq_v[...].reshape(TP * R3, D))
                    xh, inv = ln_stats(x_ref[0].astype(f32))
                    r.va[4:5, :] += over_rows(jnp.sum, dh1 * xh)
                    r.va[5:6, :] += over_rows(jnp.sum, dh1)
                    h1_s[s] = (r.dacc[rows, :] + ln_grad(dh1, xh, inv, gain1[...])).astype(bf16)
                    gx_a2a.start(s)
                    cp = gx_a2a.local_out(s, h1_s)
                    cp.start()
                    cp.wait()

                pltpu.emit_pipeline(close_bwd, grid=(n_half,),
                                    in_specs=[pl.BlockSpec((1, S, D), lambda sh: (half * n_half + sh, 0, 0))])(r.xs)
            last = jnp.int32(TP - 1)
            rs.later(last, last, False)
            rs.second([buf, r.landing.at[pl.ds(FB, FB)]], r.chunk, r.gq_b)

        pl.run_scoped(heads, vm(n_half, TP * R3, S, dtype=bf16), vm(TP, R3, D, dtype=bf16), vm(FB, D))

        for g in range(TP):
            r.msg[g] = r.va[...]
            for j in range(3):
                cols = jnp.broadcast_to(gb_a[g * R3 + j * PW:g * R3 + (j + 1) * PW, :], (PW, PW))
                r.msg[g, 6:7, j * PW:(j + 1) * PW] = cols.T[0:1, :]
            r.msg[g, 6:7, R3:R3 + FB] = r.gbu[g]
        pair = remote(r.msg, r.msg_in, r.s_ss.at[0], r.s_rs.at[0], pc.partner)
        pair.start()
        pair.wait()
        r.msg_in[...] = r.msg_in[...] + r.msg[...]
        chip = lax.div(pc.me, 2)
        small = [remote(r.msg_in.at[pc.slot_of(m)], r.msgs.at[chip], r.s_ss.at[1], r.s_rs.at[1], pc.peer(m)) for m in (2, 4, 6)]
        for cp in small:
            cp.start()
        own = pltpu.make_async_copy(r.msg_in.at[pc.slot_of(0)], r.msgs.at[chip], r.s_ss.at[2])
        own.start()

        def tail(bufs, act_v, turned):
            b0, b1, b2 = (bufs.at[i] for i in range(3))
            y_own = [(pltpu.make_async_copy(r.y_seq.at[s, y_a2a._rows(pc.me)], act_v.at[s], r.tmp.at[s]),
                      pltpu.make_async_copy(act_v.at[s], r.y_out.at[pc.me * NS + s], r.tmp.at[NS + s])) for s in range(NS)]
            for load, _ in y_own:
                load.start()
            for load, store in y_own:
                load.wait()
                store.start()
            for g in (g_bs, g_wq, g_wo, g_wu, g_wd):
                g.sent()
            for _, store in y_own:
                store.wait()
            rs_m.finish()
            wait_for(r.m_r1.at[0], r.m_sem.at[4])
            for p in range(2):
                half = pl.ds(p * FB, FB)
                for cp in load_all([(r.m_stage.at[3, half], b0), (r.m_r1.at[0, half], b1), (r.m_r2.at[half], b2)], r.tmp):
                    cp.wait()
                row_add(b0, [b1, b2])
                if p == 0:
                    cp = pltpu.make_async_copy(b0, r.gd, r.tmp.at[0])
                else:
                    for k in range(D // FB):
                        cols = slice(k * FB, (k + 1) * FB)
                        turned[cols, :] = b0[:, cols].T
                    cp = pltpu.make_async_copy(turned, r.gu, r.tmp.at[0])
                cp.start()
                cp.wait()
            rs.own_part(b0, b1, r.tmp)
            for s in range(NS):
                y_a2a.finish(s)
            for s in range(NS):
                gx_a2a.finish(s)
            rs.finish()
            own.wait()
            for sem in (r.s_ss.at[1], r.s_rs.at[1]):
                wait_for(r.msgs.at[pl.ds(0, len(small))], sem)

        pl.run_scoped(tail, vm(3, FB, D), vm(NS, SL, D, dtype=bf16), vm(D, FB))

    seqs = vm(NS, S, D, dtype=bf16)
    pl.run_scoped(attn_bwd, seqs, vm(NS, D, S, dtype=bf16), vm(TP, R3 + PW, D), vm(TP * R3, 1))


def layer_call(*args):
    out = pl.pallas_call(
        layer_kernel,
        in_specs=[ANY] * len(IN_NAMES),
        out_specs=[ANY] * len(OUT_SHAPES),
        out_shape=[sds(*v) for v in OUT_SHAPES.values()],
        scratch_shapes=list(SCRATCH.values()),
        compiler_params=pltpu.CompilerParams(collective_id=0, has_side_effects=True, vmem_limit_bytes=VMEM_LIMIT),
        name="layer",
    )(*args)
    return out[:8]


FINAL = {"y": ((TP * NS, SL, D), bf16), "gx": ((TP * NS, SL, D), bf16), "gd": ((FB, D), f32), "gu": ((D, FB), f32),
         "go": ((PW, D), f32), "gbq": ((3, 2, HD), f32), "gbu": ((1, FB), f32)}
VECS = ("bd", "g2", "b2", "bo", "g1", "b1")
FINAL |= {k: ((1, D), f32) for k in VECS}
LATE = ("gbq", "gbu") + VECS


def final_kernel(y_in, gx_in, msgs, gd_in, gu_in, stage, r2, *refs):
    outs, refs = Refs(FINAL, refs), refs[len(FINAL):]
    msg_v, y_v, gx_v, gd_v, gu_v, sums, ld, st = refs[:8]
    late = Refs(LATE, refs[8:])
    moves = [([(msgs, msg_v)], [])]
    moves.append(([(t, sums.at[x]) for x, t in enumerate((stage.at[3, pl.ds(R3, PW)], r2))], [(sums.at[0], outs.go)]))
    for src, buf, dst in ((gd_in, gd_v, outs.gd), (gu_in, gu_v, outs.gu), (y_in, y_v, outs.y), (gx_in, gx_v, outs.gx)):
        moves.append(([(src, buf)], [(buf, dst)]))
    copy = pltpu.make_async_copy
    loads = [[copy(s, d, ld.at[i, x]) for x, (s, d) in enumerate(m[0])] for i, m in enumerate(moves)]
    stores = [[copy(s, d, st.at[i, x]) for x, (s, d) in enumerate(m[1])] for i, m in enumerate(moves)]
    for cps in loads:
        for cp in cps:
            cp.start()
    for i, (cps, outward) in enumerate(zip(loads, stores)):
        for cp in cps:
            cp.wait()
        if i == 0:
            small = msg_v[0]
            for j in range(1, msg_v.shape[0]):
                small = small + msg_v[j]
            for j, k in enumerate(VECS):
                getattr(late, k)[...] = small[j:j + 1, :]
            for j in range(3):
                for h in range(2):
                    lo = j * PW + h * HD
                    late.gbq[j, h:h + 1, :] = small[6:7, lo:lo + HD]
            late.gbu[...] = small[6:7, R3:R3 + FB]
        if i == 1:
            row_add(sums.at[0], [sums.at[1]])
        for cp in outward:
            cp.start()
    small_out = load_all([(getattr(late, k), getattr(outs, k)) for k in LATE], st.at[len(moves)])
    for cps in stores + [small_out]:
        for cp in cps:
            cp.wait()


def final_call(y, gx, msgs, gd, gu, stage, r2):
    act = vm(*y.shape, dtype=bf16)
    return pl.pallas_call(
        final_kernel,
        in_specs=[ANY] * 7,
        out_specs=[ANY] * len(FINAL),
        out_shape=[sds(*v) for v in FINAL.values()],
        scratch_shapes=[vm(*msgs.shape), act, act, vm(FB, D), vm(D, FB), vm(2, PW, D), DMA((6, 2)), DMA((7, len(LATE)))]
        + [vm(*FINAL[k][0]) for k in LATE],
        compiler_params=pltpu.CompilerParams(vmem_limit_bytes=VMEM_LIMIT),
        cost_estimate=pl.CostEstimate(flops=10 ** 10, bytes_accessed=3 * 10 ** 7, transcendentals=0),
        name="results",
    )(y, gx, msgs, gd, gu, stage, r2)


def rope_tables():
    inv_freq = (ROPE_BASE ** (-2.0 * np.arange(HH, dtype=np.float32) / HD)).astype(np.float32)
    angles = np.outer(inv_freq, np.arange(S, dtype=np.float32))
    return np.cos(angles), np.sin(angles)


def solution(mesh):
    no = None
    act_spec = P('dp', 'tp', no)
    rep, part = P(no), P('dp')
    in_specs = (act_spec, act_spec, P('dp', no), rep, rep, P(no, no, 'tp', no), P(no, 'tp', no),
                P('tp', no, no), rep, rep, rep, P(no, 'tp'), P('tp'), P('tp', no), rep)
    out_specs = (act_spec, act_spec, part, part, P('dp', no, 'tp', no), P('dp', 'tp', no), P(('dp', 'tp'), no, no),
                 part, part, part, P('dp', 'tp'), P(('dp', 'tp')), P(('dp', 'tp'), no), part)

    def device_step(x_in, grad_y, pad_mask, ln1_gain, ln1_bias, w_qkv, b_qkv, w_out, b_out, ln2_gain, ln2_bias, w_up, b_up, w_down, b_down):
        assert x_in.shape == (TP * NS, SL, D) and w_qkv.shape == (3, D, 2, HD) and w_up.shape == (D, FB)
        row = lambda v: v.reshape(1, -1)
        wq = w_qkv.transpose(0, 2, 3, 1).reshape(R3, D)
        cos, sin = rope_tables()
        parts = layer_call(
            x_in, grad_y, wq, w_out.reshape(PW, D), w_up, w_down, b_qkv, row(b_up), pad_mask, cos, sin,
            row(ln1_gain), row(ln1_bias), row(ln2_gain), row(ln2_bias), row(b_out), row(b_down))
        *parts, gq_b = parts
        stage = parts[-2]
        to_b = [(i, i ^ (4 - 2 * (i % 2))) for i in range(TP)]
        gq = stage[-1, :R3] + lax.ppermute(gq_b, 'tp', to_b)
        y, gx, gd, gu, go, gbq, gbu, *vecs = final_call(*parts)
        bd, g2, b2, bo, g1, b1 = (v.reshape(D) for v in vecs)
        return (y, gx, g1, b1, gq.reshape(3, 2, HD, D).transpose(0, 3, 1, 2), gbq, go.reshape(2, HD, D), bo, g2, b2,
                gu, gbu.reshape(FB), gd, bd)

    return jax.shard_map(device_step, mesh=mesh, in_specs=in_specs, out_specs=out_specs, check_vma=False)
```

```python
import functools

import jax
import jax.numpy as jnp
import numpy as np
from jax import lax
from jax.experimental import pallas as pl
from jax.experimental.pallas import tpu as pltpu
from jax.sharding import PartitionSpec as P

f32 = jnp.float32
bf16 = jnp.bfloat16
LN_EPS = 1e-5
ROPE_BASE = 10000.0
INV_SQRT2 = 0.7071067811865476
INV_SQRT_2PI = 0.3989422804014327
NEG_LARGE = -1e30
MESH = pl.DeviceIdType.MESH
ANY = pl.BlockSpec(memory_space=pl.ANY)
VMEM_LIMIT = 66_000_000

TP = 8
NS = 4
S = 512
D = 1024
PW = 128
HD = 64
HH = HD // 2
FB = 512
SL = 64
QS = HD ** -0.5
R3 = 3 * PW
ROWS = 8


def dg(a, b, ca, cb):
    return lax.dot_general(a, b, (((ca,), (cb,)), ((), ())), preferred_element_type=f32)


def nn(a, b):
    return dg(a, b, 1, 0)


def nt(a, b):
    return dg(a, b, 1, 1)


def tn(a, b):
    return dg(a, b, 0, 0)


def over_rows(reduce, v):
    return reduce(v, axis=0, keepdims=True)


def over_cols(reduce, v):
    return reduce(v, axis=1, keepdims=True)


def sds(shape, dtype):
    return jax.ShapeDtypeStruct(shape, dtype)


class Place:
    def __init__(self):
        me = lax.axis_index("tp")
        self.me = me
        self.c = lax.rem(me, 2)
        self.dc = 1 - 2 * self.c
        self.dx = 2 - 4 * lax.rem(lax.div(me, 2), 2)
        self.dy = 4 - 8 * lax.div(me, 4)
        self.partner = me + self.dc
        self.a = me + (1 - self.c) * self.dx + self.c * self.dy
        self.b = me + (1 - self.c) * self.dy + self.c * self.dx

    def peer(self, m):
        return self.me + (m & 1) * self.dc + ((m >> 1) & 1) * self.dx + (m >> 2) * self.dy

    def slot_of(self, m):
        k = self.c if m % 2 == 0 else 1 - self.c
        lo, hi = {0: (6, 7), 1: (0, 5), 2: (4, 1), 3: (2, 3)}[m >> 1]
        return lo + k * (hi - lo)


def remote(src, dst, send_sem, recv_sem, device):
    return pltpu.make_async_remote_copy(src_ref=src, dst_ref=dst, send_sem=send_sem, recv_sem=recv_sem,
                                        device_id={"tp": device}, device_id_type=MESH)


def wait_for(ref, sem):
    pltpu.make_async_copy(ref, ref, sem).wait()


def entry_barrier(pc):
    bar = pltpu.get_barrier_semaphore()
    for m in range(1, TP):
        pl.semaphore_signal(bar, inc=1, device_id={"tp": pc.peer(m)}, device_id_type=MESH)
    pl.semaphore_wait(bar, TP - 1)


class AllToAll:
    def __init__(self, pc, pos_ref, seq_ref, send_sem, recv_sem, inward):
        self.pc, self.pos, self.seq, self.ss, self.rs, self.inward = pc, pos_ref, seq_ref, send_sem, recv_sem, inward

    def _rows(self, dev):
        return pl.ds(pl.multiple_of(dev * SL, SL), SL)

    def _copy(self, s, m):
        pc, dev = self.pc, self.pc.peer(m)
        if self.inward:
            src, dst = self.pos.at[dev * NS + s], self.seq.at[s, self._rows(pc.me)]
        else:
            src, dst = self.seq.at[s, self._rows(dev)], self.pos.at[pc.me * NS + s]
        return remote(src, dst, self.ss.at[s], self.rs.at[s], dev)

    def start(self, s):
        for m in (*range(2, TP), 1):
            self._copy(s, m).start()

    def finish(self, s):
        all_rows = self.seq.at[s, pl.ds(0, S - SL)]
        wait_for(all_rows, self.ss.at[s])
        wait_for(all_rows, self.rs.at[s])

    def local_in(self, buf):
        pc = self.pc
        return (pltpu.make_async_copy(self.pos.at[pl.ds(pc.me * NS, NS)], buf, self.ss.at[NS]),
                pltpu.make_async_copy(buf, self.seq.at[:, self._rows(pc.me)], self.rs.at[NS]))

    def local_out(self, s, src):
        return pltpu.make_async_copy(src.at[s, self._rows(self.pc.me)], self.pos.at[self.pc.me * NS + s], self.ss.at[NS])


class Gather:
    def __init__(self, pc, src_ref, dst_ref, send_sem, recv_sem):
        self.pc, self.src, self.dst, self.ss, self.rs = pc, src_ref, dst_ref, send_sem, recv_sem

    def _send(self, src, slot, dev):
        return remote(src, self.dst.at[slot], self.ss, self.rs.at[slot], dev)

    def _direct(self):
        pc, c = self.pc, self.pc.c
        return [self._send(self.src, c, pc.a), self._send(self.src, 6 + c, pc.partner),
                self._send(self.src, 4 + c, pc.b)]

    def _hop(self):
        pc, c = self.pc, self.pc.c
        return [self._send(self.dst.at[c], 2 + c, pc.b), self._send(self.dst.at[c], c, pc.partner),
                self._send(self.dst.at[4 + c], 4 + c, pc.partner)]

    def _last(self):
        pc, c = self.pc, self.pc.c
        return self._send(self.dst.at[2 + c], 2 + c, pc.partner)

    def arrived(self, slot):
        wait_for(self.dst.at[slot], self.rs.at[slot])

    def start(self):
        self.start_a()
        self.start_b()

    def start_a(self):
        for cp in self._direct()[:2]:
            cp.start()

    def start_b(self):
        self._direct()[2].start()

    def forward(self):
        self.forward_a()
        self.forward_b()

    def forward_a(self):
        hop = self._hop()
        self.arrived(self.pc.c)
        hop[0].start()
        hop[1].start()

    def forward_b(self):
        self.arrived(4 + self.pc.c)
        self._hop()[2].start()

    def last(self):
        self.arrived(2 + self.pc.c)
        self._last().start()

    def local(self, buf):
        return (pltpu.make_async_copy(self.src, buf, self.rs.at[TP]),
                pltpu.make_async_copy(buf, self.dst.at[6 + self.pc.c], self.rs.at[6 + self.pc.c]))

    def arrived_near(self):
        for j in (0, 2, 3):
            self.arrived(2 * j + 1 - self.pc.c)
        self.arrived(6 + self.pc.c)

    def arrived_far(self):
        self.arrived(3 - self.pc.c)

    def sent(self):
        wait_for(self.dst.at[pl.ds(0, TP - 1)], self.ss)


def row_add(acc, others):
    step = 64

    def body(i, carry):
        r = pl.ds(pl.multiple_of(i * step, step), step)
        v = acc[r, :]
        for o in others:
            v = v + o[r, :]
        acc[r, :] = v
        return carry

    lax.fori_loop(0, acc.shape[0] // step, body, 0)


class GradScatter:
    def __init__(self, pc, acc, landing, stage, r1, r2, sems, free):
        self.pc, self.acc, self.landing, self.stage, self.r1, self.r2 = pc, acc, landing, stage, r1, r2
        self.sem, self.free = sems, free

    def _pair(self, b):
        return remote(self.acc.at[b], self.landing, self.sem.at[0], self.sem.at[1], self.pc.partner)

    def _first(self, j):
        return remote(self.stage.at[j], self.r1.at[j], self.sem.at[2 + j], self.sem.at[4 + j], self.pc.a)

    def _second(self):
        return remote(self.stage.at[2], self.r2, self.sem.at[6], self.sem.at[7], self.pc.b)

    def send_pair(self, b, needs_credit):
        @pl.when(needs_credit)
        def _():
            pl.semaphore_wait(self.free, 1)

        self._pair(b).start()

    def sent_pair(self, b):
        self._pair(b).wait_send()

    def settle(self, j, b, landed, gives_credit):
        landed()
        row_add(self.acc.at[b], [self.landing])

        @pl.when(gives_credit)
        def _():
            pl.semaphore_signal(self.free, inc=1, device_id={"tp": self.pc.partner}, device_id_type=MESH)

        store = pltpu.make_async_copy(self.acc.at[b], self.stage.at[j], self.sem.at[8])
        store.start()
        store.wait()

        @pl.when(j < 2)
        def _():
            self._first(j).start()

    def landed(self):
        wait_for(self.landing, self.sem.at[1])

    def block_done(self, slot, b):
        pl.when(lax.rem(slot, 2) != self.pc.c)(lambda: self.send_pair(b, True))

    def later(self, slot, b, gives_credit):
        own = lax.rem(slot, 2) == self.pc.c
        pl.when(own)(lambda: self.settle(lax.div(slot, 2), b, self.landed, gives_credit))
        pl.when(jnp.logical_not(own))(lambda: self.sent_pair(b))

    def second(self, bufs, chunk_sem, dsts):
        n = chunk_sem.shape[1]
        size = bufs[0].shape[0]
        rows = size // n
        part = lambda ref, k: ref.at[pl.ds(k * rows, rows)]
        wait_for(self.r1.at[1], self.sem.at[5])
        dsts = [part(d, k) for d in dsts for k in range(d.shape[0] // rows)]
        for p in range(self.stage.shape[1] // size):
            mine, theirs = (ref.at[pl.ds(p * size, size)] for ref in (self.stage.at[2], self.r1.at[1]))
            loads = [[pltpu.make_async_copy(part(src, k), part(buf, k), chunk_sem.at[x, k])
                      for x, (src, buf) in enumerate(zip((mine, theirs), bufs))] for k in range(n)]
            stores = [pltpu.make_async_copy(part(bufs[0], k), dsts[p * n + k], chunk_sem.at[2, k]) for k in range(n)]
            for group in loads:
                for cp in group:
                    cp.start()
            for k in range(n):
                for cp in loads[k]:
                    cp.wait()
                row_add(part(bufs[0], k), [part(bufs[1], k)])
                stores[k].start()
            for cp in stores:
                cp.wait()

    def send_second(self):
        self._second().start()

    def own_part(self, b0, b1, sem):
        wait_for(self.r1.at[0], self.sem.at[4])
        for cp in load_all([(self.stage.at[3], b0), (self.r1.at[0], b1)], sem):
            cp.wait()
        row_add(b0, [b1])
        cp = pltpu.make_async_copy(b0, self.stage.at[3], sem.at[0])
        cp.start()
        cp.wait()

    def sent_first(self):
        for j in range(2):
            self._first(j).wait_send()

    def finish(self):
        self.sent_first()
        self._second().wait()


def ln_stats(v):
    c = v - over_cols(jnp.mean, v)
    inv = lax.rsqrt(over_cols(jnp.mean, c * c) + LN_EPS)
    return c * inv, inv


def ln_grad(d_out, x_hat, inv, gain):
    dh = d_out * gain
    return inv * (dh - over_cols(jnp.mean, dh) - x_hat * over_cols(jnp.mean, dh * x_hat))


def masked_scores(q, k, ok):
    return jnp.where(ok, tn(k, q), NEG_LARGE)


def key_mask(mask):
    return jnp.concatenate([mask] * (S // PW), axis=1) > 0


def column(row):
    return jnp.broadcast_to(row, (PW, row.shape[1])).T[:, :1]


def clear(*refs):
    for ref in refs:
        ref[...] = jnp.zeros(ref.shape, ref.dtype)


def load_all(pairs, sem):
    cps = [pltpu.make_async_copy(s, d, sem.at[i]) for i, (s, d) in enumerate(pairs)]
    for cp in cps:
        cp.start()
    return cps


def vm(*shape, dtype=f32):
    return pltpu.VMEM(shape, dtype)


TT = 1024
NT = NS * S // TT
SMALL = {
    "bqkv": vm(3, 2, HD), "bup": vm(1, FB), "pad": vm(TP * NS, S, dtype=jnp.int32), "cos": vm(HH, S), "sin": vm(HH, S),
    "gain1": vm(1, D), "bias1": vm(1, D), "gain2": vm(1, D), "bias2": vm(1, D), "b_out": vm(1, D), "b_down": vm(1, D),
}
IN_NAMES = ("x_in", "dy_in", "wq", "wo", "wu", "wd") + tuple("in_" + k for k in SMALL)
OUT_SHAPES = {
    "y_out": ((TP * NS, SL, D), bf16), "gx_out": ((TP * NS, SL, D), bf16), "msgs": ((TP // 2, ROWS, D), f32), "gd": ((FB, D), f32), "gu": ((D, FB), f32),
    "a_stage": ((4, R3 + PW, D), f32), "gq_b": ((R3, D), f32), "go_b": ((PW, D), f32), "a_r1": ((2, R3 + PW, D), f32),
    "m_r0": ((2 * FB, D), f32), "m_stage": ((4, 2 * FB, D), f32), "m_r1": ((2, 2 * FB, D), f32), "m_r2": ((2 * FB, D), f32),
    "xs": ((NS, S, D), bf16), "dys": ((NS, S, D), bf16), "wq_all": ((TP, R3, D), bf16), "wo_all": ((TP, PW, D), bf16),
    "wu_all": ((TP, D, FB), bf16), "wd_all": ((TP, FB, D), bf16),
    "qkv": ((NS, TP, R3, S), bf16), "ml": ((NS, TP, 4, S), f32), "o": ((NS, TP, PW, S), bf16),
    "x1": ((NS, S, D), bf16), "y_seq": ((NS, S, D), bf16),
}
DMA = pltpu.SemaphoreType.DMA
SCRATCH = SMALL | {
    "in_sem": DMA((len(SMALL),)),
    "bs_all": vm(TP, ROWS, PW), "bs": vm(ROWS, PW), "mask": vm(NS, S, PW), "dacc": vm(NS * S, D), "landing": vm(2 * FB, D), "gbu": vm(TP, 1, FB), "va": vm(ROWS, D),
    "msg": vm(TP, ROWS, D), "msg_in": vm(TP, ROWS, D),
    "free": pltpu.SemaphoreType.REGULAR,
    "x_ss": DMA((NS + 1,)), "x_rs": DMA((NS + 1,)), "dy_ss": DMA((NS + 1,)), "dy_rs": DMA((NS + 1,)),
    "y_ss": DMA((NS + 1,)), "y_rs": DMA((NS + 1,)), "gx_ss": DMA((NS + 1,)), "gx_rs": DMA((NS + 1,)),
    "g_ss": DMA((5,)), "g_rs": DMA((5, TP + 1)), "m_sem": DMA((11,)), "a_sem": DMA((9,)), "s_ss": DMA((3,)), "s_rs": DMA((2,)),
    "tmp": DMA((TP,)), "chunk": DMA((3, 4)), "w_sem": DMA((2, 2)),
}


class Refs:
    def __init__(self, names, refs):
        for n, r in zip(names, refs):
            setattr(self, n, r)


def layer_kernel(*refs):
    r = Refs(IN_NAMES + tuple(OUT_SHAPES) + tuple(SCRATCH), refs)
    pc = Place()
    small_in = load_all([(getattr(r, "in_" + k), getattr(r, k)) for k in SMALL], r.in_sem)
    entry_barrier(pc)
    x_a2a = AllToAll(pc, r.x_in, r.xs, r.x_ss, r.x_rs, True)
    dy_a2a = AllToAll(pc, r.dy_in, r.dys, r.dy_ss, r.dy_rs, True)
    y_a2a = AllToAll(pc, r.y_out, r.y_seq, r.y_ss, r.y_rs, False)
    g_bs, g_wq, g_wo, g_wu, g_wd = [
        Gather(pc, s, d, r.g_ss.at[i], r.g_rs.at[i])
        for i, (s, d) in enumerate(((r.bs, r.bs_all), (r.wq, r.wq_all), (r.wo, r.wo_all), (r.wu, r.wu_all), (r.wd, r.wd_all)))]
    gain1, bias1, gain2, bias2, b_out, b_down = r.gain1, r.bias1, r.gain2, r.bias2, r.b_out, r.b_down

    def arrivals(b_x, b_dy, b_q, b_o, b_u, b_d):
        first = (g_bs, g_wq, g_wo)
        for g in first[1:]:
            g.start()
        x_a2a.start(0)
        for cp in small_in:
            cp.wait()
        for i in range(3):
            for h in range(2):
                r.bs[pl.ds(i, 1), pl.ds(h * HD, HD)] = r.bqkv[i, pl.ds(h, 1), :]
        for k in range(FB // PW):
            r.bs[pl.ds(4 + k, 1), :] = r.bup[:, pl.ds(k * PW, PW)]
        local = [x_a2a.local_in(b_x), dy_a2a.local_in(b_dy)]
        local += [g.local(b) for g, b in ((g_wq, b_q), (g_wo, b_o), (g_wu, b_u), (g_wd, b_d))]
        for load, _ in local:
            load.start()
        for s in range(NS):
            keys = jnp.broadcast_to(r.pad[pl.ds(pc.me * NS + s, 1), :].astype(f32), (PW, S))
            r.mask[s] = keys.T
        g_bs.start()
        pltpu.make_async_copy(r.bs, r.bs_all.at[6 + pc.c], r.g_rs.at[0, 6 + pc.c]).start()
        for load, store in local:
            load.wait()
            store.start()
        for g in (g_wq, g_wo, g_bs):
            g.forward_a()
        for g in (g_wq, g_wo, g_bs):
            g.forward_b()
        x_a2a.finish(0)
        x_a2a.start(1)
        for g in first:
            g.arrived_near()
        for g in (g_wu, g_wd):
            g.arrived(6 + pc.c)
        local[0][1].wait()
        local[1][1].wait()

    def later_arrivals():
        for g in (g_bs, g_wq, g_wo):
            g.last()
        for s in range(2, NS):
            x_a2a.start(s)
        for s in range(NS):
            dy_a2a.start(s)
        g_wu.start_a()
        g_wd.start_a()
        for g in (g_bs, g_wq, g_wo):
            g.arrived_far()

    act = vm(NS, SL, D, dtype=bf16)
    pl.run_scoped(arrivals, act, act, vm(R3, D, dtype=bf16), vm(PW, D, dtype=bf16), vm(D, FB, dtype=bf16), vm(FB, D, dtype=bf16))

    def attn_fwd(h2_v, wq_v, wo_v, h1_s, o_s):
        def fetch(*pairs):
            for cp in load_all(pairs, r.tmp):
                cp.wait()

        fetch(*[(r.wq_all.at[pl.ds(k, 2)], wq_v.at[pl.ds(k, 2)]) for k in (6, 0, 4)])

        def slot_at(n):
            return jnp.where(n < 2, n + 6, jnp.where(n < 4, n - 2, jnp.where(n < 6, n, n - 4)))

        def body(x_ref, qkv_ref, ml_ref, o_ref, x1_ref):
            s, n = pl.program_id(0), pl.program_id(1)
            g = slot_at(n)

            @pl.when(n == 0)
            def _():
                xh, _ = ln_stats(x_ref[0].astype(f32))
                h1_s[...] = (xh * gain1[...] + bias1[...]).astype(bf16)

            bias = r.bs_all[g]
            bias = jnp.concatenate([column(bias[i:i + 1]) for i in range(3)], axis=0)
            qkv = nt(wq_v[g], h1_s[...]) + bias
            cos, sin = r.cos[...], r.sin[...]
            ok = key_mask(r.mask[s])

            def rot(t):
                a, b = t[:HH], t[HH:]
                return jnp.concatenate([a * cos - b * sin, b * cos + a * sin], axis=0).astype(bf16)

            for h in range(2):
                lo = h * HD
                at_q, at_k, at_v = (slice(j * PW + lo, j * PW + lo + HD) for j in range(3))
                q, k, v = rot(qkv[at_q] * QS), rot(qkv[at_k]), qkv[at_v].astype(bf16)
                for at, t in ((at_q, q), (at_k, k), (at_v, v)):
                    qkv_ref[0, 0, at, :] = t
                sc = masked_scores(q, k, ok)
                m = over_rows(jnp.max, sc)
                e = jnp.exp(sc - m)
                li = 1.0 / over_rows(jnp.sum, e)
                p = (e * li).astype(bf16)
                ml = ml_ref.at[0, 0]
                ml[h:h + 1, :] = m
                ml[2 + h:3 + h, :] = li
                o = nn(v, p).astype(bf16)
                o_ref[0, 0, lo:lo + HD, :] = o
                o_s[pl.ds(pl.multiple_of(g * PW + lo, HD), HD), :] = o

            @pl.when((s == 0) & (n == 5))
            def _():
                later_arrivals()
                fetch((r.wq_all.at[pl.ds(2, 2)], wq_v.at[pl.ds(2, 2)]), (r.wo_all, wo_v))

            @pl.when(n == TP - 1)
            def _():
                attn = tn(o_s[...], wo_v[...].reshape(TP * PW, D))
                x1 = (x_ref[0].astype(f32) + (attn + b_out[...])).astype(bf16)
                x1_ref[0] = x1
                xh, _ = ln_stats(x1.astype(f32))
                h2_v[pl.ds(pl.multiple_of(s * S, S), S), :] = (xh * gain2[...] + bias2[...]).astype(bf16)

            for k in range(1, NS):
                @pl.when((s == k - 1) & (n == TP - 2))
                def _():
                    x_a2a.finish(k)

        seq = pl.BlockSpec((1, S, D), lambda s, n: (s, 0, 0))
        pair = lambda rows: pl.BlockSpec((1, 1, rows, S), lambda s, n: (s, slot_at(n), 0, 0))
        pltpu.emit_pipeline(body, grid=(NS, TP), in_specs=[seq], out_specs=[pair(R3), pair(4), pair(PW), seq])(
            r.xs, r.qkv, r.ml, r.o, r.x1)

    def mlp(h2_v, dy_v, wu_v, wd_v, yacc, acc):
        rs = GradScatter(pc, acc, r.landing, r.m_stage, r.m_r1, r.m_r2, r.m_sem, r.free)

        def is_own(i):
            return (i == 2) | (i == 4) | (i == 5) | (i == 7)

        def role_at(i):
            return jnp.where((i == 0) | (i == 5), 3, jnp.where(i < 3, 0, jnp.where(i < 5, 1, 2)))

        def slot_at(i):
            return 2 * role_at(i) + jnp.where(is_own(i), pc.c, 1 - pc.c)

        early = lambda b: remote(acc.at[b], r.m_r0, r.m_sem.at[9], r.m_sem.at[10], pc.partner)

        def landed(i):
            @pl.when(i == 5)
            def _():
                wait_for(r.m_r0, r.m_sem.at[10])
                cp = pltpu.make_async_copy(r.m_r0, r.landing, r.tmp.at[0])
                cp.start()
                cp.wait()

            pl.when(i != 5)(rs.landed)

        def weights(slot, b):
            return (pltpu.make_async_copy(r.wu_all.at[slot], wu_v.at[b], r.w_sem.at[0, b]),
                    pltpu.make_async_copy(r.wd_all.at[slot], wd_v.at[b], r.w_sem.at[1, b]))

        def fetch(i):
            slot = slot_at(i)

            @pl.when(jnp.logical_not(is_own(i)))
            def _():
                g_wu.arrived(slot)
                g_wd.arrived(slot)

            for cp in weights(slot, lax.rem(i, 2)):
                cp.start()

        fetch(jnp.int32(0))
        cps = []
        for s in range(NS):
            dy_a2a.finish(s)
            cps.append(pltpu.make_async_copy(r.dys.at[s], dy_v.at[pl.ds(s * S, S)], r.tmp.at[s]))
            cps[s].start()
        clear(yacc, r.dacc, r.gbu)
        for cp in cps:
            cp.wait()

        def step(n, carry):
            i, t = lax.div(n, NT), lax.rem(n, NT)
            b = lax.rem(i, 2)
            slot = slot_at(i)

            @pl.when(t == 0)
            def _():
                for cp in weights(slot, b):
                    cp.wait()
                clear(acc.at[b])

            @pl.when((t == NT - 1) & (i != 0) & (i != 2) & (i < TP - 1))
            def _():
                fetch(i + 1)

            rows = pl.ds(pl.multiple_of(t * TT, TT), TT)
            h2, dy = h2_v[rows, :], dy_v[rows, :]
            wu, wd = wu_v[b], wd_v[b]
            bias = r.bs_all[slot]
            bias = jnp.concatenate([bias[k:k + 1] for k in range(4, TP)], axis=1)
            pre = nn(h2, wu) + bias
            d_act = nt(dy, wd)
            cdf = 0.5 * (1.0 + lax.erf(pre * INV_SQRT2))
            act = (pre * cdf).astype(bf16)
            d_pre = d_act * (cdf + pre * jnp.exp(-0.5 * pre * pre) * INV_SQRT_2PI)
            d_pre_b = d_pre.astype(bf16)
            yacc[rows, :] += nn(act, wd)
            r.dacc[rows, :] += nt(d_pre_b, wu)
            acc[b, :FB, :] += tn(act, dy)
            acc[b, FB:, :] += tn(d_pre_b, h2)
            r.gbu[slot] += over_rows(jnp.sum, d_pre)

            done = (t == NT - 1)
            pl.when(done & (i == 0))(lambda: early(b).start())
            pl.when(done & (i > 0) & jnp.logical_not(is_own(i)))(lambda: rs.send_pair(b, i > 1))
            pl.when(done & is_own(i))(lambda: rs.settle(role_at(i), b, lambda: landed(i), i != 4))
            pl.when((t == 0) & (i == 1))(lambda: early(1 - b).wait_send())
            pl.when((t == 0) & (i > 1) & jnp.logical_not(is_own(i - 1)))(lambda: rs.sent_pair(1 - b))

            for when, hops in ((1, ("forward_a", "start_b")), (4, ("last",)), (5, ()), (9, ("forward_b",))):
                @pl.when(n == when)
                def _():
                    for hop in hops:
                        for gather in (g_wu, g_wd):
                            getattr(gather, hop)()
                    if when in (1, 5):
                        fetch(i + 1)

            return carry

        lax.fori_loop(0, TP * NT, step, 0)
        cps = load_all([(r.x1.at[s], h2_v.at[pl.ds(s * S, S)]) for s in range(NS)], r.tmp)
        stores = []
        for s in range(NS):
            rows = pl.ds(s * S, S)
            cps[s].wait()
            dy_v[rows, :] = (h2_v[rows, :].astype(f32) + (yacc[rows, :] + b_down[...])).astype(bf16)
            cp = pltpu.make_async_copy(dy_v.at[rows], r.y_seq.at[s], r.tmp.at[NS + s])
            cp.start()
            stores.append(cp)
        for s in range(NS):
            stores[s].wait()
            y_a2a.start(s)

    tok = vm(NS * S, D, dtype=bf16)

    def forward_and_mlp(h2_v, dy_v, wu_v, wd_v):
        pl.run_scoped(functools.partial(attn_fwd, h2_v), vm(TP, R3, D, dtype=bf16), vm(TP, PW, D, dtype=bf16),
                      vm(S, D, dtype=bf16), vm(D, S, dtype=bf16))
        pl.run_scoped(functools.partial(mlp, h2_v, dy_v, wu_v, wd_v), vm(NS * S, D), vm(2, 2 * FB, D))

    pl.run_scoped(forward_and_mlp, tok, tok, vm(2, D, FB, dtype=bf16), vm(2, FB, D, dtype=bf16))

    rs_m = GradScatter(pc, r.landing, r.landing, r.m_stage, r.m_r1, r.m_r2, r.m_sem, r.free)

    def attn_bwd(h1_s, do_s, acc, gb_a):
        gx_a2a = AllToAll(pc, r.gx_out, h1_s, r.gx_ss, r.gx_rs, False)

        def open_bwd(wo_v):
            wo_cp = pltpu.make_async_copy(r.wo_all, wo_v, r.tmp.at[0])
            wo_cp.start()
            wo_cp.wait()
            clear(r.va, acc, gb_a)

            def body(x_ref, x1_ref, dy_ref, o_ref):
                s = pl.program_id(0)
                rows = pl.ds(pl.multiple_of(s * S, S), S)
                dy, dh2 = dy_ref[0].astype(f32), r.dacc[rows, :]
                xh2, inv2 = ln_stats(x1_ref[0].astype(f32))
                d = dy + ln_grad(dh2, xh2, inv2, gain2[...])
                r.dacc[rows, :] = d
                db = d.astype(bf16)
                r.va[0:1, :] += over_rows(jnp.sum, dy)
                r.va[1:2, :] += over_rows(jnp.sum, dh2 * xh2)
                r.va[2:3, :] += over_rows(jnp.sum, dh2)
                r.va[3:4, :] += over_rows(jnp.sum, d)
                xh, _ = ln_stats(x_ref[0].astype(f32))
                h1_s[s] = (xh * gain1[...] + bias1[...]).astype(bf16)
                do_s[s] = nt(wo_v[...].reshape(TP * PW, D), db).astype(bf16)
                acc[:, R3:, :] += nn(o_ref[0].reshape(TP * PW, S), db).reshape(TP, PW, D)

            seq = pl.BlockSpec((1, S, D), lambda s: (s, 0, 0))
            pltpu.emit_pipeline(body, grid=(NS,), in_specs=[seq, seq, seq, pl.BlockSpec((1, TP, PW, S), lambda s: (s, 0, 0, 0))])(
                r.xs, r.x1, r.dys, r.o)

        pl.run_scoped(open_bwd, vm(TP, PW, D, dtype=bf16))
        n_half = NS // 2
        rs = GradScatter(pc, acc, r.landing.at[pl.ds(0, R3 + PW)], r.a_stage, r.a_r1, r.landing, r.a_sem, r.free)

        def slot_at(g):
            return jnp.where(g < 4, lax.rem(g + 2, 4), g)

        def heads(dq_s, wq_v, buf):
            wq_cp = pltpu.make_async_copy(r.wq_all, wq_v, r.tmp.at[1])
            wq_cp.start()
            for half in range(2):
                def body(qkv_ref, ml_ref):
                    n, sh = pl.program_id(0), pl.program_id(1)
                    g = slot_at(n)
                    s = half * n_half + sh
                    cos, sin = r.cos[...], r.sin[...]
                    ok = key_mask(r.mask[s])

                    def rot_back(t):
                        a, b = t[:HH], t[HH:]
                        return jnp.concatenate([a * cos + b * sin, b * cos - a * sin], axis=0)

                    base = pl.multiple_of(g * R3, PW)
                    for h in range(2):
                        lo = h * HD
                        qkv, ml = qkv_ref.at[0, 0], ml_ref.at[0, 0]
                        q, k, v = (qkv[j * PW + lo:j * PW + lo + HD, :] for j in range(3))
                        do = do_s[s, pl.ds(pl.multiple_of(g * PW + lo, HD), HD), :]
                        sc = masked_scores(q, k, ok)
                        p = jnp.exp(sc - ml[h:h + 1, :]) * ml[2 + h:3 + h, :]
                        dp = tn(v, do)
                        ds = (p * (dp - over_rows(jnp.sum, dp * p))).astype(bf16)
                        dv = nt(p.astype(bf16), do).T
                        dk = rot_back(nt(ds, q).T)
                        dq = rot_back(nn(k, ds)) * QS
                        for j, t in enumerate((dq, dk, dv)):
                            at = pl.ds(base + j * PW + lo, HD)
                            dq_s[sh, at, :] = t.astype(bf16)
                            gb_a[at, :] += over_cols(jnp.sum, t)

                    acc[g, :R3, :] += nn(dq_s[sh, pl.ds(base, R3), :], h1_s[s])
                    if half == 0:
                        @pl.when((sh == 0) & (n == 1))
                        def _():
                            rs_m.second([buf, r.landing.at[pl.ds(FB, FB)]], r.chunk, [r.m_stage.at[2]])
                            rs_m.send_second()
                    else:
                        @pl.when(sh == n_half - 1)
                        def _():
                            rs.block_done(g, g)

                            @pl.when(n > 0)
                            def _():
                                rs.later(slot_at(n - 1), slot_at(n - 1), n < TP - 1)

                pair = lambda rows: pl.BlockSpec((1, 1, rows, S), lambda n, sh: (half * n_half + sh, slot_at(n), 0, 0))
                pltpu.emit_pipeline(body, grid=(TP, n_half), in_specs=[pair(R3), pair(4)])(r.qkv, r.ml)
                if half == 0:
                    wq_cp.wait()

                def close_bwd(x_ref):
                    sh = pl.program_id(0)
                    s = half * n_half + sh
                    rows = pl.ds(pl.multiple_of(s * S, S), S)
                    dh1 = tn(dq_s[sh], wq_v[...].reshape(TP * R3, D))
                    xh, inv = ln_stats(x_ref[0].astype(f32))
                    r.va[4:5, :] += over_rows(jnp.sum, dh1 * xh)
                    r.va[5:6, :] += over_rows(jnp.sum, dh1)
                    h1_s[s] = (r.dacc[rows, :] + ln_grad(dh1, xh, inv, gain1[...])).astype(bf16)
                    gx_a2a.start(s)
                    cp = gx_a2a.local_out(s, h1_s)
                    cp.start()
                    cp.wait()

                pltpu.emit_pipeline(close_bwd, grid=(n_half,),
                                    in_specs=[pl.BlockSpec((1, S, D), lambda sh: (half * n_half + sh, 0, 0))])(r.xs)
            last = jnp.int32(TP - 1)
            rs.later(last, last, False)
            rs.second([buf, r.landing.at[pl.ds(FB, FB)]], r.chunk, [r.gq_b, r.go_b])

        pl.run_scoped(heads, vm(n_half, TP * R3, S, dtype=bf16), vm(TP, R3, D, dtype=bf16), vm(FB, D))

        for g in range(TP):
            r.msg[g] = r.va[...]
            for j in range(3):
                cols = jnp.broadcast_to(gb_a[g * R3 + j * PW:g * R3 + (j + 1) * PW, :], (PW, PW))
                r.msg[g, 6:7, j * PW:(j + 1) * PW] = cols.T[0:1, :]
            r.msg[g, 6:7, R3:R3 + FB] = r.gbu[g]
        pair = remote(r.msg, r.msg_in, r.s_ss.at[0], r.s_rs.at[0], pc.partner)
        pair.start()
        pair.wait()
        r.msg_in[...] = r.msg_in[...] + r.msg[...]
        chip = lax.div(pc.me, 2)
        small = [remote(r.msg_in.at[pc.slot_of(m)], r.msgs.at[chip], r.s_ss.at[1], r.s_rs.at[1], pc.peer(m)) for m in (2, 4, 6)]
        for cp in small:
            cp.start()
        own = pltpu.make_async_copy(r.msg_in.at[pc.slot_of(0)], r.msgs.at[chip], r.s_ss.at[2])
        own.start()

        def tail(bufs, act_v, turned):
            b0, b1, b2 = (bufs.at[i] for i in range(3))
            y_own = [(pltpu.make_async_copy(r.y_seq.at[s, y_a2a._rows(pc.me)], act_v.at[s], r.tmp.at[s]),
                      pltpu.make_async_copy(act_v.at[s], r.y_out.at[pc.me * NS + s], r.tmp.at[NS + s])) for s in range(NS)]
            for load, _ in y_own:
                load.start()
            for load, store in y_own:
                load.wait()
                store.start()
            for g in (g_bs, g_wq, g_wo, g_wu, g_wd):
                g.sent()
            for _, store in y_own:
                store.wait()
            rs_m.finish()
            wait_for(r.m_r1.at[0], r.m_sem.at[4])
            for p in range(2):
                half = pl.ds(p * FB, FB)
                for cp in load_all([(r.m_stage.at[3, half], b0), (r.m_r1.at[0, half], b1), (r.m_r2.at[half], b2)], r.tmp):
                    cp.wait()
                row_add(b0, [b1, b2])
                if p == 0:
                    cp = pltpu.make_async_copy(b0, r.gd, r.tmp.at[0])
                else:
                    for k in range(D // FB):
                        cols = slice(k * FB, (k + 1) * FB)
                        turned[cols, :] = b0[:, cols].T
                    cp = pltpu.make_async_copy(turned, r.gu, r.tmp.at[0])
                cp.start()
                cp.wait()
            rs.own_part(b0, b1, r.tmp)
            for s in range(NS):
                y_a2a.finish(s)
            for s in range(NS):
                gx_a2a.finish(s)
            rs.sent_first()
            own.wait()
            for sem in (r.s_ss.at[1], r.s_rs.at[1]):
                wait_for(r.msgs.at[pl.ds(0, len(small))], sem)

        pl.run_scoped(tail, vm(3, FB, D), vm(NS, SL, D, dtype=bf16), vm(D, FB))

    seqs = vm(NS, S, D, dtype=bf16)
    pl.run_scoped(attn_bwd, seqs, vm(NS, D, S, dtype=bf16), vm(TP, R3 + PW, D), vm(TP * R3, 1))


def layer_call(*args):
    out = pl.pallas_call(
        layer_kernel,
        in_specs=[ANY] * len(IN_NAMES),
        out_specs=[ANY] * len(OUT_SHAPES),
        out_shape=[sds(*v) for v in OUT_SHAPES.values()],
        scratch_shapes=list(SCRATCH.values()),
        compiler_params=pltpu.CompilerParams(collective_id=0, has_side_effects=True, vmem_limit_bytes=VMEM_LIMIT),
        name="layer",
    )(*args)
    return out[:8]


FINAL = {"y": ((TP * NS, SL, D), bf16), "gx": ((TP * NS, SL, D), bf16), "gd": ((FB, D), f32), "gu": ((D, FB), f32),
         "gbq": ((3, 2, HD), f32), "gbu": ((1, FB), f32)}
VECS = ("bd", "g2", "b2", "bo", "g1", "b1")
FINAL |= {k: ((1, D), f32) for k in VECS}
LATE = ("gbq", "gbu") + VECS


def final_kernel(y_in, gx_in, msgs, gd_in, gu_in, *refs):
    outs, refs = Refs(FINAL, refs), refs[len(FINAL):]
    msg_v, y_v, gx_v, gd_v, gu_v, ld, st = refs[:7]
    late = Refs(LATE, refs[7:])
    moves = [([(msgs, msg_v)], [])]
    for src, buf, dst in ((gd_in, gd_v, outs.gd), (gu_in, gu_v, outs.gu), (y_in, y_v, outs.y), (gx_in, gx_v, outs.gx)):
        moves.append(([(src, buf)], [(buf, dst)]))
    copy = pltpu.make_async_copy
    loads = [[copy(s, d, ld.at[i]) for s, d in m[0]] for i, m in enumerate(moves)]
    stores = [[copy(s, d, st.at[i]) for s, d in m[1]] for i, m in enumerate(moves)]
    for cps in loads:
        for cp in cps:
            cp.start()
    for i, (cps, outward) in enumerate(zip(loads, stores)):
        for cp in cps:
            cp.wait()
        if i == 0:
            small = msg_v[0]
            for j in range(1, msg_v.shape[0]):
                small = small + msg_v[j]
            for j, k in enumerate(VECS):
                getattr(late, k)[...] = small[j:j + 1, :]
            for j in range(3):
                for h in range(2):
                    lo = j * PW + h * HD
                    late.gbq[j, h:h + 1, :] = small[6:7, lo:lo + HD]
            late.gbu[...] = small[6:7, R3:R3 + FB]
        for cp in outward:
            cp.start()
    small_out = load_all([(getattr(late, k), getattr(outs, k)) for k in LATE], st.at[pl.ds(len(moves), len(LATE))])
    for cps in stores + [small_out]:
        for cp in cps:
            cp.wait()


def final_call(y, gx, msgs, gd, gu):
    act = vm(*y.shape, dtype=bf16)
    return pl.pallas_call(
        final_kernel,
        in_specs=[ANY] * 5,
        out_specs=[ANY] * len(FINAL),
        out_shape=[sds(*v) for v in FINAL.values()],
        scratch_shapes=[vm(*msgs.shape), act, act, vm(FB, D), vm(D, FB), DMA((5,)), DMA((5 + len(LATE),))]
        + [vm(*FINAL[k][0]) for k in LATE],
        compiler_params=pltpu.CompilerParams(vmem_limit_bytes=VMEM_LIMIT),
        cost_estimate=pl.CostEstimate(flops=10 ** 10, bytes_accessed=3 * 10 ** 7, transcendentals=0),
        name="results",
    )(y, gx, msgs, gd, gu)


def rope_tables():
    inv_freq = (ROPE_BASE ** (-2.0 * np.arange(HH, dtype=np.float32) / HD)).astype(np.float32)
    angles = np.outer(inv_freq, np.arange(S, dtype=np.float32))
    return np.cos(angles), np.sin(angles)


def solution(mesh):
    no = None
    act_spec = P('dp', 'tp', no)
    rep, part = P(no), P('dp')
    in_specs = (act_spec, act_spec, P('dp', no), rep, rep, P(no, no, 'tp', no), P(no, 'tp', no),
                P('tp', no, no), rep, rep, rep, P(no, 'tp'), P('tp'), P('tp', no), rep)
    out_specs = (act_spec, act_spec, part, part, P('dp', no, 'tp', no), P('dp', 'tp', no), P(('dp', 'tp'), no, no),
                 part, part, part, P('dp', 'tp'), P(('dp', 'tp')), P(('dp', 'tp'), no), part)

    def device_step(x_in, grad_y, pad_mask, ln1_gain, ln1_bias, w_qkv, b_qkv, w_out, b_out, ln2_gain, ln2_bias, w_up, b_up, w_down, b_down):
        assert x_in.shape == (TP * NS, SL, D) and w_qkv.shape == (3, D, 2, HD) and w_up.shape == (D, FB)
        row = lambda v: v.reshape(1, -1)
        wq = w_qkv.transpose(0, 2, 3, 1).reshape(R3, D)
        cos, sin = rope_tables()
        parts = layer_call(
            x_in, grad_y, wq, w_out.reshape(PW, D), w_up, w_down, b_qkv, row(b_up), pad_mask, cos, sin,
            row(ln1_gain), row(ln1_bias), row(ln2_gain), row(ln2_bias), row(b_out), row(b_down))
        *parts, stage, gq_b, go_b = parts
        to_b = [(i, i ^ (4 - 2 * (i % 2))) for i in range(TP)]
        gq = stage[-1, :R3] + lax.ppermute(gq_b, 'tp', to_b)
        go = lax.ppermute(go_b, 'tp', to_b)
        gq, stage = lax.optimization_barrier((gq, stage))
        go = stage[-1, R3:] + go
        y, gx, gd, gu, gbq, gbu, *vecs = final_call(*parts)
        bd, g2, b2, bo, g1, b1 = (v.reshape(D) for v in vecs)
        return (y, gx, g1, b1, gq.reshape(3, 2, HD, D).transpose(0, 3, 1, 2), gbq, go.reshape(2, HD, D), bo, g2, b2,
                gu, gbu.reshape(FB), gd, bd)

    return jax.shard_map(device_step, mesh=mesh, in_specs=in_specs, out_specs=out_specs, check_vma=False)
```

```python
import functools

import jax
import jax.numpy as jnp
import numpy as np
from jax import lax
from jax.experimental import pallas as pl
from jax.experimental.pallas import tpu as pltpu
from jax.sharding import PartitionSpec as P

f32 = jnp.float32
bf16 = jnp.bfloat16
LN_EPS = 1e-5
ROPE_BASE = 10000.0
INV_SQRT2 = 0.7071067811865476
INV_SQRT_2PI = 0.3989422804014327
NEG_LARGE = -1e30
MESH = pl.DeviceIdType.MESH
ANY = pl.BlockSpec(memory_space=pl.ANY)
VMEM_LIMIT = 66_000_000

TP = 8
NS = 4
S = 512
D = 1024
PW = 128
HD = 64
HH = HD // 2
FB = 512
SL = 64
QS = HD ** -0.5
R3 = 3 * PW
ROWS = 8


def dg(a, b, ca, cb):
    return lax.dot_general(a, b, (((ca,), (cb,)), ((), ())), preferred_element_type=f32)


def nn(a, b):
    return dg(a, b, 1, 0)


def nt(a, b):
    return dg(a, b, 1, 1)


def tn(a, b):
    return dg(a, b, 0, 0)


def over_rows(reduce, v):
    return reduce(v, axis=0, keepdims=True)


def over_cols(reduce, v):
    return reduce(v, axis=1, keepdims=True)


def sds(shape, dtype):
    return jax.ShapeDtypeStruct(shape, dtype)


class Place:
    def __init__(self):
        me = lax.axis_index("tp")
        self.me = me
        self.c = lax.rem(me, 2)
        self.dc = 1 - 2 * self.c
        self.dx = 2 - 4 * lax.rem(lax.div(me, 2), 2)
        self.dy = 4 - 8 * lax.div(me, 4)
        self.partner = me + self.dc
        self.a = me + (1 - self.c) * self.dx + self.c * self.dy
        self.b = me + (1 - self.c) * self.dy + self.c * self.dx

    def peer(self, m):
        return self.me + (m & 1) * self.dc + ((m >> 1) & 1) * self.dx + (m >> 2) * self.dy

    def slot_of(self, m):
        k = self.c if m % 2 == 0 else 1 - self.c
        lo, hi = {0: (6, 7), 1: (0, 5), 2: (4, 1), 3: (2, 3)}[m >> 1]
        return lo + k * (hi - lo)


def remote(src, dst, send_sem, recv_sem, device):
    return pltpu.make_async_remote_copy(src_ref=src, dst_ref=dst, send_sem=send_sem, recv_sem=recv_sem,
                                        device_id={"tp": device}, device_id_type=MESH)


def wait_for(ref, sem):
    pltpu.make_async_copy(ref, ref, sem).wait()


def entry_barrier(pc):
    bar = pltpu.get_barrier_semaphore()
    for m in range(1, TP):
        pl.semaphore_signal(bar, inc=1, device_id={"tp": pc.peer(m)}, device_id_type=MESH)
    pl.semaphore_wait(bar, TP - 1)


class AllToAll:
    def __init__(self, pc, pos_ref, seq_ref, send_sem, recv_sem, inward):
        self.pc, self.pos, self.seq, self.ss, self.rs, self.inward = pc, pos_ref, seq_ref, send_sem, recv_sem, inward

    def _rows(self, dev):
        return pl.ds(pl.multiple_of(dev * SL, SL), SL)

    def _copy(self, s, m):
        pc, dev = self.pc, self.pc.peer(m)
        if self.inward:
            src, dst = self.pos.at[dev * NS + s], self.seq.at[s, self._rows(pc.me)]
        else:
            src, dst = self.seq.at[s, self._rows(dev)], self.pos.at[pc.me * NS + s]
        one = s if self.inward else 0
        return remote(src, dst, self.ss.at[one], self.rs.at[one], dev)

    def start(self, s):
        for m in (*range(2, TP), 1):
            self._copy(s, m).start()

    def start_all(self):
        for m in (*range(2, TP), 1):
            pc, dev = self.pc, self.pc.peer(m)
            if self.inward:
                src, dst = self.pos.at[pl.ds(dev * NS, NS)], self.seq.at[:, self._rows(pc.me)]
            else:
                src, dst = self.seq.at[:, self._rows(dev)], self.pos.at[pl.ds(pc.me * NS, NS)]
            remote(src, dst, self.ss.at[0], self.rs.at[0], dev).start()

    def finish_all(self):
        rest = self.seq.at[:, pl.ds(0, S - SL)]
        wait_for(rest, self.ss.at[0])
        wait_for(rest, self.rs.at[0])

    def finish(self, s):
        all_rows = self.seq.at[s, pl.ds(0, S - SL)]
        wait_for(all_rows, self.ss.at[s])
        wait_for(all_rows, self.rs.at[s])

    def local_in(self, buf):
        pc = self.pc
        return (pltpu.make_async_copy(self.pos.at[pl.ds(pc.me * NS, NS)], buf, self.ss.at[self.ss.shape[0] - 1]),
                pltpu.make_async_copy(buf, self.seq.at[:, self._rows(pc.me)], self.rs.at[self.rs.shape[0] - 1]))

    def local_out(self, s, src):
        return pltpu.make_async_copy(src.at[s, self._rows(self.pc.me)], self.pos.at[self.pc.me * NS + s], self.ss.at[self.ss.shape[0] - 1])


class Gather:
    def __init__(self, pc, src_ref, dst_ref, send_sem, recv_sem):
        self.pc, self.src, self.dst, self.ss, self.rs = pc, src_ref, dst_ref, send_sem, recv_sem

    def _send(self, src, slot, dev):
        return remote(src, self.dst.at[slot], self.ss, self.rs.at[slot], dev)

    def _direct(self):
        pc, c = self.pc, self.pc.c
        return [self._send(self.src, c, pc.a), self._send(self.src, 6 + c, pc.partner),
                self._send(self.src, 4 + c, pc.b)]

    def _hop(self):
        pc, c = self.pc, self.pc.c
        return [self._send(self.dst.at[c], 2 + c, pc.b), self._send(self.dst.at[c], c, pc.partner),
                self._send(self.dst.at[4 + c], 4 + c, pc.partner)]

    def _last(self):
        pc, c = self.pc, self.pc.c
        return self._send(self.dst.at[2 + c], 2 + c, pc.partner)

    def arrived(self, slot):
        wait_for(self.dst.at[slot], self.rs.at[slot])

    def start(self):
        self.start_a()
        self.start_b()

    def start_a(self):
        for cp in self._direct()[:2]:
            cp.start()

    def start_b(self):
        self._direct()[2].start()

    def forward(self):
        self.forward_a()
        self.forward_b()

    def forward_a(self):
        hop = self._hop()
        self.arrived(self.pc.c)
        hop[0].start()
        hop[1].start()

    def forward_b(self):
        self.arrived(4 + self.pc.c)
        self._hop()[2].start()

    def last(self):
        self.arrived(2 + self.pc.c)
        self._last().start()

    def local(self, buf):
        return (pltpu.make_async_copy(self.src, buf, self.rs.at[TP]),
                pltpu.make_async_copy(buf, self.dst.at[6 + self.pc.c], self.rs.at[6 + self.pc.c]))

    def arrived_near(self):
        for j in (0, 2, 3):
            self.arrived(2 * j + 1 - self.pc.c)
        self.arrived(6 + self.pc.c)

    def arrived_far(self):
        self.arrived(3 - self.pc.c)

    def sent(self):
        wait_for(self.dst.at[pl.ds(0, TP - 1)], self.ss)


def row_add(acc, others):
    step = 64

    def body(i, carry):
        r = pl.ds(pl.multiple_of(i * step, step), step)
        v = acc[r, :]
        for o in others:
            v = v + o[r, :]
        acc[r, :] = v
        return carry

    lax.fori_loop(0, acc.shape[0] // step, body, 0)


class GradScatter:
    def __init__(self, pc, acc, landing, stage, r1, r2, sems, free):
        self.pc, self.acc, self.landing, self.stage, self.r1, self.r2 = pc, acc, landing, stage, r1, r2
        self.sem, self.free = sems, free

    def _pair(self, b):
        return remote(self.acc.at[b], self.landing, self.sem.at[0], self.sem.at[1], self.pc.partner)

    def _first(self, j):
        return remote(self.stage.at[j], self.r1.at[j], self.sem.at[2 + j], self.sem.at[4 + j], self.pc.a)

    def _second(self):
        return remote(self.stage.at[2], self.r2, self.sem.at[6], self.sem.at[7], self.pc.b)

    def send_pair(self, b, needs_credit):
        @pl.when(needs_credit)
        def _():
            pl.semaphore_wait(self.free, 1)

        self._pair(b).start()

    def sent_pair(self, b):
        self._pair(b).wait_send()

    def settle(self, j, b, landed, gives_credit):
        landed()
        row_add(self.acc.at[b], [self.landing])

        @pl.when(gives_credit)
        def _():
            pl.semaphore_signal(self.free, inc=1, device_id={"tp": self.pc.partner}, device_id_type=MESH)

        store = pltpu.make_async_copy(self.acc.at[b], self.stage.at[j], self.sem.at[8])
        store.start()
        store.wait()

        @pl.when(j < 2)
        def _():
            self._first(j).start()

    def landed(self):
        wait_for(self.landing, self.sem.at[1])

    def block_done(self, slot, b):
        pl.when(lax.rem(slot, 2) != self.pc.c)(lambda: self.send_pair(b, True))

    def later(self, slot, b, gives_credit):
        own = lax.rem(slot, 2) == self.pc.c
        pl.when(own)(lambda: self.settle(lax.div(slot, 2), b, self.landed, gives_credit))
        pl.when(jnp.logical_not(own))(lambda: self.sent_pair(b))

    def second(self, bufs, chunk_sem, dsts):
        n = chunk_sem.shape[0] // 3
        size = bufs[0].shape[0]
        rows = size // n
        part = lambda ref, k: ref.at[pl.ds(k * rows, rows)]
        wait_for(self.r1.at[1], self.sem.at[5])
        dsts = [part(d, k) for d in dsts for k in range(d.shape[0] // rows)]
        for p in range(self.stage.shape[1] // size):
            mine, theirs = (ref.at[pl.ds(p * size, size)] for ref in (self.stage.at[2], self.r1.at[1]))
            loads = [[pltpu.make_async_copy(part(src, k), part(buf, k), chunk_sem.at[x * n + k])
                      for x, (src, buf) in enumerate(zip((mine, theirs), bufs))] for k in range(n)]
            stores = [pltpu.make_async_copy(part(bufs[0], k), dsts[p * n + k], chunk_sem.at[2 * n + k]) for k in range(n)]
            for group in loads:
                for cp in group:
                    cp.start()
            for k in range(n):
                for cp in loads[k]:
                    cp.wait()
                row_add(part(bufs[0], k), [part(bufs[1], k)])
                stores[k].start()
            for cp in stores:
                cp.wait()

    def send_second(self):
        self._second().start()

    def own_part(self, b0, b1, sem):
        wait_for(self.r1.at[0], self.sem.at[4])
        for cp in load_all([(self.stage.at[3], b0), (self.r1.at[0], b1)], sem):
            cp.wait()
        row_add(b0, [b1])
        cp = pltpu.make_async_copy(b0, self.stage.at[3], sem.at[0])
        cp.start()
        cp.wait()

    def sent_first(self):
        for j in range(2):
            self._first(j).wait_send()

    def finish(self):
        self.sent_first()
        self._second().wait()


def ln_stats(v):
    c = v - over_cols(jnp.mean, v)
    inv = lax.rsqrt(over_cols(jnp.mean, c * c) + LN_EPS)
    return c * inv, inv


def ln_grad(d_out, x_hat, inv, gain):
    dh = d_out * gain
    return inv * (dh - over_cols(jnp.mean, dh) - x_hat * over_cols(jnp.mean, dh * x_hat))


def masked_scores(q, k, ok):
    return jnp.where(ok, tn(k, q), NEG_LARGE)


def key_mask(mask):
    return jnp.concatenate([mask] * (S // PW), axis=1) > 0


def column(row):
    return jnp.broadcast_to(row, (PW, row.shape[1])).T[:, :1]


def clear(*refs):
    for ref in refs:
        ref[...] = jnp.zeros(ref.shape, ref.dtype)


def load_all(pairs, sem):
    cps = [pltpu.make_async_copy(s, d, sem.at[i]) for i, (s, d) in enumerate(pairs)]
    for cp in cps:
        cp.start()
    return cps


def vm(*shape, dtype=f32):
    return pltpu.VMEM(shape, dtype)


TT = 1024
NT = NS * S // TT
SMALL = {
    "bqkv": vm(3, 2, HD), "bup": vm(1, FB), "pad": vm(TP * NS, S, dtype=jnp.int32), "cos": vm(HH, S), "sin": vm(HH, S),
    "gain1": vm(1, D), "bias1": vm(1, D), "gain2": vm(1, D), "bias2": vm(1, D), "b_out": vm(1, D), "b_down": vm(1, D),
}
IN_NAMES = ("x_in", "dy_in", "wq", "wo", "wu", "wd") + tuple("in_" + k for k in SMALL)
OUT_SHAPES = {
    "y_out": ((TP * NS, SL, D), bf16), "gx_out": ((TP * NS, SL, D), bf16), "msgs": ((TP // 2, ROWS, D), f32), "gd": ((FB, D), f32), "gu": ((D, FB), f32),
    "a_stage": ((4, R3 + PW, D), f32), "gq_b": ((R3, D), f32), "go_b": ((PW, D), f32), "a_r1": ((2, R3 + PW, D), f32),
    "m_r0": ((2 * FB, D), f32), "m_stage": ((4, 2 * FB, D), f32), "m_r1": ((2, 2 * FB, D), f32), "m_r2": ((2 * FB, D), f32),
    "xs": ((NS, S, D), bf16), "dys": ((NS, S, D), bf16), "wq_all": ((TP, R3, D), bf16), "wo_all": ((TP, PW, D), bf16),
    "wu_all": ((TP, D, FB), bf16), "wd_all": ((TP, FB, D), bf16),
    "qkv": ((NS, TP, R3, S), bf16), "ml": ((NS, TP, 4, S), f32), "o": ((NS, TP, PW, S), bf16),
    "x1": ((NS, S, D), bf16), "y_seq": ((NS, S, D), bf16),
}
DMA = pltpu.SemaphoreType.DMA
SCRATCH = SMALL | {
    "bs_all": vm(TP, ROWS, PW), "bs": vm(ROWS, PW), "mask": vm(NS, S, PW), "dacc": vm(NS * S, D), "landing": vm(2 * FB, D), "gbu": vm(TP, 1, FB), "va": vm(ROWS, D),
    "msg": vm(TP, ROWS, D), "msg_in": vm(TP, ROWS, D),
    "free": pltpu.SemaphoreType.REGULAR,
    "x_ss": DMA((NS + 1,)), "x_rs": DMA((NS + 1,)), "dy_ss": DMA((2,)), "dy_rs": DMA((2,)),
    "y_ss": DMA((1,)), "y_rs": DMA((1,)), "gx_ss": DMA((2,)), "gx_rs": DMA((1,)),
    "g_ss": DMA((5,)), "g_rs": DMA((5, TP + 1)), "m_sem": DMA((11,)), "a_sem": DMA((9,)), "s_ss": DMA((3,)), "s_rs": DMA((2,)),
    "tmp": DMA((TP,)), "chunk": DMA((12,)), "w_sem": DMA((2, 2)),
}


class Refs:
    def __init__(self, names, refs):
        for n, r in zip(names, refs):
            setattr(self, n, r)


def layer_kernel(*refs):
    r = Refs(IN_NAMES + tuple(OUT_SHAPES) + tuple(SCRATCH), refs)
    pc = Place()
    small_in = load_all([(getattr(r, "in_" + k), getattr(r, k)) for k in SMALL], r.chunk)
    entry_barrier(pc)
    x_a2a = AllToAll(pc, r.x_in, r.xs, r.x_ss, r.x_rs, True)
    dy_a2a = AllToAll(pc, r.dy_in, r.dys, r.dy_ss, r.dy_rs, True)
    y_a2a = AllToAll(pc, r.y_out, r.y_seq, r.y_ss, r.y_rs, False)
    g_bs, g_wq, g_wo, g_wu, g_wd = [
        Gather(pc, s, d, r.g_ss.at[i], r.g_rs.at[i])
        for i, (s, d) in enumerate(((r.bs, r.bs_all), (r.wq, r.wq_all), (r.wo, r.wo_all), (r.wu, r.wu_all), (r.wd, r.wd_all)))]
    gain1, bias1, gain2, bias2, b_out, b_down = r.gain1, r.bias1, r.gain2, r.bias2, r.b_out, r.b_down

    def arrivals(b_x, b_dy, b_q, b_o, b_u, b_d):
        first = (g_bs, g_wq, g_wo)
        for g in first[1:]:
            g.start()
        x_a2a.start(0)
        for cp in small_in:
            cp.wait()
        for i in range(3):
            for h in range(2):
                r.bs[pl.ds(i, 1), pl.ds(h * HD, HD)] = r.bqkv[i, pl.ds(h, 1), :]
        for k in range(FB // PW):
            r.bs[pl.ds(4 + k, 1), :] = r.bup[:, pl.ds(k * PW, PW)]
        local = [x_a2a.local_in(b_x), dy_a2a.local_in(b_dy)]
        local += [g.local(b) for g, b in ((g_wq, b_q), (g_wo, b_o), (g_wu, b_u), (g_wd, b_d))]
        for load, _ in local:
            load.start()
        for s in range(NS):
            keys = jnp.broadcast_to(r.pad[pl.ds(pc.me * NS + s, 1), :].astype(f32), (PW, S))
            r.mask[s] = keys.T
        g_bs.start()
        pltpu.make_async_copy(r.bs, r.bs_all.at[6 + pc.c], r.g_rs.at[0, 6 + pc.c]).start()
        for load, store in local:
            load.wait()
            store.start()
        for g in (g_wq, g_wo, g_bs):
            g.forward_a()
        for g in (g_wq, g_wo, g_bs):
            g.forward_b()
        x_a2a.finish(0)
        x_a2a.start(1)
        for g in first:
            g.arrived_near()
        for g in (g_wu, g_wd):
            g.arrived(6 + pc.c)
        local[0][1].wait()
        local[1][1].wait()

    def later_arrivals():
        for g in (g_bs, g_wq, g_wo):
            g.last()
        for s in range(2, NS):
            x_a2a.start(s)
        dy_a2a.start_all()
        g_wu.start_a()
        g_wd.start_a()
        for g in (g_bs, g_wq, g_wo):
            g.arrived_far()

    act = vm(NS, SL, D, dtype=bf16)
    pl.run_scoped(arrivals, act, act, vm(R3, D, dtype=bf16), vm(PW, D, dtype=bf16), vm(D, FB, dtype=bf16), vm(FB, D, dtype=bf16))

    def attn_fwd(h2_v, wq_v, wo_v, h1_s, o_s):
        def fetch(*pairs):
            for cp in load_all(pairs, r.tmp):
                cp.wait()

        fetch(*[(r.wq_all.at[pl.ds(k, 2)], wq_v.at[pl.ds(k, 2)]) for k in (6, 0, 4)])

        def slot_at(n):
            return jnp.where(n < 2, n + 6, jnp.where(n < 4, n - 2, jnp.where(n < 6, n, n - 4)))

        def body(x_ref, qkv_ref, ml_ref, o_ref, x1_ref):
            s, n = pl.program_id(0), pl.program_id(1)
            g = slot_at(n)

            @pl.when(n == 0)
            def _():
                xh, _ = ln_stats(x_ref[0].astype(f32))
                h1_s[...] = (xh * gain1[...] + bias1[...]).astype(bf16)

            bias = r.bs_all[g]
            bias = jnp.concatenate([column(bias[i:i + 1]) for i in range(3)], axis=0)
            qkv = nt(wq_v[g], h1_s[...]) + bias
            cos, sin = r.cos[...], r.sin[...]
            ok = key_mask(r.mask[s])

            def rot(t):
                a, b = t[:HH], t[HH:]
                return jnp.concatenate([a * cos - b * sin, b * cos + a * sin], axis=0).astype(bf16)

            for h in range(2):
                lo = h * HD
                at_q, at_k, at_v = (slice(j * PW + lo, j * PW + lo + HD) for j in range(3))
                q, k, v = rot(qkv[at_q] * QS), rot(qkv[at_k]), qkv[at_v].astype(bf16)
                for at, t in ((at_q, q), (at_k, k), (at_v, v)):
                    qkv_ref[0, 0, at, :] = t
                sc = masked_scores(q, k, ok)
                m = over_rows(jnp.max, sc)
                e = jnp.exp(sc - m)
                li = 1.0 / over_rows(jnp.sum, e)
                p = (e * li).astype(bf16)
                ml = ml_ref.at[0, 0]
                ml[h:h + 1, :] = m
                ml[2 + h:3 + h, :] = li
                o = nn(v, p).astype(bf16)
                o_ref[0, 0, lo:lo + HD, :] = o
                o_s[pl.ds(pl.multiple_of(g * PW + lo, HD), HD), :] = o

            @pl.when((s == 0) & (n == 5))
            def _():
                later_arrivals()
                fetch((r.wq_all.at[pl.ds(2, 2)], wq_v.at[pl.ds(2, 2)]), (r.wo_all, wo_v))

            @pl.when(n == TP - 1)
            def _():
                attn = tn(o_s[...], wo_v[...].reshape(TP * PW, D))
                x1 = (x_ref[0].astype(f32) + (attn + b_out[...])).astype(bf16)
                x1_ref[0] = x1
                xh, _ = ln_stats(x1.astype(f32))
                h2_v[pl.ds(pl.multiple_of(s * S, S), S), :] = (xh * gain2[...] + bias2[...]).astype(bf16)

            for k in range(1, NS):
                @pl.when((s == k - 1) & (n == TP - 2))
                def _():
                    x_a2a.finish(k)

        seq = pl.BlockSpec((1, S, D), lambda s, n: (s, 0, 0))
        pair = lambda rows: pl.BlockSpec((1, 1, rows, S), lambda s, n: (s, slot_at(n), 0, 0))
        pltpu.emit_pipeline(body, grid=(NS, TP), in_specs=[seq], out_specs=[pair(R3), pair(4), pair(PW), seq])(
            r.xs, r.qkv, r.ml, r.o, r.x1)

    def mlp(h2_v, dy_v, wu_v, wd_v, yacc, acc):
        rs = GradScatter(pc, acc, r.landing, r.m_stage, r.m_r1, r.m_r2, r.m_sem, r.free)

        def is_own(i):
            return (i == 2) | (i == 4) | (i == 5) | (i == 7)

        def role_at(i):
            return jnp.where((i == 0) | (i == 5), 3, jnp.where(i < 3, 0, jnp.where(i < 5, 1, 2)))

        def slot_at(i):
            return 2 * role_at(i) + jnp.where(is_own(i), pc.c, 1 - pc.c)

        early = lambda b: remote(acc.at[b], r.m_r0, r.m_sem.at[9], r.m_sem.at[10], pc.partner)

        def landed(i):
            @pl.when(i == 5)
            def _():
                wait_for(r.m_r0, r.m_sem.at[10])
                cp = pltpu.make_async_copy(r.m_r0, r.landing, r.tmp.at[0])
                cp.start()
                cp.wait()

            pl.when(i != 5)(rs.landed)

        def weights(slot, b):
            return (pltpu.make_async_copy(r.wu_all.at[slot], wu_v.at[b], r.w_sem.at[0, b]),
                    pltpu.make_async_copy(r.wd_all.at[slot], wd_v.at[b], r.w_sem.at[1, b]))

        def fetch(i):
            slot = slot_at(i)

            @pl.when(jnp.logical_not(is_own(i)))
            def _():
                g_wu.arrived(slot)
                g_wd.arrived(slot)

            for cp in weights(slot, lax.rem(i, 2)):
                cp.start()

        fetch(jnp.int32(0))
        cps = []
        dy_a2a.finish_all()
        for s in range(NS):
            cps.append(pltpu.make_async_copy(r.dys.at[s], dy_v.at[pl.ds(s * S, S)], r.tmp.at[s]))
            cps[s].start()
        clear(yacc, r.dacc, r.gbu)
        for cp in cps:
            cp.wait()

        def step(n, carry):
            i, t = lax.div(n, NT), lax.rem(n, NT)
            b = lax.rem(i, 2)
            slot = slot_at(i)

            @pl.when(t == 0)
            def _():
                for cp in weights(slot, b):
                    cp.wait()
                clear(acc.at[b])

            @pl.when((t == NT - 1) & (i != 0) & (i != 2) & (i < TP - 1))
            def _():
                fetch(i + 1)

            rows = pl.ds(pl.multiple_of(t * TT, TT), TT)
            h2, dy = h2_v[rows, :], dy_v[rows, :]
            wu, wd = wu_v[b], wd_v[b]
            bias = r.bs_all[slot]
            bias = jnp.concatenate([bias[k:k + 1] for k in range(4, TP)], axis=1)
            pre = nn(h2, wu) + bias
            d_act = nt(dy, wd)
            cdf = 0.5 * (1.0 + lax.erf(pre * INV_SQRT2))
            act = (pre * cdf).astype(bf16)
            d_pre = d_act * (cdf + pre * jnp.exp(-0.5 * pre * pre) * INV_SQRT_2PI)
            d_pre_b = d_pre.astype(bf16)
            yacc[rows, :] += nn(act, wd)
            r.dacc[rows, :] += nt(d_pre_b, wu)
            acc[b, :FB, :] += tn(act, dy)
            acc[b, FB:, :] += tn(d_pre_b, h2)
            r.gbu[slot] += over_rows(jnp.sum, d_pre)

            done = (t == NT - 1)
            pl.when(done & (i == 0))(lambda: early(b).start())
            pl.when(done & (i > 0) & jnp.logical_not(is_own(i)))(lambda: rs.send_pair(b, i > 1))
            pl.when(done & is_own(i))(lambda: rs.settle(role_at(i), b, lambda: landed(i), i != 4))
            pl.when((t == 0) & (i == 1))(lambda: early(1 - b).wait_send())
            pl.when((t == 0) & (i > 1) & jnp.logical_not(is_own(i - 1)))(lambda: rs.sent_pair(1 - b))

            for when, hops in ((1, ("forward_a", "start_b")), (4, ("last",)), (5, ()), (9, ("forward_b",))):
                @pl.when(n == when)
                def _():
                    for hop in hops:
                        for gather in (g_wu, g_wd):
                            getattr(gather, hop)()
                    if when in (1, 5):
                        fetch(i + 1)

            return carry

        lax.fori_loop(0, TP * NT, step, 0)
        cps = load_all([(r.x1.at[s], h2_v.at[pl.ds(s * S, S)]) for s in range(NS)], r.tmp)
        stores = []
        for s in range(NS):
            rows = pl.ds(s * S, S)
            cps[s].wait()
            dy_v[rows, :] = (h2_v[rows, :].astype(f32) + (yacc[rows, :] + b_down[...])).astype(bf16)
            cp = pltpu.make_async_copy(dy_v.at[rows], r.y_seq.at[s], r.tmp.at[NS + s])
            cp.start()
            stores.append(cp)
        for cp in stores:
            cp.wait()
        y_a2a.start_all()

    tok = vm(NS * S, D, dtype=bf16)

    def forward_and_mlp(h2_v, dy_v, wu_v, wd_v):
        pl.run_scoped(functools.partial(attn_fwd, h2_v), vm(TP, R3, D, dtype=bf16), vm(TP, PW, D, dtype=bf16),
                      vm(S, D, dtype=bf16), vm(D, S, dtype=bf16))
        pl.run_scoped(functools.partial(mlp, h2_v, dy_v, wu_v, wd_v), vm(NS * S, D), vm(2, 2 * FB, D))

    pl.run_scoped(forward_and_mlp, tok, tok, vm(2, D, FB, dtype=bf16), vm(2, FB, D, dtype=bf16))

    rs_m = GradScatter(pc, r.landing, r.landing, r.m_stage, r.m_r1, r.m_r2, r.m_sem, r.free)

    def attn_bwd(h1_s, do_s, acc, gb_a):
        gx_a2a = AllToAll(pc, r.gx_out, h1_s, r.gx_ss, r.gx_rs, False)

        def open_bwd(wo_v):
            wo_cp = pltpu.make_async_copy(r.wo_all, wo_v, r.tmp.at[0])
            wo_cp.start()
            wo_cp.wait()
            clear(r.va, acc, gb_a)

            def body(x_ref, x1_ref, dy_ref, o_ref):
                s = pl.program_id(0)
                rows = pl.ds(pl.multiple_of(s * S, S), S)
                dy, dh2 = dy_ref[0].astype(f32), r.dacc[rows, :]
                xh2, inv2 = ln_stats(x1_ref[0].astype(f32))
                d = dy + ln_grad(dh2, xh2, inv2, gain2[...])
                r.dacc[rows, :] = d
                db = d.astype(bf16)
                r.va[0:1, :] += over_rows(jnp.sum, dy)
                r.va[1:2, :] += over_rows(jnp.sum, dh2 * xh2)
                r.va[2:3, :] += over_rows(jnp.sum, dh2)
                r.va[3:4, :] += over_rows(jnp.sum, d)
                xh, _ = ln_stats(x_ref[0].astype(f32))
                h1_s[s] = (xh * gain1[...] + bias1[...]).astype(bf16)
                do_s[s] = nt(wo_v[...].reshape(TP * PW, D), db).astype(bf16)
                acc[:, R3:, :] += nn(o_ref[0].reshape(TP * PW, S), db).reshape(TP, PW, D)

            seq = pl.BlockSpec((1, S, D), lambda s: (s, 0, 0))
            pltpu.emit_pipeline(body, grid=(NS,), in_specs=[seq, seq, seq, pl.BlockSpec((1, TP, PW, S), lambda s: (s, 0, 0, 0))])(
                r.xs, r.x1, r.dys, r.o)

        pl.run_scoped(open_bwd, vm(TP, PW, D, dtype=bf16))
        n_half = NS // 2
        rs = GradScatter(pc, acc, r.landing.at[pl.ds(0, R3 + PW)], r.a_stage, r.a_r1, r.landing, r.a_sem, r.free)

        def slot_at(g):
            return jnp.where(g < 4, lax.rem(g + 2, 4), g)

        def heads(dq_s, wq_v, buf):
            wq_cp = pltpu.make_async_copy(r.wq_all, wq_v, r.tmp.at[1])
            wq_cp.start()
            for half in range(2):
                def body(qkv_ref, ml_ref):
                    n, sh = pl.program_id(0), pl.program_id(1)
                    g = slot_at(n)
                    s = half * n_half + sh
                    cos, sin = r.cos[...], r.sin[...]
                    ok = key_mask(r.mask[s])

                    def rot_back(t):
                        a, b = t[:HH], t[HH:]
                        return jnp.concatenate([a * cos + b * sin, b * cos - a * sin], axis=0)

                    base = pl.multiple_of(g * R3, PW)
                    for h in range(2):
                        lo = h * HD
                        qkv, ml = qkv_ref.at[0, 0], ml_ref.at[0, 0]
                        q, k, v = (qkv[j * PW + lo:j * PW + lo + HD, :] for j in range(3))
                        do = do_s[s, pl.ds(pl.multiple_of(g * PW + lo, HD), HD), :]
                        sc = masked_scores(q, k, ok)
                        p = jnp.exp(sc - ml[h:h + 1, :]) * ml[2 + h:3 + h, :]
                        dp = tn(v, do)
                        ds = (p * (dp - over_rows(jnp.sum, dp * p))).astype(bf16)
                        dv = nt(p.astype(bf16), do).T
                        dk = rot_back(nt(ds, q).T)
                        dq = rot_back(nn(k, ds)) * QS
                        for j, t in enumerate((dq, dk, dv)):
                            at = pl.ds(base + j * PW + lo, HD)
                            dq_s[sh, at, :] = t.astype(bf16)
                            gb_a[at, :] += over_cols(jnp.sum, t)

                    acc[g, :R3, :] += nn(dq_s[sh, pl.ds(base, R3), :], h1_s[s])
                    if half == 0:
                        @pl.when((sh == 0) & (n == 1))
                        def _():
                            rs_m.second([buf, r.landing.at[pl.ds(FB, FB)]], r.chunk, [r.m_stage.at[2]])
                            rs_m.send_second()
                    else:
                        @pl.when(sh == n_half - 1)
                        def _():
                            rs.block_done(g, g)

                            @pl.when(n > 0)
                            def _():
                                rs.later(slot_at(n - 1), slot_at(n - 1), n < TP - 1)

                pair = lambda rows: pl.BlockSpec((1, 1, rows, S), lambda n, sh: (half * n_half + sh, slot_at(n), 0, 0))
                pltpu.emit_pipeline(body, grid=(TP, n_half), in_specs=[pair(R3), pair(4)])(r.qkv, r.ml)
                if half == 0:
                    wq_cp.wait()

                def close_bwd(x_ref):
                    sh = pl.program_id(0)
                    s = half * n_half + sh
                    rows = pl.ds(pl.multiple_of(s * S, S), S)
                    dh1 = tn(dq_s[sh], wq_v[...].reshape(TP * R3, D))
                    xh, inv = ln_stats(x_ref[0].astype(f32))
                    r.va[4:5, :] += over_rows(jnp.sum, dh1 * xh)
                    r.va[5:6, :] += over_rows(jnp.sum, dh1)
                    h1_s[s] = (r.dacc[rows, :] + ln_grad(dh1, xh, inv, gain1[...])).astype(bf16)
                    gx_a2a.start(s)
                    cp = gx_a2a.local_out(s, h1_s)
                    cp.start()
                    cp.wait()

                pltpu.emit_pipeline(close_bwd, grid=(n_half,),
                                    in_specs=[pl.BlockSpec((1, S, D), lambda sh: (half * n_half + sh, 0, 0))])(r.xs)
            last = jnp.int32(TP - 1)
            rs.later(last, last, False)
            rs.second([buf, r.landing.at[pl.ds(FB, FB)]], r.chunk, [r.gq_b, r.go_b])

        pl.run_scoped(heads, vm(n_half, TP * R3, S, dtype=bf16), vm(TP, R3, D, dtype=bf16), vm(FB, D))

        for g in range(TP):
            r.msg[g] = r.va[...]
            for j in range(3):
                cols = jnp.broadcast_to(gb_a[g * R3 + j * PW:g * R3 + (j + 1) * PW, :], (PW, PW))
                r.msg[g, 6:7, j * PW:(j + 1) * PW] = cols.T[0:1, :]
            r.msg[g, 6:7, R3:R3 + FB] = r.gbu[g]
        pair = remote(r.msg, r.msg_in, r.s_ss.at[0], r.s_rs.at[0], pc.partner)
        pair.start()
        pair.wait()
        r.msg_in[...] = r.msg_in[...] + r.msg[...]
        chip = lax.div(pc.me, 2)
        small = [remote(r.msg_in.at[pc.slot_of(m)], r.msgs.at[chip], r.s_ss.at[1], r.s_rs.at[1], pc.peer(m)) for m in (2, 4, 6)]
        for cp in small:
            cp.start()
        own = pltpu.make_async_copy(r.msg_in.at[pc.slot_of(0)], r.msgs.at[chip], r.s_ss.at[2])
        own.start()

        def tail(bufs, act_v, turned):
            b0, b1, b2 = (bufs.at[i] for i in range(3))
            y_own = [(pltpu.make_async_copy(r.y_seq.at[s, y_a2a._rows(pc.me)], act_v.at[s], r.tmp.at[s]),
                      pltpu.make_async_copy(act_v.at[s], r.y_out.at[pc.me * NS + s], r.tmp.at[NS + s])) for s in range(NS)]
            for load, _ in y_own:
                load.start()
            for load, store in y_own:
                load.wait()
                store.start()
            for g in (g_bs, g_wq, g_wo, g_wu, g_wd):
                g.sent()
            for _, store in y_own:
                store.wait()
            rs_m.finish()
            wait_for(r.m_r1.at[0], r.m_sem.at[4])
            for p in range(2):
                half = pl.ds(p * FB, FB)
                for cp in load_all([(r.m_stage.at[3, half], b0), (r.m_r1.at[0, half], b1), (r.m_r2.at[half], b2)], r.tmp):
                    cp.wait()
                row_add(b0, [b1, b2])
                if p == 0:
                    cp = pltpu.make_async_copy(b0, r.gd, r.tmp.at[0])
                else:
                    for k in range(D // FB):
                        cols = slice(k * FB, (k + 1) * FB)
                        turned[cols, :] = b0[:, cols].T
                    cp = pltpu.make_async_copy(turned, r.gu, r.tmp.at[0])
                cp.start()
                cp.wait()
            rs.own_part(b0, b1, r.tmp)
            y_a2a.finish_all()
            gx_a2a.finish_all()
            rs.sent_first()
            own.wait()
            for sem in (r.s_ss.at[1], r.s_rs.at[1]):
                wait_for(r.msgs.at[pl.ds(0, len(small))], sem)

        pl.run_scoped(tail, vm(3, FB, D), vm(NS, SL, D, dtype=bf16), vm(D, FB))

    seqs = vm(NS, S, D, dtype=bf16)
    pl.run_scoped(attn_bwd, seqs, vm(NS, D, S, dtype=bf16), vm(TP, R3 + PW, D), vm(TP * R3, 1))


def layer_call(*args):
    out = pl.pallas_call(
        layer_kernel,
        in_specs=[ANY] * len(IN_NAMES),
        out_specs=[ANY] * len(OUT_SHAPES),
        out_shape=[sds(*v) for v in OUT_SHAPES.values()],
        scratch_shapes=list(SCRATCH.values()),
        compiler_params=pltpu.CompilerParams(collective_id=0, has_side_effects=True, vmem_limit_bytes=VMEM_LIMIT),
        name="layer",
    )(*args)
    return out[:8]


FINAL = {"y": ((TP * NS, SL, D), bf16), "gx": ((TP * NS, SL, D), bf16), "gd": ((FB, D), f32), "gu": ((D, FB), f32),
         "gbq": ((3, 2, HD), f32), "gbu": ((1, FB), f32)}
VECS = ("bd", "g2", "b2", "bo", "g1", "b1")
FINAL |= {k: ((1, D), f32) for k in VECS}
LATE = ("gbq", "gbu") + VECS


def final_kernel(y_in, gx_in, msgs, gd_in, gu_in, *refs):
    outs, refs = Refs(FINAL, refs), refs[len(FINAL):]
    msg_v, y_v, gx_v, gd_v, gu_v, ld, st = refs[:7]
    late = Refs(LATE, refs[7:])
    moves = [([(msgs, msg_v)], [])]
    for src, buf, dst in ((gd_in, gd_v, outs.gd), (gu_in, gu_v, outs.gu), (y_in, y_v, outs.y), (gx_in, gx_v, outs.gx)):
        moves.append(([(src, buf)], [(buf, dst)]))
    copy = pltpu.make_async_copy
    loads = [[copy(s, d, ld.at[i]) for s, d in m[0]] for i, m in enumerate(moves)]
    stores = [[copy(s, d, st.at[i]) for s, d in m[1]] for i, m in enumerate(moves)]
    for cps in loads:
        for cp in cps:
            cp.start()
    for i, (cps, outward) in enumerate(zip(loads, stores)):
        for cp in cps:
            cp.wait()
        if i == 0:
            small = msg_v[0]
            for j in range(1, msg_v.shape[0]):
                small = small + msg_v[j]
            for j, k in enumerate(VECS):
                getattr(late, k)[...] = small[j:j + 1, :]
            for j in range(3):
                for h in range(2):
                    lo = j * PW + h * HD
                    late.gbq[j, h:h + 1, :] = small[6:7, lo:lo + HD]
            late.gbu[...] = small[6:7, R3:R3 + FB]
        for cp in outward:
            cp.start()
    small_out = load_all([(getattr(late, k), getattr(outs, k)) for k in LATE], st.at[pl.ds(len(moves), len(LATE))])
    for cps in stores + [small_out]:
        for cp in cps:
            cp.wait()


def final_call(y, gx, msgs, gd, gu):
    act = vm(*y.shape, dtype=bf16)
    return pl.pallas_call(
        final_kernel,
        in_specs=[ANY] * 5,
        out_specs=[ANY] * len(FINAL),
        out_shape=[sds(*v) for v in FINAL.values()],
        scratch_shapes=[vm(*msgs.shape), act, act, vm(FB, D), vm(D, FB), DMA((5,)), DMA((5 + len(LATE),))]
        + [vm(*FINAL[k][0]) for k in LATE],
        compiler_params=pltpu.CompilerParams(vmem_limit_bytes=VMEM_LIMIT),
        cost_estimate=pl.CostEstimate(flops=10 ** 10, bytes_accessed=3 * 10 ** 7, transcendentals=0),
        name="results",
    )(y, gx, msgs, gd, gu)


def rope_tables():
    inv_freq = (ROPE_BASE ** (-2.0 * np.arange(HH, dtype=np.float32) / HD)).astype(np.float32)
    angles = np.outer(inv_freq, np.arange(S, dtype=np.float32))
    return np.cos(angles), np.sin(angles)


def solution(mesh):
    no = None
    act_spec = P('dp', 'tp', no)
    rep, part = P(no), P('dp')
    in_specs = (act_spec, act_spec, P('dp', no), rep, rep, P(no, no, 'tp', no), P(no, 'tp', no),
                P('tp', no, no), rep, rep, rep, P(no, 'tp'), P('tp'), P('tp', no), rep)
    out_specs = (act_spec, act_spec, part, part, P('dp', no, 'tp', no), P('dp', 'tp', no), P(('dp', 'tp'), no, no),
                 part, part, part, P('dp', 'tp'), P(('dp', 'tp')), P(('dp', 'tp'), no), part)

    def device_step(x_in, grad_y, pad_mask, ln1_gain, ln1_bias, w_qkv, b_qkv, w_out, b_out, ln2_gain, ln2_bias, w_up, b_up, w_down, b_down):
        assert x_in.shape == (TP * NS, SL, D) and w_qkv.shape == (3, D, 2, HD) and w_up.shape == (D, FB)
        row = lambda v: v.reshape(1, -1)
        wq = w_qkv.transpose(0, 2, 3, 1).reshape(R3, D)
        cos, sin = rope_tables()
        parts = layer_call(
            x_in, grad_y, wq, w_out.reshape(PW, D), w_up, w_down, b_qkv, row(b_up), pad_mask, cos, sin,
            row(ln1_gain), row(ln1_bias), row(ln2_gain), row(ln2_bias), row(b_out), row(b_down))
        *parts, stage, gq_b, go_b = parts
        to_b = [(i, i ^ (4 - 2 * (i % 2))) for i in range(TP)]
        gq = stage[-1, :R3] + lax.ppermute(gq_b, 'tp', to_b)
        go = lax.ppermute(go_b, 'tp', to_b)
        gq, stage = lax.optimization_barrier((gq, stage))
        go = stage[-1, R3:] + go
        y, gx, gd, gu, gbq, gbu, *vecs = final_call(*parts)
        bd, g2, b2, bo, g1, b1 = (v.reshape(D) for v in vecs)
        return (y, gx, g1, b1, gq.reshape(3, 2, HD, D).transpose(0, 3, 1, 2), gbq, go.reshape(2, HD, D), bo, g2, b2,
                gu, gbu.reshape(FB), gd, bd)

    return jax.shard_map(device_step, mesh=mesh, in_specs=in_specs, out_specs=out_specs, check_vma=False)
```

```python
import functools

import jax
import jax.numpy as jnp
import numpy as np
from jax import lax
from jax.experimental import pallas as pl
from jax.experimental.pallas import tpu as pltpu
from jax.sharding import PartitionSpec as P

f32 = jnp.float32
bf16 = jnp.bfloat16
LN_EPS = 1e-5
ROPE_BASE = 10000.0
INV_SQRT2 = 0.7071067811865476
INV_SQRT_2PI = 0.3989422804014327
NEG_LARGE = -1e30
MESH = pl.DeviceIdType.MESH
ANY = pl.BlockSpec(memory_space=pl.ANY)
VMEM_LIMIT = 66_000_000

TP = 8
NS = 4
S = 512
D = 1024
PW = 128
HD = 64
HH = HD // 2
FB = 512
SL = 64
QS = HD ** -0.5
R3 = 3 * PW
ROWS = 8


def dg(a, b, ca, cb):
    return lax.dot_general(a, b, (((ca,), (cb,)), ((), ())), preferred_element_type=f32)


def nn(a, b):
    return dg(a, b, 1, 0)


def nt(a, b):
    return dg(a, b, 1, 1)


def tn(a, b):
    return dg(a, b, 0, 0)


def over_rows(reduce, v):
    return reduce(v, axis=0, keepdims=True)


def over_cols(reduce, v):
    return reduce(v, axis=1, keepdims=True)


def sds(shape, dtype):
    return jax.ShapeDtypeStruct(shape, dtype)


class Place:
    def __init__(self):
        me = lax.axis_index("tp")
        self.me = me
        self.c = lax.rem(me, 2)
        self.dc = 1 - 2 * self.c
        self.dx = 2 - 4 * lax.rem(lax.div(me, 2), 2)
        self.dy = 4 - 8 * lax.div(me, 4)
        self.partner = me + self.dc
        self.a = me + (1 - self.c) * self.dx + self.c * self.dy
        self.b = me + (1 - self.c) * self.dy + self.c * self.dx

    def peer(self, m):
        return self.me + (m & 1) * self.dc + ((m >> 1) & 1) * self.dx + (m >> 2) * self.dy

    def slot_of(self, m):
        k = self.c if m % 2 == 0 else 1 - self.c
        lo, hi = {0: (6, 7), 1: (0, 5), 2: (4, 1), 3: (2, 3)}[m >> 1]
        return lo + k * (hi - lo)


def remote(src, dst, send_sem, recv_sem, device):
    return pltpu.make_async_remote_copy(src_ref=src, dst_ref=dst, send_sem=send_sem, recv_sem=recv_sem,
                                        device_id={"tp": device}, device_id_type=MESH)


def wait_for(ref, sem):
    pltpu.make_async_copy(ref, ref, sem).wait()


def entry_barrier(pc):
    bar = pltpu.get_barrier_semaphore()
    for m in range(1, TP):
        pl.semaphore_signal(bar, inc=1, device_id={"tp": pc.peer(m)}, device_id_type=MESH)
    pl.semaphore_wait(bar, TP - 1)


class AllToAll:
    def __init__(self, pc, pos_ref, seq_ref, send_sem, recv_sem, inward):
        self.pc, self.pos, self.seq, self.ss, self.rs, self.inward = pc, pos_ref, seq_ref, send_sem, recv_sem, inward

    def _rows(self, dev):
        return pl.ds(pl.multiple_of(dev * SL, SL), SL)

    def _copy(self, s, m):
        pc, dev = self.pc, self.pc.peer(m)
        if self.inward:
            src, dst = self.pos.at[dev * NS + s], self.seq.at[s, self._rows(pc.me)]
        else:
            src, dst = self.seq.at[s, self._rows(dev)], self.pos.at[pc.me * NS + s]
        one = s if self.inward else 0
        return remote(src, dst, self.ss.at[one], self.rs.at[one], dev)

    def start(self, s):
        for m in (*range(2, TP), 1):
            self._copy(s, m).start()

    def start_all(self):
        for m in (*range(2, TP), 1):
            pc, dev = self.pc, self.pc.peer(m)
            if self.inward:
                src, dst = self.pos.at[pl.ds(dev * NS, NS)], self.seq.at[:, self._rows(pc.me)]
            else:
                src, dst = self.seq.at[:, self._rows(dev)], self.pos.at[pl.ds(pc.me * NS, NS)]
            remote(src, dst, self.ss.at[0], self.rs.at[0], dev).start()

    def finish_all(self):
        rest = self.seq.at[:, pl.ds(0, S - SL)]
        wait_for(rest, self.ss.at[0])
        wait_for(rest, self.rs.at[0])

    def finish(self, s):
        all_rows = self.seq.at[s, pl.ds(0, S - SL)]
        wait_for(all_rows, self.ss.at[s])
        wait_for(all_rows, self.rs.at[s])

    def local_in(self, buf):
        pc = self.pc
        return (pltpu.make_async_copy(self.pos.at[pl.ds(pc.me * NS, NS)], buf, self.ss.at[self.ss.shape[0] - 1]),
                pltpu.make_async_copy(buf, self.seq.at[:, self._rows(pc.me)], self.rs.at[self.rs.shape[0] - 1]))

    def local_out(self, s, src):
        return pltpu.make_async_copy(src.at[s, self._rows(self.pc.me)], self.pos.at[self.pc.me * NS + s], self.ss.at[self.ss.shape[0] - 1])


class Gather:
    def __init__(self, pc, src_ref, dst_ref, send_sem, recv_sem):
        self.pc, self.src, self.dst, self.ss, self.rs = pc, src_ref, dst_ref, send_sem, recv_sem

    def _send(self, src, slot, dev):
        return remote(src, self.dst.at[slot], self.ss, self.rs.at[slot], dev)

    def _direct(self):
        pc, c = self.pc, self.pc.c
        return [self._send(self.src, c, pc.a), self._send(self.src, 6 + c, pc.partner),
                self._send(self.src, 4 + c, pc.b)]

    def _hop(self):
        pc, c = self.pc, self.pc.c
        return [self._send(self.dst.at[c], 2 + c, pc.b), self._send(self.dst.at[c], c, pc.partner),
                self._send(self.dst.at[4 + c], 4 + c, pc.partner)]

    def _last(self):
        pc, c = self.pc, self.pc.c
        return self._send(self.dst.at[2 + c], 2 + c, pc.partner)

    def arrived(self, slot):
        wait_for(self.dst.at[slot], self.rs.at[slot])

    def start(self):
        self.start_a()
        self.start_b()

    def start_a(self):
        for cp in self._direct()[:2]:
            cp.start()

    def start_b(self):
        self._direct()[2].start()

    def forward(self):
        self.forward_a()
        self.forward_b()

    def forward_a(self):
        hop = self._hop()
        self.arrived(self.pc.c)
        hop[0].start()
        hop[1].start()

    def forward_b(self):
        self.arrived(4 + self.pc.c)
        self._hop()[2].start()

    def last(self):
        self.arrived(2 + self.pc.c)
        self._last().start()

    def local(self, buf):
        return (pltpu.make_async_copy(self.src, buf, self.rs.at[TP]),
                pltpu.make_async_copy(buf, self.dst.at[6 + self.pc.c], self.rs.at[6 + self.pc.c]))

    def arrived_near(self):
        for j in (0, 2, 3):
            self.arrived(2 * j + 1 - self.pc.c)
        self.arrived(6 + self.pc.c)

    def arrived_far(self):
        self.arrived(3 - self.pc.c)

    def sent(self):
        wait_for(self.dst.at[pl.ds(0, TP - 1)], self.ss)


def row_add(acc, others):
    step = 64

    def body(i, carry):
        r = pl.ds(pl.multiple_of(i * step, step), step)
        v = acc[r, :]
        for o in others:
            v = v + o[r, :]
        acc[r, :] = v
        return carry

    lax.fori_loop(0, acc.shape[0] // step, body, 0)


class GradScatter:
    def __init__(self, pc, acc, landing, stage, r1, r2, sems, free):
        self.pc, self.acc, self.landing, self.stage, self.r1, self.r2 = pc, acc, landing, stage, r1, r2
        self.sem, self.free = sems, free

    def _pair(self, b):
        return remote(self.acc.at[b], self.landing, self.sem.at[0], self.sem.at[1], self.pc.partner)

    def _first(self, j):
        return remote(self.stage.at[j], self.r1.at[j], self.sem.at[2 + j], self.sem.at[4 + j], self.pc.a)

    def _second(self):
        return remote(self.stage.at[2], self.r2, self.sem.at[6], self.sem.at[7], self.pc.b)

    def send_pair(self, b, needs_credit):
        @pl.when(needs_credit)
        def _():
            pl.semaphore_wait(self.free, 1)

        self._pair(b).start()

    def sent_pair(self, b):
        self._pair(b).wait_send()

    def settle(self, j, b, landed, gives_credit):
        landed()
        row_add(self.acc.at[b], [self.landing])

        @pl.when(gives_credit)
        def _():
            pl.semaphore_signal(self.free, inc=1, device_id={"tp": self.pc.partner}, device_id_type=MESH)

        store = pltpu.make_async_copy(self.acc.at[b], self.stage.at[j], self.sem.at[8])
        store.start()
        store.wait()

        @pl.when(j < 2)
        def _():
            self._first(j).start()

    def landed(self):
        wait_for(self.landing, self.sem.at[1])

    def block_done(self, slot, b):
        pl.when(lax.rem(slot, 2) != self.pc.c)(lambda: self.send_pair(b, True))

    def later(self, slot, b, gives_credit):
        own = lax.rem(slot, 2) == self.pc.c
        pl.when(own)(lambda: self.settle(lax.div(slot, 2), b, self.landed, gives_credit))
        pl.when(jnp.logical_not(own))(lambda: self.sent_pair(b))

    def second(self, bufs, chunk_sem, dsts):
        n = chunk_sem.shape[0] // 3
        size = bufs[0].shape[0]
        rows = size // n
        part = lambda ref, k: ref.at[pl.ds(k * rows, rows)]
        wait_for(self.r1.at[1], self.sem.at[5])
        dsts = [part(d, k) for d in dsts for k in range(d.shape[0] // rows)]
        for p in range(self.stage.shape[1] // size):
            mine, theirs = (ref.at[pl.ds(p * size, size)] for ref in (self.stage.at[2], self.r1.at[1]))
            loads = [[pltpu.make_async_copy(part(src, k), part(buf, k), chunk_sem.at[x * n + k])
                      for x, (src, buf) in enumerate(zip((mine, theirs), bufs))] for k in range(n)]
            stores = [pltpu.make_async_copy(part(bufs[0], k), dsts[p * n + k], chunk_sem.at[2 * n + k]) for k in range(n)]
            for group in loads:
                for cp in group:
                    cp.start()
            for k in range(n):
                for cp in loads[k]:
                    cp.wait()
                row_add(part(bufs[0], k), [part(bufs[1], k)])
                stores[k].start()
            for cp in stores:
                cp.wait()

    def send_second(self):
        self._second().start()

    def own_part(self, b0, b1, sem, dsts):
        wait_for(self.r1.at[0], self.sem.at[4])
        for cp in load_all([(self.stage.at[3], b0), (self.r1.at[0], b1)], sem):
            cp.wait()
        row_add(b0, [b1])
        n = dsts[0].shape[0]
        for cp in load_all(list(zip((b0.at[pl.ds(0, n)], b0.at[pl.ds(n, PW)]), dsts)), sem):
            cp.wait()

    def sent_first(self):
        for j in range(2):
            self._first(j).wait_send()

    def finish(self):
        self.sent_first()
        self._second().wait()


def ln_stats(v):
    c = v - over_cols(jnp.mean, v)
    inv = lax.rsqrt(over_cols(jnp.mean, c * c) + LN_EPS)
    return c * inv, inv


def ln_grad(d_out, x_hat, inv, gain):
    dh = d_out * gain
    return inv * (dh - over_cols(jnp.mean, dh) - x_hat * over_cols(jnp.mean, dh * x_hat))


def masked_scores(q, k, ok):
    return jnp.where(ok, tn(k, q), NEG_LARGE)


def key_mask(mask):
    return jnp.concatenate([mask] * (S // PW), axis=1) > 0


def column(row):
    return jnp.broadcast_to(row, (PW, row.shape[1])).T[:, :1]


def clear(*refs):
    for ref in refs:
        ref[...] = jnp.zeros(ref.shape, ref.dtype)


def load_all(pairs, sem):
    cps = [pltpu.make_async_copy(s, d, sem.at[i]) for i, (s, d) in enumerate(pairs)]
    for cp in cps:
        cp.start()
    return cps


def vm(*shape, dtype=f32):
    return pltpu.VMEM(shape, dtype)


TT = 1024
NT = NS * S // TT
SMALL = {
    "bqkv": vm(3, 2, HD), "bup": vm(1, FB), "pad": vm(TP * NS, S, dtype=jnp.int32), "cos": vm(HH, S), "sin": vm(HH, S),
    "gain1": vm(1, D), "bias1": vm(1, D), "gain2": vm(1, D), "bias2": vm(1, D), "b_out": vm(1, D), "b_down": vm(1, D),
}
IN_NAMES = ("x_in", "dy_in", "wq", "wo", "wu", "wd") + tuple("in_" + k for k in SMALL)
OUT_SHAPES = {
    "y_out": ((TP * NS, SL, D), bf16), "gx_out": ((TP * NS, SL, D), bf16), "msgs": ((TP // 2, ROWS, D), f32), "gd": ((FB, D), f32), "gu": ((D, FB), f32),
    "gq_own": ((R3, D), f32), "go_own": ((PW, D), f32), "gq_b": ((R3, D), f32), "go_b": ((PW, D), f32), "a_stage": ((4, R3 + PW, D), f32), "a_r1": ((2, R3 + PW, D), f32),
    "m_r0": ((2 * FB, D), f32), "m_stage": ((4, 2 * FB, D), f32), "m_r1": ((2, 2 * FB, D), f32), "m_r2": ((2 * FB, D), f32),
    "xs": ((NS, S, D), bf16), "dys": ((NS, S, D), bf16), "wq_all": ((TP, R3, D), bf16), "wo_all": ((TP, PW, D), bf16),
    "wu_all": ((TP, D, FB), bf16), "wd_all": ((TP, FB, D), bf16),
    "qkv": ((NS, TP, R3, S), bf16), "ml": ((NS, TP, 4, S), f32), "o": ((NS, TP, PW, S), bf16),
    "x1": ((NS, S, D), bf16), "y_seq": ((NS, S, D), bf16),
}
DMA = pltpu.SemaphoreType.DMA
SCRATCH = SMALL | {
    "bs_all": vm(TP, ROWS, PW), "bs": vm(ROWS, PW), "mask": vm(NS, S, PW), "dacc": vm(NS * S, D), "landing": vm(2 * FB, D), "gbu": vm(TP, 1, FB), "va": vm(ROWS, D),
    "msg": vm(TP, ROWS, D), "msg_in": vm(TP, ROWS, D),
    "free": pltpu.SemaphoreType.REGULAR,
    "x_ss": DMA((NS + 1,)), "x_rs": DMA((NS + 1,)), "dy_ss": DMA((2,)), "dy_rs": DMA((2,)),
    "y_ss": DMA((1,)), "y_rs": DMA((1,)), "gx_ss": DMA((2,)), "gx_rs": DMA((1,)),
    "g_ss": DMA((5,)), "g_rs": DMA((5, TP + 1)), "m_sem": DMA((11,)), "a_sem": DMA((9,)), "s_ss": DMA((3,)), "s_rs": DMA((2,)),
    "tmp": DMA((TP,)), "chunk": DMA((12,)), "w_sem": DMA((2, 2)),
}


class Refs:
    def __init__(self, names, refs):
        for n, r in zip(names, refs):
            setattr(self, n, r)


def layer_kernel(*refs):
    r = Refs(IN_NAMES + tuple(OUT_SHAPES) + tuple(SCRATCH), refs)
    pc = Place()
    small_in = load_all([(getattr(r, "in_" + k), getattr(r, k)) for k in SMALL], r.chunk)
    entry_barrier(pc)
    x_a2a = AllToAll(pc, r.x_in, r.xs, r.x_ss, r.x_rs, True)
    dy_a2a = AllToAll(pc, r.dy_in, r.dys, r.dy_ss, r.dy_rs, True)
    y_a2a = AllToAll(pc, r.y_out, r.y_seq, r.y_ss, r.y_rs, False)
    g_bs, g_wq, g_wo, g_wu, g_wd = [
        Gather(pc, s, d, r.g_ss.at[i], r.g_rs.at[i])
        for i, (s, d) in enumerate(((r.bs, r.bs_all), (r.wq, r.wq_all), (r.wo, r.wo_all), (r.wu, r.wu_all), (r.wd, r.wd_all)))]
    gain1, bias1, gain2, bias2, b_out, b_down = r.gain1, r.bias1, r.gain2, r.bias2, r.b_out, r.b_down

    def arrivals(b_x, b_dy, b_q, b_o, b_u, b_d):
        first = (g_bs, g_wq, g_wo)
        for g in first[1:]:
            g.start()
        x_a2a.start(0)
        for cp in small_in:
            cp.wait()
        for i in range(3):
            for h in range(2):
                r.bs[pl.ds(i, 1), pl.ds(h * HD, HD)] = r.bqkv[i, pl.ds(h, 1), :]
        for k in range(FB // PW):
            r.bs[pl.ds(4 + k, 1), :] = r.bup[:, pl.ds(k * PW, PW)]
        local = [x_a2a.local_in(b_x), dy_a2a.local_in(b_dy)]
        local += [g.local(b) for g, b in ((g_wq, b_q), (g_wo, b_o), (g_wu, b_u), (g_wd, b_d))]
        for load, _ in local:
            load.start()
        for s in range(NS):
            keys = jnp.broadcast_to(r.pad[pl.ds(pc.me * NS + s, 1), :].astype(f32), (PW, S))
            r.mask[s] = keys.T
        g_bs.start()
        pltpu.make_async_copy(r.bs, r.bs_all.at[6 + pc.c], r.g_rs.at[0, 6 + pc.c]).start()
        for load, store in local:
            load.wait()
            store.start()
        for g in (g_wq, g_wo, g_bs):
            g.forward_a()
        for g in (g_wq, g_wo, g_bs):
            g.forward_b()
        x_a2a.finish(0)
        x_a2a.start(1)
        for g in first:
            g.arrived_near()
        for g in (g_wu, g_wd):
            g.arrived(6 + pc.c)
        local[0][1].wait()
        local[1][1].wait()

    def later_arrivals():
        for g in (g_bs, g_wq, g_wo):
            g.last()
        for s in range(2, NS):
            x_a2a.start(s)
        dy_a2a.start_all()
        g_wu.start_a()
        g_wd.start_a()
        for g in (g_bs, g_wq, g_wo):
            g.arrived_far()

    act = vm(NS, SL, D, dtype=bf16)
    pl.run_scoped(arrivals, act, act, vm(R3, D, dtype=bf16), vm(PW, D, dtype=bf16), vm(D, FB, dtype=bf16), vm(FB, D, dtype=bf16))

    def attn_fwd(h2_v, wq_v, wo_v, h1_s, o_s):
        def fetch(*pairs):
            for cp in load_all(pairs, r.tmp):
                cp.wait()

        fetch(*[(r.wq_all.at[pl.ds(k, 2)], wq_v.at[pl.ds(k, 2)]) for k in (6, 0, 4)])

        def slot_at(n):
            return jnp.where(n < 2, n + 6, jnp.where(n < 4, n - 2, jnp.where(n < 6, n, n - 4)))

        def body(x_ref, qkv_ref, ml_ref, o_ref, x1_ref):
            s, n = pl.program_id(0), pl.program_id(1)
            g = slot_at(n)

            @pl.when(n == 0)
            def _():
                xh, _ = ln_stats(x_ref[0].astype(f32))
                h1_s[...] = (xh * gain1[...] + bias1[...]).astype(bf16)

            bias = r.bs_all[g]
            bias = jnp.concatenate([column(bias[i:i + 1]) for i in range(3)], axis=0)
            qkv = nt(wq_v[g], h1_s[...]) + bias
            cos, sin = r.cos[...], r.sin[...]
            ok = key_mask(r.mask[s])

            def rot(t):
                a, b = t[:HH], t[HH:]
                return jnp.concatenate([a * cos - b * sin, b * cos + a * sin], axis=0).astype(bf16)

            for h in range(2):
                lo = h * HD
                at_q, at_k, at_v = (slice(j * PW + lo, j * PW + lo + HD) for j in range(3))
                q, k, v = rot(qkv[at_q] * QS), rot(qkv[at_k]), qkv[at_v].astype(bf16)
                for at, t in ((at_q, q), (at_k, k), (at_v, v)):
                    qkv_ref[0, 0, at, :] = t
                sc = masked_scores(q, k, ok)
                m = over_rows(jnp.max, sc)
                e = jnp.exp(sc - m)
                li = 1.0 / over_rows(jnp.sum, e)
                p = (e * li).astype(bf16)
                ml = ml_ref.at[0, 0]
                ml[h:h + 1, :] = m
                ml[2 + h:3 + h, :] = li
                o = nn(v, p).astype(bf16)
                o_ref[0, 0, lo:lo + HD, :] = o
                o_s[pl.ds(pl.multiple_of(g * PW + lo, HD), HD), :] = o

            @pl.when((s == 0) & (n == 5))
            def _():
                later_arrivals()
                fetch((r.wq_all.at[pl.ds(2, 2)], wq_v.at[pl.ds(2, 2)]), (r.wo_all, wo_v))

            @pl.when(n == TP - 1)
            def _():
                attn = tn(o_s[...], wo_v[...].reshape(TP * PW, D))
                x1 = (x_ref[0].astype(f32) + (attn + b_out[...])).astype(bf16)
                x1_ref[0] = x1
                xh, _ = ln_stats(x1.astype(f32))
                h2_v[pl.ds(pl.multiple_of(s * S, S), S), :] = (xh * gain2[...] + bias2[...]).astype(bf16)

            for k in range(1, NS):
                @pl.when((s == k - 1) & (n == TP - 2))
                def _():
                    x_a2a.finish(k)

        seq = pl.BlockSpec((1, S, D), lambda s, n: (s, 0, 0))
        pair = lambda rows: pl.BlockSpec((1, 1, rows, S), lambda s, n: (s, slot_at(n), 0, 0))
        pltpu.emit_pipeline(body, grid=(NS, TP), in_specs=[seq], out_specs=[pair(R3), pair(4), pair(PW), seq])(
            r.xs, r.qkv, r.ml, r.o, r.x1)

    def mlp(h2_v, dy_v, wu_v, wd_v, yacc, acc):
        rs = GradScatter(pc, acc, r.landing, r.m_stage, r.m_r1, r.m_r2, r.m_sem, r.free)

        def is_own(i):
            return (i == 2) | (i == 4) | (i == 5) | (i == 7)

        def role_at(i):
            return jnp.where((i == 0) | (i == 5), 3, jnp.where(i < 3, 0, jnp.where(i < 5, 1, 2)))

        def slot_at(i):
            return 2 * role_at(i) + jnp.where(is_own(i), pc.c, 1 - pc.c)

        early = lambda b: remote(acc.at[b], r.m_r0, r.m_sem.at[9], r.m_sem.at[10], pc.partner)

        def landed(i):
            @pl.when(i == 5)
            def _():
                wait_for(r.m_r0, r.m_sem.at[10])
                cp = pltpu.make_async_copy(r.m_r0, r.landing, r.tmp.at[0])
                cp.start()
                cp.wait()

            pl.when(i != 5)(rs.landed)

        def weights(slot, b):
            return (pltpu.make_async_copy(r.wu_all.at[slot], wu_v.at[b], r.w_sem.at[0, b]),
                    pltpu.make_async_copy(r.wd_all.at[slot], wd_v.at[b], r.w_sem.at[1, b]))

        def fetch(i):
            slot = slot_at(i)

            @pl.when(jnp.logical_not(is_own(i)))
            def _():
                g_wu.arrived(slot)
                g_wd.arrived(slot)

            for cp in weights(slot, lax.rem(i, 2)):
                cp.start()

        fetch(jnp.int32(0))
        cps = []
        dy_a2a.finish_all()
        for s in range(NS):
            cps.append(pltpu.make_async_copy(r.dys.at[s], dy_v.at[pl.ds(s * S, S)], r.tmp.at[s]))
            cps[s].start()
        clear(yacc, r.dacc, r.gbu)
        for cp in cps:
            cp.wait()

        def step(n, carry):
            i, t = lax.div(n, NT), lax.rem(n, NT)
            b = lax.rem(i, 2)
            slot = slot_at(i)

            @pl.when(t == 0)
            def _():
                for cp in weights(slot, b):
                    cp.wait()
                clear(acc.at[b])

            @pl.when((t == NT - 1) & (i != 0) & (i != 2) & (i < TP - 1))
            def _():
                fetch(i + 1)

            rows = pl.ds(pl.multiple_of(t * TT, TT), TT)
            h2, dy = h2_v[rows, :], dy_v[rows, :]
            wu, wd = wu_v[b], wd_v[b]
            bias = r.bs_all[slot]
            bias = jnp.concatenate([bias[k:k + 1] for k in range(4, TP)], axis=1)
            pre = nn(h2, wu) + bias
            d_act = nt(dy, wd)
            cdf = 0.5 * (1.0 + lax.erf(pre * INV_SQRT2))
            act = (pre * cdf).astype(bf16)
            d_pre = d_act * (cdf + pre * jnp.exp(-0.5 * pre * pre) * INV_SQRT_2PI)
            d_pre_b = d_pre.astype(bf16)
            yacc[rows, :] += nn(act, wd)
            r.dacc[rows, :] += nt(d_pre_b, wu)
            acc[b, :FB, :] += tn(act, dy)
            acc[b, FB:, :] += tn(d_pre_b, h2)
            r.gbu[slot] += over_rows(jnp.sum, d_pre)

            done = (t == NT - 1)
            pl.when(done & (i == 0))(lambda: early(b).start())
            pl.when(done & (i > 0) & jnp.logical_not(is_own(i)))(lambda: rs.send_pair(b, i > 1))
            pl.when(done & is_own(i))(lambda: rs.settle(role_at(i), b, lambda: landed(i), i != 4))
            pl.when((t == 0) & (i == 1))(lambda: early(1 - b).wait_send())
            pl.when((t == 0) & (i > 1) & jnp.logical_not(is_own(i - 1)))(lambda: rs.sent_pair(1 - b))

            for when, hops in ((1, ("forward_a", "start_b")), (4, ("last",)), (5, ()), (9, ("forward_b",))):
                @pl.when(n == when)
                def _():
                    for hop in hops:
                        for gather in (g_wu, g_wd):
                            getattr(gather, hop)()
                    if when in (1, 5):
                        fetch(i + 1)

            return carry

        lax.fori_loop(0, TP * NT, step, 0)
        cps = load_all([(r.x1.at[s], h2_v.at[pl.ds(s * S, S)]) for s in range(NS)], r.tmp)
        stores = []
        for s in range(NS):
            rows = pl.ds(s * S, S)
            cps[s].wait()
            dy_v[rows, :] = (h2_v[rows, :].astype(f32) + (yacc[rows, :] + b_down[...])).astype(bf16)
            cp = pltpu.make_async_copy(dy_v.at[rows], r.y_seq.at[s], r.tmp.at[NS + s])
            cp.start()
            stores.append(cp)
        for cp in stores:
            cp.wait()
        y_a2a.start_all()

    tok = vm(NS * S, D, dtype=bf16)

    def forward_and_mlp(h2_v, dy_v, wu_v, wd_v):
        pl.run_scoped(functools.partial(attn_fwd, h2_v), vm(TP, R3, D, dtype=bf16), vm(TP, PW, D, dtype=bf16),
                      vm(S, D, dtype=bf16), vm(D, S, dtype=bf16))
        pl.run_scoped(functools.partial(mlp, h2_v, dy_v, wu_v, wd_v), vm(NS * S, D), vm(2, 2 * FB, D))

    pl.run_scoped(forward_and_mlp, tok, tok, vm(2, D, FB, dtype=bf16), vm(2, FB, D, dtype=bf16))

    rs_m = GradScatter(pc, r.landing, r.landing, r.m_stage, r.m_r1, r.m_r2, r.m_sem, r.free)

    def attn_bwd(h1_s, do_s, acc, gb_a):
        gx_a2a = AllToAll(pc, r.gx_out, h1_s, r.gx_ss, r.gx_rs, False)

        def open_bwd(wo_v):
            wo_cp = pltpu.make_async_copy(r.wo_all, wo_v, r.tmp.at[0])
            wo_cp.start()
            wo_cp.wait()
            clear(r.va, acc, gb_a)

            def body(x_ref, x1_ref, dy_ref, o_ref):
                s = pl.program_id(0)
                rows = pl.ds(pl.multiple_of(s * S, S), S)
                dy, dh2 = dy_ref[0].astype(f32), r.dacc[rows, :]
                xh2, inv2 = ln_stats(x1_ref[0].astype(f32))
                d = dy + ln_grad(dh2, xh2, inv2, gain2[...])
                r.dacc[rows, :] = d
                db = d.astype(bf16)
                r.va[0:1, :] += over_rows(jnp.sum, dy)
                r.va[1:2, :] += over_rows(jnp.sum, dh2 * xh2)
                r.va[2:3, :] += over_rows(jnp.sum, dh2)
                r.va[3:4, :] += over_rows(jnp.sum, d)
                xh, _ = ln_stats(x_ref[0].astype(f32))
                h1_s[s] = (xh * gain1[...] + bias1[...]).astype(bf16)
                do_s[s] = nt(wo_v[...].reshape(TP * PW, D), db).astype(bf16)
                acc[:, R3:, :] += nn(o_ref[0].reshape(TP * PW, S), db).reshape(TP, PW, D)

            seq = pl.BlockSpec((1, S, D), lambda s: (s, 0, 0))
            pltpu.emit_pipeline(body, grid=(NS,), in_specs=[seq, seq, seq, pl.BlockSpec((1, TP, PW, S), lambda s: (s, 0, 0, 0))])(
                r.xs, r.x1, r.dys, r.o)

        pl.run_scoped(open_bwd, vm(TP, PW, D, dtype=bf16))
        n_half = NS // 2
        rs = GradScatter(pc, acc, r.landing.at[pl.ds(0, R3 + PW)], r.a_stage, r.a_r1, r.landing, r.a_sem, r.free)

        def slot_at(g):
            return jnp.where(g < 4, lax.rem(g + 2, 4), g)

        def heads(dq_s, wq_v, buf):
            wq_cp = pltpu.make_async_copy(r.wq_all, wq_v, r.tmp.at[1])
            wq_cp.start()
            for half in range(2):
                def body(qkv_ref, ml_ref):
                    n, sh = pl.program_id(0), pl.program_id(1)
                    g = slot_at(n)
                    s = half * n_half + sh
                    cos, sin = r.cos[...], r.sin[...]
                    ok = key_mask(r.mask[s])

                    def rot_back(t):
                        a, b = t[:HH], t[HH:]
                        return jnp.concatenate([a * cos + b * sin, b * cos - a * sin], axis=0)

                    base = pl.multiple_of(g * R3, PW)
                    for h in range(2):
                        lo = h * HD
                        qkv, ml = qkv_ref.at[0, 0], ml_ref.at[0, 0]
                        q, k, v = (qkv[j * PW + lo:j * PW + lo + HD, :] for j in range(3))
                        do = do_s[s, pl.ds(pl.multiple_of(g * PW + lo, HD), HD), :]
                        sc = masked_scores(q, k, ok)
                        p = jnp.exp(sc - ml[h:h + 1, :]) * ml[2 + h:3 + h, :]
                        dp = tn(v, do)
                        ds = (p * (dp - over_rows(jnp.sum, dp * p))).astype(bf16)
                        dv = nt(p.astype(bf16), do).T
                        dk = rot_back(nt(ds, q).T)
                        dq = rot_back(nn(k, ds)) * QS
                        for j, t in enumerate((dq, dk, dv)):
                            at = pl.ds(base + j * PW + lo, HD)
                            dq_s[sh, at, :] = t.astype(bf16)
                            gb_a[at, :] += over_cols(jnp.sum, t)

                    acc[g, :R3, :] += nn(dq_s[sh, pl.ds(base, R3), :], h1_s[s])
                    if half == 0:
                        @pl.when((sh == 0) & (n == 1))
                        def _():
                            rs_m.second([buf, r.landing.at[pl.ds(FB, FB)]], r.chunk, [r.m_stage.at[2]])
                            rs_m.send_second()
                    else:
                        @pl.when(sh == n_half - 1)
                        def _():
                            rs.block_done(g, g)

                            @pl.when(n > 0)
                            def _():
                                rs.later(slot_at(n - 1), slot_at(n - 1), n < TP - 1)

                pair = lambda rows: pl.BlockSpec((1, 1, rows, S), lambda n, sh: (half * n_half + sh, slot_at(n), 0, 0))
                pltpu.emit_pipeline(body, grid=(TP, n_half), in_specs=[pair(R3), pair(4)])(r.qkv, r.ml)
                if half == 0:
                    wq_cp.wait()

                def close_bwd(x_ref):
                    sh = pl.program_id(0)
                    s = half * n_half + sh
                    rows = pl.ds(pl.multiple_of(s * S, S), S)
                    dh1 = tn(dq_s[sh], wq_v[...].reshape(TP * R3, D))
                    xh, inv = ln_stats(x_ref[0].astype(f32))
                    r.va[4:5, :] += over_rows(jnp.sum, dh1 * xh)
                    r.va[5:6, :] += over_rows(jnp.sum, dh1)
                    h1_s[s] = (r.dacc[rows, :] + ln_grad(dh1, xh, inv, gain1[...])).astype(bf16)
                    gx_a2a.start(s)
                    cp = gx_a2a.local_out(s, h1_s)
                    cp.start()
                    cp.wait()

                pltpu.emit_pipeline(close_bwd, grid=(n_half,),
                                    in_specs=[pl.BlockSpec((1, S, D), lambda sh: (half * n_half + sh, 0, 0))])(r.xs)
            last = jnp.int32(TP - 1)
            rs.later(last, last, False)
            rs.second([buf, r.landing.at[pl.ds(FB, FB)]], r.chunk, [r.gq_b, r.go_b])

        pl.run_scoped(heads, vm(n_half, TP * R3, S, dtype=bf16), vm(TP, R3, D, dtype=bf16), vm(FB, D))

        for g in range(TP):
            r.msg[g] = r.va[...]
            for j in range(3):
                cols = jnp.broadcast_to(gb_a[g * R3 + j * PW:g * R3 + (j + 1) * PW, :], (PW, PW))
                r.msg[g, 6:7, j * PW:(j + 1) * PW] = cols.T[0:1, :]
            r.msg[g, 6:7, R3:R3 + FB] = r.gbu[g]
        pair = remote(r.msg, r.msg_in, r.s_ss.at[0], r.s_rs.at[0], pc.partner)
        pair.start()
        pair.wait()
        r.msg_in[...] = r.msg_in[...] + r.msg[...]
        chip = lax.div(pc.me, 2)
        small = [remote(r.msg_in.at[pc.slot_of(m)], r.msgs.at[chip], r.s_ss.at[1], r.s_rs.at[1], pc.peer(m)) for m in (2, 4, 6)]
        for cp in small:
            cp.start()
        own = pltpu.make_async_copy(r.msg_in.at[pc.slot_of(0)], r.msgs.at[chip], r.s_ss.at[2])
        own.start()

        def tail(bufs, act_v, turned):
            b0, b1, b2 = (bufs.at[i] for i in range(3))
            y_own = [(pltpu.make_async_copy(r.y_seq.at[s, y_a2a._rows(pc.me)], act_v.at[s], r.tmp.at[s]),
                      pltpu.make_async_copy(act_v.at[s], r.y_out.at[pc.me * NS + s], r.tmp.at[NS + s])) for s in range(NS)]
            for load, _ in y_own:
                load.start()
            for load, store in y_own:
                load.wait()
                store.start()
            for g in (g_bs, g_wq, g_wo, g_wu, g_wd):
                g.sent()
            for _, store in y_own:
                store.wait()
            rs_m.finish()
            wait_for(r.m_r1.at[0], r.m_sem.at[4])
            for p in range(2):
                half = pl.ds(p * FB, FB)
                for cp in load_all([(r.m_stage.at[3, half], b0), (r.m_r1.at[0, half], b1), (r.m_r2.at[half], b2)], r.tmp):
                    cp.wait()
                row_add(b0, [b1, b2])
                if p == 0:
                    cp = pltpu.make_async_copy(b0, r.gd, r.tmp.at[0])
                else:
                    for k in range(D // FB):
                        cols = slice(k * FB, (k + 1) * FB)
                        turned[cols, :] = b0[:, cols].T
                    cp = pltpu.make_async_copy(turned, r.gu, r.tmp.at[0])
                cp.start()
                cp.wait()
            rs.own_part(b0, b1, r.tmp, (r.gq_own, r.go_own))
            y_a2a.finish_all()
            gx_a2a.finish_all()
            rs.sent_first()
            own.wait()
            for sem in (r.s_ss.at[1], r.s_rs.at[1]):
                wait_for(r.msgs.at[pl.ds(0, len(small))], sem)

        pl.run_scoped(tail, vm(3, FB, D), vm(NS, SL, D, dtype=bf16), vm(D, FB))

    seqs = vm(NS, S, D, dtype=bf16)
    pl.run_scoped(attn_bwd, seqs, vm(NS, D, S, dtype=bf16), vm(TP, R3 + PW, D), vm(TP * R3, 1))


def layer_call(*args):
    out = pl.pallas_call(
        layer_kernel,
        in_specs=[ANY] * len(IN_NAMES),
        out_specs=[ANY] * len(OUT_SHAPES),
        out_shape=[sds(*v) for v in OUT_SHAPES.values()],
        scratch_shapes=list(SCRATCH.values()),
        compiler_params=pltpu.CompilerParams(collective_id=0, has_side_effects=True, vmem_limit_bytes=VMEM_LIMIT),
        name="layer",
    )(*args)
    return out[:9]


FINAL = {"y": ((TP * NS, SL, D), bf16), "gx": ((TP * NS, SL, D), bf16), "gd": ((FB, D), f32), "gu": ((D, FB), f32),
         "gbq": ((3, 2, HD), f32), "gbu": ((1, FB), f32)}
VECS = ("bd", "g2", "b2", "bo", "g1", "b1")
FINAL |= {k: ((1, D), f32) for k in VECS}
LATE = ("gbq", "gbu") + VECS


def final_kernel(y_in, gx_in, msgs, gd_in, gu_in, *refs):
    outs, refs = Refs(FINAL, refs), refs[len(FINAL):]
    msg_v, y_v, gx_v, gd_v, gu_v, ld, st = refs[:7]
    late = Refs(LATE, refs[7:])
    moves = [([(msgs, msg_v)], [])]
    for src, buf, dst in ((gd_in, gd_v, outs.gd), (gu_in, gu_v, outs.gu), (y_in, y_v, outs.y), (gx_in, gx_v, outs.gx)):
        moves.append(([(src, buf)], [(buf, dst)]))
    copy = pltpu.make_async_copy
    loads = [[copy(s, d, ld.at[i]) for s, d in m[0]] for i, m in enumerate(moves)]
    stores = [[copy(s, d, st.at[i]) for s, d in m[1]] for i, m in enumerate(moves)]
    for cps in loads:
        for cp in cps:
            cp.start()
    for i, (cps, outward) in enumerate(zip(loads, stores)):
        for cp in cps:
            cp.wait()
        if i == 0:
            small = msg_v[0]
            for j in range(1, msg_v.shape[0]):
                small = small + msg_v[j]
            for j, k in enumerate(VECS):
                getattr(late, k)[...] = small[j:j + 1, :]
            for j in range(3):
                for h in range(2):
                    lo = j * PW + h * HD
                    late.gbq[j, h:h + 1, :] = small[6:7, lo:lo + HD]
            late.gbu[...] = small[6:7, R3:R3 + FB]
        for cp in outward:
            cp.start()
    small_out = load_all([(getattr(late, k), getattr(outs, k)) for k in LATE], st.at[pl.ds(len(moves), len(LATE))])
    for cps in stores + [small_out]:
        for cp in cps:
            cp.wait()


def final_call(y, gx, msgs, gd, gu):
    act = vm(*y.shape, dtype=bf16)
    return pl.pallas_call(
        final_kernel,
        in_specs=[ANY] * 5,
        out_specs=[ANY] * len(FINAL),
        out_shape=[sds(*v) for v in FINAL.values()],
        scratch_shapes=[vm(*msgs.shape), act, act, vm(FB, D), vm(D, FB), DMA((5,)), DMA((5 + len(LATE),))]
        + [vm(*FINAL[k][0]) for k in LATE],
        compiler_params=pltpu.CompilerParams(vmem_limit_bytes=VMEM_LIMIT),
        cost_estimate=pl.CostEstimate(flops=10 ** 10, bytes_accessed=3 * 10 ** 7, transcendentals=0),
        name="results",
    )(y, gx, msgs, gd, gu)


def rope_tables():
    inv_freq = (ROPE_BASE ** (-2.0 * np.arange(HH, dtype=np.float32) / HD)).astype(np.float32)
    angles = np.outer(inv_freq, np.arange(S, dtype=np.float32))
    return np.cos(angles), np.sin(angles)


def solution(mesh):
    no = None
    act_spec = P('dp', 'tp', no)
    rep, part = P(no), P('dp')
    in_specs = (act_spec, act_spec, P('dp', no), rep, rep, P(no, no, 'tp', no), P(no, 'tp', no),
                P('tp', no, no), rep, rep, rep, P(no, 'tp'), P('tp'), P('tp', no), rep)
    out_specs = (act_spec, act_spec, part, part, P('dp', no, 'tp', no), P('dp', 'tp', no), P(('dp', 'tp'), no, no),
                 part, part, part, P('dp', 'tp'), P(('dp', 'tp')), P(('dp', 'tp'), no), part)

    def device_step(x_in, grad_y, pad_mask, ln1_gain, ln1_bias, w_qkv, b_qkv, w_out, b_out, ln2_gain, ln2_bias, w_up, b_up, w_down, b_down):
        assert x_in.shape == (TP * NS, SL, D) and w_qkv.shape == (3, D, 2, HD) and w_up.shape == (D, FB)
        row = lambda v: v.reshape(1, -1)
        wq = w_qkv.transpose(0, 2, 3, 1).reshape(R3, D)
        cos, sin = rope_tables()
        parts = layer_call(
            x_in, grad_y, wq, w_out.reshape(PW, D), w_up, w_down, b_qkv, row(b_up), pad_mask, cos, sin,
            row(ln1_gain), row(ln1_bias), row(ln2_gain), row(ln2_bias), row(b_out), row(b_down))
        *parts, gq_own, go_own, gq_b, go_b = parts
        to_b = [(i, i ^ (4 - 2 * (i % 2))) for i in range(TP)]
        gq = gq_own + lax.ppermute(gq_b, 'tp', to_b)
        go = lax.ppermute(go_b, 'tp', to_b)
        gq, go_own = lax.optimization_barrier((gq, go_own))
        go = go_own + go
        y, gx, gd, gu, gbq, gbu, *vecs = final_call(*parts)
        bd, g2, b2, bo, g1, b1 = (v.reshape(D) for v in vecs)
        return (y, gx, g1, b1, gq.reshape(3, 2, HD, D).transpose(0, 3, 1, 2), gbq, go.reshape(2, HD, D), bo, g2, b2,
                gu, gbu.reshape(FB), gd, bd)

    return jax.shard_map(device_step, mesh=mesh, in_specs=in_specs, out_specs=out_specs, check_vma=False)
```
